32 devices in a mesh: dp: 8 (over y, x, core), tensor: 4 (over z).
Axes of the slice: x: 2, y: 2, z: 4, core: 2. Of those that a mesh axis runs over, the one named last changes fastest.
Arguments:
- block_input: bfloat16 [8192, 2048], P('dp'), may hold values from -24 to 24
- segments: int32 [8192], P('dp'), may hold values from 0 to 15, never falling along the last dimension, each value on 1 to 2048 neighbouring positions
- norm_gain: bfloat16 [2048], P('dp'), may hold values from 0.5 to 1.5
- norm_bias: bfloat16 [2048], P('dp'), may hold values from -1.75 to 1.75
- qkv_weight: bfloat16 [2048, 3, 2048], P('dp', None, 'tensor'), may hold values from -1 to 1
- query_value_bias: bfloat16 [2, 32, 64], P(None, 'tensor', 'dp'), may hold values from -1.75 to 1.75
- key_bias: bfloat16 [32, 32], P('tensor', 'dp'), may hold values from -3 to 3
- dense_weight: bfloat16 [2048, 2048], P('tensor', 'dp'), may hold values from -1.5 to 1.5
- dense_bias: bfloat16 [2048], P('dp'), may hold values from -1.75 to 1.75
- up_weight: bfloat16 [2048, 8192], P('dp', 'tensor'), may hold values from -0.125 to 0.125
- up_bias: bfloat16 [128, 64], P('tensor', 'dp'), may hold values from -1.75 to 1.75
- down_weight: bfloat16 [8192, 2048], P('tensor', 'dp'), may hold values from -0.0625 to 0.0625
- down_bias: bfloat16 [2048], P('dp'), may hold values from -1.75 to 1.75
- cotangent: bfloat16 [8192, 2048], P('dp'), may hold values from -8 to 8
Outputs:
- block_output: bfloat16 [8192, 2048], P('dp')
- input_grad: float32 [8192, 2048], P('dp')
- norm_gain_grad: float32 [2048], P('dp')
- norm_bias_grad: float32 [2048], P('dp')
- qkv_weight_grad: float32 [2048, 3, 2048], P('dp', None, 'tensor')
- query_value_bias_grad: float32 [2, 32, 64], P(None, 'tensor', 'dp')
- key_bias_grad: float32 [32, 32], P('tensor', 'dp')
- dense_weight_grad: float32 [2048, 2048], P('tensor', 'dp')
- dense_bias_grad: float32 [2048], P('dp')
- up_weight_grad: float32 [2048, 8192], P('dp', 'tensor')
- up_bias_grad: float32 [128, 64], P('tensor', 'dp')
- down_weight_grad: float32 [8192, 2048], P('tensor', 'dp')
- down_bias_grad: float32 [2048], P('dp')
The draws below stay inside these ranges and needn't reach their ends.
Inputs may be any that keep to these rules, and one draw needn't show every extreme that they name: `segments`: segment numbers never fall along the tokens; each segment has 1 to 2048 tokens, one exactly 2048.
All inputs are finite; a program needn't handle non-finite values.
Results may differ from the reference program's by a relative error of at most 0.015.
The reference program's roundings to bfloat16 on the way count: a program that leaves them out, or rounds other values in their place, can miss the bound.
Values may be sent and summed in bfloat16 or wider, within the bound.
A program may use at most 256 MiB of HBM per device.

```python
import math
import jax
import jax.numpy as jnp
import numpy as np
from jax import lax

D = 2048
HEADS = 32
HEAD = 64
ROT = 32
FF = 8192
SEQ = 512
TOKENS = 8192


def draw_block_input(key, part):
    normal_draw = jax.random.normal(key, (TOKENS, D), jnp.float32)
    return jnp.clip(normal_draw, -6.0, 6.0).astype(jnp.bfloat16)


def draw_qkv_weight(key, part):
    drawn = jax.random.normal(key, (D, 3, HEADS, HEAD), jnp.float32) * float(D) ** (-0.5)
    return jnp.clip(drawn, -1.0, 1.0).reshape(D, 3, D).astype(jnp.bfloat16)


def strengthened(values, rng, source, target, parts, factor):
    owner, partner = [(jnp.arange(values.shape[axis_at]) // (values.shape[axis_at] // parts)).reshape([-1 if axis == axis_at else 1 for axis in range(values.ndim)]) for axis_at in (source, target)]
    chosen = jax.random.permutation(rng, parts)[partner]
    strong = (owner == chosen) | (owner == (partner + parts // 2) % parts)
    return jnp.where(strong, factor * values, values)


def level_of(rng, extent, pieces, smallest, high):
    def one(axis_at, parts):
        heights = jax.random.uniform(jax.random.fold_in(jax.random.fold_in(rng, 6), axis_at), (parts,), jnp.float32, smallest / len(pieces), high / len(pieces))
        return jnp.repeat(jnp.exp(heights), extent[axis_at] // parts).reshape((-1,) + (1,) * (len(extent) - axis_at - 1))

    gain = one(*pieces[0])
    for cut in pieces[1:]:
        gain = gain * one(*cut)
    return gain


def split_up(number_of, total, most, slope):
    weights = [(1 << 20) // math.isqrt(rank ** slope) + 1 for rank in range(2, number_of + 1)]
    rest, given = total - most - (number_of - 1), [1] * (number_of - 1)
    while rest > 0:
        free = [i for i in range(number_of - 1) if given[i] < most]
        mass, budget = sum([weights[i] for i in free]), rest
        for i in free:
            extra = min(most - given[i], max(1, budget * weights[i] // mass), rest)
            given[i] = given[i] + extra
            rest = rest - extra
    return np.array([most] + given)


def uneven(stream_key, number_of, total, most, slope):
    if number_of == 2:
        one = jax.random.randint(stream_key, (), max(1, total - most), min(most, total - 1) + 1)
        return jnp.stack([one, total - one])
    lengths = jnp.asarray(split_up(number_of, total, most, slope), jnp.int32)
    pairs = (number_of - 1) // 2
    giver, taker = lengths[1:1 + 2 * pairs:2], lengths[2:2 + 2 * pairs:2]
    margin = jnp.minimum(giver - 1, most - taker)
    passed = jax.random.randint(jax.random.fold_in(stream_key, 1), (pairs,), 0, 1 << 20) % (margin + 1)
    lengths = lengths.at[1:1 + 2 * pairs:2].set(giver - passed).at[2:2 + 2 * pairs:2].set(taker + passed)
    return lengths[jax.random.permutation(jax.random.fold_in(stream_key, 2), number_of)]


def bell_draw(rng, extent, deviation, bound, split=(), kind=jnp.bfloat16):
    result = jax.random.normal(rng, extent, jnp.float32) * deviation
    if len(split) > 0:
        result = level_of(rng, extent, split, -0.22, 0.18) * result
    return jnp.clip(result, min=-bound, max=bound).astype(kind)


def gaussian_with(rng, extent, width, most, shards, heavy, kind=jnp.bfloat16):
    entries = width * jax.random.normal(rng, extent, jnp.float32)
    if shards:
        entries = entries * level_of(rng, extent, shards, -0.22, 0.18)
    return jnp.clip(strengthened(entries, jax.random.fold_in(rng, 3), *heavy), -most, most).astype(kind)


def setup_inputs(seed: int = 0) -> dict:
    keys = jax.random.split(jax.random.key(seed), 15)
    block_input = draw_block_input(jax.random.fold_in(keys[14], 71), 0)
    segments = jnp.searchsorted(jnp.cumsum(uneven(keys[1], TOKENS // SEQ, TOKENS, 4 * SEQ, 1)), jnp.arange(TOKENS), side="right").astype(jnp.int32)
    norm_gain = jnp.clip(1.0 + 0.1 * jax.random.normal(keys[2], (D,), jnp.float32), 0.5, 1.5).astype(jnp.bfloat16)
    norm_bias = bell_draw(keys[3], (D,), 0.3, 1.75, ((0, 8),))
    qkv_weight = draw_qkv_weight(jax.random.fold_in(keys[14], 71), 0)
    query_value_bias = bell_draw(keys[5], (2, HEADS, HEAD), 0.3, 1.75, ((1, 4), (2, 8)))
    key_bias = bell_draw(keys[6], (HEADS, ROT), 0.5, 3.0, ((0, 4), (1, 8)))
    dense_weight = bell_draw(keys[7], (D, D), (D // 128) ** -0.5, 1.5, ((0, 4), (1, 8)))
    dense_bias = bell_draw(keys[8], (D,), 0.3, 1.75, ((0, 8),))
    up_weight = bell_draw(keys[9], (D, FF), D ** -0.5, 0.125, ((0, 8), (1, 4)))
    up_bias = bell_draw(keys[10], (FF // 64, 64), 0.3, 1.75, ((0, 4), (1, 8)))
    down_weight = bell_draw(keys[11], (FF, D), FF ** -0.5, 0.0625, ((0, 4), (1, 8)))
    down_bias = bell_draw(keys[12], (D,), 0.3, 1.75, ((0, 8),))
    cotangent = gaussian_with(keys[13], (TOKENS, D), 1.0, 8.0, ((0, 8),), (0, 1, 8, 2.0))
    return {"block_input": block_input, "segments": segments, "norm_gain": norm_gain, "norm_bias": norm_bias, "qkv_weight": qkv_weight, "query_value_bias": query_value_bias, "key_bias": key_bias, "dense_weight": dense_weight, "dense_bias": dense_bias, "up_weight": up_weight, "up_bias": up_bias, "down_weight": down_weight, "down_bias": down_bias, "cotangent": cotangent}


EPSILON = 1e-05
SCALE = 0.125
NEGATIVE = -1e+30

def rotary_tables(seg_rows):
    seq_len = seg_rows.shape[1]
    position = jnp.arange(seq_len, dtype=jnp.int32)
    starting = jnp.concatenate([jnp.ones((seg_rows.shape[0], 1), dtype=jnp.bool_), seg_rows[:, 1:] != seg_rows[:, :-1]], axis=1)
    starts = lax.cummax(jnp.where(starting, position[None, :], jnp.int32(0)), axis=1)
    offset = (position[None, :] - starts).astype(jnp.float32)
    halfway = ROT // 2
    inverse = 10000.0 ** (-(jnp.arange(halfway, dtype=jnp.float32) * (2.0 / ROT)))
    angles = offset[:, :, None] * inverse
    return (jnp.cos(angles), jnp.sin(angles))

def rotate(tensor, cosine_table, sine_table, direction):
    halfway = ROT // 2
    leading = tensor[..., :halfway]
    trailing = tensor[..., halfway:ROT]
    others = tensor[..., ROT:]
    cosine_part = cosine_table[:, :, None, :]
    sine_part = sine_table[:, :, None, :] * direction
    return jnp.concatenate([leading * cosine_part - trailing * sine_part, trailing * cosine_part + leading * sine_part, others], axis=-1)

def allowed_pairs(seg_rows):
    seq_len = seg_rows.shape[1]
    position = jnp.arange(seq_len, dtype=jnp.int32)
    causal = position[:, None] >= position[None, :]
    same_doc = seg_rows[:, :, None] == seg_rows[:, None, :]
    return (same_doc & causal[None])[:, None]

def gelu_tanh(inputs):
    return jax.nn.gelu(inputs, approximate=True)

def reference(block_input, segments, norm_gain, norm_bias, qkv_weight, query_value_bias, key_bias, dense_weight, dense_bias, up_weight, up_bias, down_weight, down_bias, cotangent):
    per_block = SEQ * 8 if TOKENS // SEQ % 8 == 0 else SEQ
    block_count = TOKENS // per_block
    gain_wide = norm_gain.astype(jnp.float32)
    shift_wide = norm_bias.astype(jnp.float32)
    qv_wide = query_value_bias.astype(jnp.float32)
    key_full = jnp.concatenate([key_bias.astype(jnp.float32), jnp.zeros((HEADS, HEAD - ROT), jnp.float32)], axis=1)
    up_flat = up_bias.reshape(FF).astype(jnp.float32)
    dense_shift = dense_bias.astype(jnp.float32)
    down_shift = down_bias.astype(jnp.float32)
    qkv_flat = qkv_weight.reshape(D, 3 * D)

    def one_block(sums_so_far, inputs):
        input_rows, grad_rows, seg_rows = inputs
        seq_count = input_rows.shape[0] // SEQ
        widened = input_rows.astype(jnp.float32)
        row_mean = lax.optimization_barrier(jnp.mean(widened, axis=1, keepdims=True))
        centred = widened - row_mean
        row_var = lax.optimization_barrier(jnp.mean(centred * centred, axis=1, keepdims=True))
        inv_std = lax.rsqrt(row_var + EPSILON)
        normed = centred * inv_std
        normed_low = (normed * gain_wide + shift_wide).astype(jnp.bfloat16)
        projected = jnp.dot(normed_low, qkv_flat, preferred_element_type=jnp.float32).reshape(seq_count, SEQ, 3, HEADS, HEAD)
        seq_segs = seg_rows.reshape(seq_count, SEQ)
        cosine_table, sine_table = rotary_tables(seq_segs)
        allowed = allowed_pairs(seq_segs)
        queries = rotate(projected[:, :, 0] + qv_wide[0], cosine_table, sine_table, 1.0).astype(jnp.bfloat16)
        key_rows = rotate(projected[:, :, 1] + key_full, cosine_table, sine_table, 1.0).astype(jnp.bfloat16)
        values = (projected[:, :, 2] + qv_wide[1]).astype(jnp.bfloat16)
        scores = jnp.einsum('nqhd,nkhd->nhqk', queries.astype(jnp.float32), key_rows.astype(jnp.float32)) * SCALE
        scores = jnp.where(allowed, scores, NEGATIVE)
        row_max = lax.optimization_barrier(jnp.max(scores, axis=-1, keepdims=True))
        row_total = lax.optimization_barrier(jnp.sum(jnp.exp(scores - row_max), axis=-1, keepdims=True))
        log_total = row_max + jnp.log(row_total)
        probabilities = jnp.exp(scores - log_total)
        prob_low = probabilities.astype(jnp.bfloat16)
        mixed_rows = jnp.einsum('nhqk,nkhd->nqhd', prob_low.astype(jnp.float32), values.astype(jnp.float32)).astype(jnp.bfloat16).reshape(-1, D)
        hidden = jnp.dot(normed_low, up_weight, preferred_element_type=jnp.float32) + up_flat
        activated = gelu_tanh(hidden).astype(jnp.bfloat16)
        branches = jnp.dot(mixed_rows, dense_weight, preferred_element_type=jnp.float32) + jnp.dot(activated, down_weight, preferred_element_type=jnp.float32)
        output_rows = (widened + branches + dense_shift + down_shift).astype(jnp.bfloat16)
        grad_wide = grad_rows.astype(jnp.float32)
        grad_bias_out = lax.optimization_barrier(jnp.sum(grad_wide, axis=0))
        grad_dense = jnp.dot(mixed_rows.T, grad_rows, preferred_element_type=jnp.float32)
        grad_down = jnp.dot(activated.T, grad_rows, preferred_element_type=jnp.float32)
        grad_mixed = jnp.dot(grad_rows, dense_weight.T, preferred_element_type=jnp.float32).astype(jnp.bfloat16).reshape(seq_count, SEQ, HEADS, HEAD)
        grad_act = jnp.dot(grad_rows, down_weight.T, preferred_element_type=jnp.float32)
        grad_hidden = jax.vjp(gelu_tanh, hidden)[1](grad_act)[0]
        grad_up_bias = lax.optimization_barrier(jnp.sum(grad_hidden, axis=0))
        grad_hidden_low = grad_hidden.astype(jnp.bfloat16)
        grad_up = jnp.dot(normed_low.T, grad_hidden_low, preferred_element_type=jnp.float32)
        grad_values = jnp.einsum('nhqk,nqhd->nkhd', prob_low.astype(jnp.float32), grad_mixed.astype(jnp.float32))
        grad_probs = jnp.einsum('nqhd,nkhd->nhqk', grad_mixed.astype(jnp.float32), values.astype(jnp.float32))
        row_delta = lax.optimization_barrier(jnp.sum(probabilities * grad_probs, axis=-1, keepdims=True))
        grad_scores = (probabilities * (grad_probs - row_delta) * SCALE).astype(jnp.bfloat16)
        grad_queries = rotate(jnp.einsum('nhqk,nkhd->nqhd', grad_scores.astype(jnp.float32), key_rows.astype(jnp.float32)), cosine_table, sine_table, -1.0)
        grad_keys = rotate(jnp.einsum('nhqk,nqhd->nkhd', grad_scores.astype(jnp.float32), queries.astype(jnp.float32)), cosine_table, sine_table, -1.0)
        grad_qv = jnp.stack([lax.optimization_barrier(jnp.sum(grad_queries, axis=(0, 1))), lax.optimization_barrier(jnp.sum(grad_values, axis=(0, 1)))])
        grad_key_bias = lax.optimization_barrier(jnp.sum(grad_keys[..., :ROT], axis=(0, 1)))
        grad_projected = jnp.stack([grad_queries, grad_keys, grad_values], axis=2).reshape(-1, 3 * D).astype(jnp.bfloat16)
        grad_qkv = jnp.dot(normed_low.T, grad_projected, preferred_element_type=jnp.float32).reshape(D, 3, D)
        grad_normed = jnp.dot(grad_projected, qkv_flat.T, preferred_element_type=jnp.float32) + jnp.dot(grad_hidden_low, up_weight.T, preferred_element_type=jnp.float32)
        grad_gain = lax.optimization_barrier(jnp.sum(grad_normed * normed, axis=0))
        grad_shift = lax.optimization_barrier(jnp.sum(grad_normed, axis=0))
        scaled = grad_normed * gain_wide
        input_grad_rows = inv_std * (scaled - lax.optimization_barrier(jnp.mean(scaled, axis=1, keepdims=True)) - normed * lax.optimization_barrier(jnp.mean(scaled * normed, axis=1, keepdims=True))) + grad_wide
        terms = (grad_gain, grad_shift, grad_qkv, grad_qv, grad_key_bias, grad_dense, grad_bias_out, grad_up, grad_up_bias, grad_down)
        updated = jax.tree.map(lambda left, right: left + right, sums_so_far, terms)
        return (updated, (output_rows, input_grad_rows))
    zeros_start = (jnp.zeros((D,), jnp.float32), jnp.zeros((D,), jnp.float32), jnp.zeros((D, 3, D), jnp.float32), jnp.zeros((2, HEADS, HEAD), jnp.float32), jnp.zeros((HEADS, ROT), jnp.float32), jnp.zeros((D, D), jnp.float32), jnp.zeros((D,), jnp.float32), jnp.zeros((D, FF), jnp.float32), jnp.zeros((FF,), jnp.float32), jnp.zeros((FF, D), jnp.float32))
    sums_final, (outputs, input_grads) = lax.scan(one_block, zeros_start, (block_input.reshape(block_count, per_block, D), cotangent.reshape(block_count, per_block, D), segments.reshape(block_count, per_block)))
    grad_gain, grad_shift, grad_qkv, grad_qv, grad_key_bias, grad_dense, grad_bias_out, grad_up, grad_up_bias, grad_down = sums_final
    return (outputs.reshape(TOKENS, D), input_grads.reshape(TOKENS, D), grad_gain, grad_shift, grad_qkv, grad_qv, grad_key_bias, grad_dense, grad_bias_out, grad_up, grad_up_bias.reshape(FF // 64, 64), grad_down, grad_bias_out)
```

```python
import functools

import jax
import jax.numpy as jnp
from jax import lax
from jax.experimental import pallas as pl
from jax.experimental.pallas import tpu as pltpu
from jax.sharding import PartitionSpec as P

HEAD = 64
ROT = 32
SEQ = 512
LANES = 128
EPSILON = 1e-05
SCALE = 0.125
NEGATIVE = -1e30

F32 = jnp.float32
BF16 = jnp.bfloat16


def dot(a, b, ca=1, cb=0):
    return lax.dot_general(a, b, (((ca,), (cb,)), ((), ())), preferred_element_type=F32)


def rotary_tables(segments):
    seg_rows = segments.reshape(-1, SEQ)
    position = jnp.arange(SEQ, dtype=jnp.int32)
    starting = jnp.concatenate(
        [jnp.ones((seg_rows.shape[0], 1), dtype=jnp.bool_), seg_rows[:, 1:] != seg_rows[:, :-1]],
        axis=1,
    )
    starts = lax.cummax(jnp.where(starting, position[None, :], jnp.int32(0)), axis=1)
    offset = (position[None, :] - starts).astype(F32).reshape(-1, 1)
    half = ROT // 2
    lane = jnp.arange(LANES, dtype=jnp.int32) % HEAD
    inverse = 10000.0 ** (-((lane % half).astype(F32) * (2.0 / ROT)))
    angles = offset * inverse[None, :]
    cosine = jnp.where(lane < ROT, jnp.cos(angles), 1.0)
    sine = jnp.sin(angles)
    return (
        cosine,
        jnp.where(lane < half, -sine, 0.0),
        jnp.where((lane >= half) & (lane < ROT), sine, 0.0),
    )


def attention_body(
    q_ref, k_ref, v_ref, go_ref, bias_ref, cos_ref, sa_ref, sb_ref, segc_ref, segr_ref,
    mixed_ref, gp_ref, gb_ref, mask_ref,
):
    half = ROT // 2

    def rotate(t, direction):
        swapped = pltpu.roll(t, LANES - half, 1) * sa_ref[...]
        swapped = swapped + pltpu.roll(t, half, 1) * sb_ref[...]
        return t * cos_ref[...] + direction * swapped

    @pl.when(pl.program_id(1) == 0)
    def _():
        rows = lax.broadcasted_iota(jnp.int32, (SEQ, SEQ), 0)
        cols = lax.broadcasted_iota(jnp.int32, (SEQ, SEQ), 1)
        allowed = (segc_ref[...] == segr_ref[0]) & (rows >= cols)
        mask_ref[...] = jnp.where(allowed, 0.0, NEGATIVE)

    q = rotate(q_ref[...] + bias_ref[0:1, :], 1.0).astype(BF16)
    k = rotate(k_ref[...] + bias_ref[1:2, :], 1.0).astype(BF16)
    v = (v_ref[...] + bias_ref[2:3, :]).astype(BF16)
    go = go_ref[...]
    lane = lax.broadcasted_iota(jnp.int32, (SEQ, LANES), 1)
    mixed = gq = gk = gv = None
    for h in range(LANES // HEAD):
        mine = (lane // HEAD) == h
        zero = jnp.zeros((), BF16)
        kh = jnp.where(mine, k, zero)
        vh = jnp.where(mine, v, zero)
        qh = jnp.where(mine, q, zero)
        gh = jnp.where(mine, go, zero)
        s = dot(q, kh, 1, 1) * SCALE + mask_ref[...]
        top = jnp.max(s, axis=1, keepdims=True)
        e = jnp.exp(s - top)
        p = e / jnp.sum(e, axis=1, keepdims=True)
        low = p.astype(BF16)
        dp = dot(go, vh, 1, 1)
        delta = jnp.sum(p * dp, axis=1, keepdims=True)
        ds = (p * (dp - delta) * SCALE).astype(BF16)
        terms = (dot(low, vh), dot(ds, kh), dot(ds, qh, 0, 0), dot(low, gh, 0, 0))
        if h == 0:
            mixed, gq, gk, gv = terms
        else:
            mixed, gq, gk, gv = [a + b for a, b in zip((mixed, gq, gk, gv), terms)]
    mixed_ref[...] = mixed.astype(BF16)
    gq = rotate(gq, -1.0)
    gk = rotate(gk, -1.0)
    for i, g in enumerate((gq, gk, gv)):
        gp_ref[i] = g.astype(BF16)
        gb_ref[0, i : i + 1, :] = jnp.sum(g, axis=0, keepdims=True)


def attention(projected, grad_mixed, bias, tables, segments):
    rows = projected.shape[0]
    width = projected.shape[1] // 3
    seqs, pairs = rows // SEQ, width // LANES
    tile = lambda f: pl.BlockSpec((SEQ, LANES), f)
    table = tile(lambda s, p: (s, 0))
    return pl.pallas_call(
        attention_body,
        grid=(seqs, pairs),
        in_specs=[
            tile(lambda s, p: (s, p)),
            tile(lambda s, p: (s, pairs + p)),
            tile(lambda s, p: (s, 2 * pairs + p)),
            tile(lambda s, p: (s, p)),
            pl.BlockSpec((8, LANES), lambda s, p: (0, p)),
            table, table, table,
            pl.BlockSpec((SEQ, 1), lambda s, p: (s, 0)),
            pl.BlockSpec((1, 1, SEQ), lambda s, p: (s, 0, 0)),
        ],
        out_specs=[
            tile(lambda s, p: (s, p)),
            pl.BlockSpec((3, SEQ, LANES), lambda s, p: (0, s, p)),
            pl.BlockSpec((1, 8, LANES), lambda s, p: (s, 0, p)),
        ],
        out_shape=[
            jax.ShapeDtypeStruct((rows, width), BF16),
            jax.ShapeDtypeStruct((3, rows, width), BF16),
            jax.ShapeDtypeStruct((seqs, 8, width), F32),
        ],
        scratch_shapes=[pltpu.VMEM((SEQ, SEQ), F32)],
        compiler_params=pltpu.CompilerParams(dimension_semantics=("arbitrary", "arbitrary")),
        cost_estimate=pl.CostEstimate(
            flops=14 * rows * SEQ * width, bytes_accessed=24 * rows * width,
            transcendentals=rows * SEQ * width // HEAD,
        ),
        name="attention",
    )(
        projected, projected, projected, grad_mixed, bias, *tables,
        segments.reshape(rows, 1), segments.reshape(seqs, 1, SEQ),
    )


def gelu_tanh(inputs):
    return jax.nn.gelu(inputs, approximate=True)


def line_sum(part, finish):
    size = lax.axis_size("tensor")
    if size != 4:
        return finish(lax.psum(part, "tensor").astype(F32))
    index = lax.axis_index("tensor")
    inward = lax.ppermute(part, "tensor", [(0, 1), (3, 2)])
    pair = (part.astype(F32) + inward.astype(F32)).astype(BF16)
    other = lax.ppermute(pair, "tensor", [(1, 2), (2, 1)])
    done = finish(pair.astype(F32) + other.astype(F32))
    back = lax.ppermute(done, "tensor", [(1, 0), (2, 3)])
    return jnp.where((index == 0) | (index == size - 1), back, done)


def local(
    block_input, segments, norm_gain, norm_bias, qkv_weight, query_value_bias, key_bias,
    dense_weight, dense_bias, up_weight, up_bias, down_weight, down_bias, cotangent,
):
    rows, width = block_input.shape
    local_width = qkv_weight.shape[2]
    heads = local_width // HEAD
    seqs = rows // SEQ
    shards = lax.axis_size("dp")
    smalls = (norm_gain, norm_bias, dense_bias, down_bias, up_bias, query_value_bias, key_bias)
    packed = jnp.concatenate([s.reshape(1, -1) for s in smalls], axis=1)
    packed = lax.all_gather(packed, "dp", axis=0, tiled=True)
    pieces = []
    at = 0
    for s in smalls:
        pieces.append(packed[:, at : at + s.size].reshape((shards,) + s.shape).astype(F32))
        at += s.size
    gain, shift, dense_shift, down_shift = [p.reshape(1, -1) for p in pieces[:4]]
    up_shift = pieces[4].transpose(1, 0, 2).reshape(1, -1)
    qv_bias = pieces[5].transpose(1, 2, 0, 3).reshape(2, local_width)
    key_part = pieces[6].transpose(1, 0, 2).reshape(heads, ROT)
    key_full = jnp.concatenate([key_part, jnp.zeros((heads, HEAD - ROT), F32)], axis=1)
    bias = jnp.concatenate(
        [qv_bias[0:1], key_full.reshape(1, -1), qv_bias[1:2], jnp.zeros((5, local_width), F32)], axis=0
    )

    dense_all = lax.all_gather(dense_weight, "dp", axis=1, tiled=True)
    qkv_all = lax.all_gather(qkv_weight.reshape(qkv_weight.shape[0], -1), "dp", axis=0, tiled=True)
    up_all = lax.all_gather(up_weight, "dp", axis=0, tiled=True)
    down_all = lax.all_gather(down_weight, "dp", axis=1, tiled=True)

    wide = block_input.astype(F32)
    mean = jnp.mean(wide, axis=1, keepdims=True)
    centred = wide - mean
    inv_std = lax.rsqrt(jnp.mean(centred * centred, axis=1, keepdims=True) + EPSILON)
    normed = centred * inv_std
    low = (normed * gain + shift).astype(BF16)

    tables = rotary_tables(segments)
    grad_mixed = dot(cotangent, dense_all, 1, 1).astype(BF16)
    projected = dot(low, qkv_all)
    mixed, grad_projected, bias_sums = attention(projected, grad_mixed, bias, tables, segments)
    bias_sums = jnp.sum(bias_sums, axis=0)

    grad_dense = dot(mixed, cotangent, 0, 0).astype(BF16)
    grad_qkv = jnp.concatenate([dot(low, grad_projected[i], 0, 0).astype(BF16) for i in range(3)], axis=1)

    hidden = dot(low, up_all) + up_shift
    activated, gelu_back = jax.vjp(gelu_tanh, hidden)
    activated = activated.astype(BF16)
    branches = (dot(mixed, dense_all) + dot(activated, down_all)).astype(BF16)
    grad_hidden = gelu_back(dot(cotangent, down_all, 1, 1))[0]
    grad_up_bias = jnp.sum(grad_hidden, axis=0)
    grad_hidden_low = grad_hidden.astype(BF16)
    grad_part = dot(grad_hidden_low, up_all, 1, 1)
    for i in range(3):
        grad_part = grad_part + dot(
            grad_projected[i], qkv_all[:, i * local_width : (i + 1) * local_width], 1, 1
        )
    grad_part = grad_part.astype(BF16)
    grad_down = dot(activated, cotangent, 0, 0).astype(BF16)
    grad_up = dot(low, grad_hidden_low, 0, 0).astype(BF16)

    outs, grads = [], []
    for s in range(seqs):
        at = slice(s * SEQ, (s + 1) * SEQ)
        outs.append(
            line_sum(
                branches[at],
                lambda t, at=at: (wide[at] + t + dense_shift + down_shift).astype(BF16),
            )
        )
    for s in range(seqs):
        at = slice(s * SEQ, (s + 1) * SEQ)
        grads.append(line_sum(grad_part[at], lambda t: t.astype(BF16)))
    block_output = jnp.concatenate(outs, axis=0)
    grad_normed = jnp.concatenate(grads, axis=0).astype(F32)

    grad_wide = cotangent.astype(F32)
    scaled = grad_normed * gain
    input_grad = (
        inv_std
        * (
            scaled
            - jnp.mean(scaled, axis=1, keepdims=True)
            - normed * jnp.mean(scaled * normed, axis=1, keepdims=True)
        )
        + grad_wide
    )

    def scatter(value, dim):
        return lax.psum_scatter(value, "dp", scatter_dimension=dim, tiled=True).astype(F32)

    qkv_out = scatter(grad_qkv, 0).reshape(qkv_weight.shape)
    dense_out = scatter(grad_dense, 1)
    up_out = scatter(grad_up, 0)
    down_out = scatter(grad_down, 1)

    key_sums = bias_sums[1].reshape(heads, HEAD)[:, :ROT]
    qv_sums = jnp.stack([bias_sums[0], bias_sums[2]]).reshape(2, heads, HEAD)
    small_sums = (
        jnp.sum(grad_normed * normed, axis=0).reshape(shards, -1),
        jnp.sum(grad_normed, axis=0).reshape(shards, -1),
        jnp.sum(grad_wide, axis=0).reshape(shards, -1),
        grad_up_bias.reshape(up_bias.shape[0], shards, -1).transpose(1, 0, 2).reshape(shards, -1),
        qv_sums.reshape(2, heads, shards, -1).transpose(2, 0, 1, 3).reshape(shards, -1),
        key_sums.reshape(heads, shards, -1).transpose(1, 0, 2).reshape(shards, -1),
    )
    total = lax.psum_scatter(
        jnp.concatenate(small_sums, axis=1), "dp", scatter_dimension=0, tiled=True
    ).reshape(-1)
    shapes = (norm_gain.shape, norm_bias.shape, dense_bias.shape, up_bias.shape,
              query_value_bias.shape, key_bias.shape)
    smalls_out = []
    at = 0
    for part, shape in zip(small_sums, shapes):
        smalls_out.append(total[at : at + part.shape[1]].reshape(shape))
        at += part.shape[1]
    gain_out, shift_out, bias_out, up_bias_out, qv_out, key_out = smalls_out
    return (
        block_output, input_grad, gain_out, shift_out, qkv_out, qv_out, key_out, dense_out,
        bias_out, up_out, up_bias_out, down_out, bias_out,
    )


def solution(mesh):
    in_specs = (
        P("dp", None),
        P("dp"),
        P("dp"),
        P("dp"),
        P("dp", None, "tensor"),
        P(None, "tensor", "dp"),
        P("tensor", "dp"),
        P("tensor", "dp"),
        P("dp"),
        P("dp", "tensor"),
        P("tensor", "dp"),
        P("tensor", "dp"),
        P("dp"),
        P("dp", None),
    )
    out_specs = (
        P("dp", None),
        P("dp", None),
        P("dp"),
        P("dp"),
        P("dp", None, "tensor"),
        P(None, "tensor", "dp"),
        P("tensor", "dp"),
        P("tensor", "dp"),
        P("dp"),
        P("dp", "tensor"),
        P("tensor", "dp"),
        P("tensor", "dp"),
        P("dp"),
    )
    return jax.shard_map(local, mesh=mesh, in_specs=in_specs, out_specs=out_specs, check_vma=False)
```

```python
import functools

import jax
import jax.numpy as jnp
from jax import lax
from jax.experimental import pallas as pl
from jax.experimental.pallas import tpu as pltpu
from jax.sharding import PartitionSpec as P

HEAD = 64
ROT = 32
SEQ = 512
LANES = 128
EPSILON = 1e-05
SCALE = 0.125
NEGATIVE = -1e30

F32 = jnp.float32
BF16 = jnp.bfloat16


def dot(a, b, ca=1, cb=0):
    return lax.dot_general(a, b, (((ca,), (cb,)), ((), ())), preferred_element_type=F32)


def rotary_tables(segments):
    seg_rows = segments.reshape(-1, SEQ)
    position = jnp.arange(SEQ, dtype=jnp.int32)
    starting = jnp.concatenate(
        [jnp.ones((seg_rows.shape[0], 1), dtype=jnp.bool_), seg_rows[:, 1:] != seg_rows[:, :-1]],
        axis=1,
    )
    starts = lax.cummax(jnp.where(starting, position[None, :], jnp.int32(0)), axis=1)
    offset = (position[None, :] - starts).astype(F32).reshape(-1, 1)
    half = ROT // 2
    lane = jnp.arange(LANES, dtype=jnp.int32) % HEAD
    inverse = 10000.0 ** (-((lane % half).astype(F32) * (2.0 / ROT)))
    angles = offset * inverse[None, :]
    cosine = jnp.where(lane < ROT, jnp.cos(angles), 1.0)
    sine = jnp.sin(angles)
    return (
        cosine,
        jnp.where(lane < half, -sine, 0.0),
        jnp.where((lane >= half) & (lane < ROT), sine, 0.0),
    )


def attention_body(
    q_ref, k_ref, v_ref, go_ref, bias_ref, cos_ref, sa_ref, sb_ref, segc_ref, segr_ref,
    mixed_ref, gp_ref, gb_ref, mask_ref,
):
    half = ROT // 2

    def rotate(t, direction):
        swapped = pltpu.roll(t, LANES - half, 1) * sa_ref[...]
        swapped = swapped + pltpu.roll(t, half, 1) * sb_ref[...]
        return t * cos_ref[...] + direction * swapped

    @pl.when(pl.program_id(1) == 0)
    def _():
        rows = lax.broadcasted_iota(jnp.int32, (SEQ, SEQ), 0)
        cols = lax.broadcasted_iota(jnp.int32, (SEQ, SEQ), 1)
        allowed = (segc_ref[...] == segr_ref[0]) & (rows >= cols)
        mask_ref[...] = jnp.where(allowed, 0.0, NEGATIVE)

    q = rotate(q_ref[...] + bias_ref[0:1, :], 1.0).astype(BF16)
    k = rotate(k_ref[...] + bias_ref[1:2, :], 1.0).astype(BF16)
    v = (v_ref[...] + bias_ref[2:3, :]).astype(BF16)
    go = go_ref[...]
    lane = lax.broadcasted_iota(jnp.int32, (SEQ, LANES), 1)
    mixed = gq = gk = gv = None
    for h in range(LANES // HEAD):
        mine = (lane // HEAD) == h
        zero = jnp.zeros((), BF16)
        kh = jnp.where(mine, k, zero)
        vh = jnp.where(mine, v, zero)
        qh = jnp.where(mine, q, zero)
        gh = jnp.where(mine, go, zero)
        s = dot(q, kh, 1, 1) * SCALE + mask_ref[...]
        top = jnp.max(s, axis=1, keepdims=True)
        e = jnp.exp(s - top)
        p = e / jnp.sum(e, axis=1, keepdims=True)
        low = p.astype(BF16)
        dp = dot(go, vh, 1, 1)
        delta = jnp.sum(p * dp, axis=1, keepdims=True)
        ds = (p * (dp - delta) * SCALE).astype(BF16)
        terms = (dot(low, vh), dot(ds, kh), dot(ds, qh, 0, 0), dot(low, gh, 0, 0))
        if h == 0:
            mixed, gq, gk, gv = terms
        else:
            mixed, gq, gk, gv = [a + b for a, b in zip((mixed, gq, gk, gv), terms)]
    mixed_ref[...] = mixed.astype(BF16)
    gq = rotate(gq, -1.0)
    gk = rotate(gk, -1.0)
    for i, g in enumerate((gq, gk, gv)):
        gp_ref[i] = g.astype(BF16)
        gb_ref[0, i : i + 1, :] = jnp.sum(g, axis=0, keepdims=True)


def attention(projected, grad_mixed, bias, tables, segments):
    rows = projected.shape[0]
    width = projected.shape[1] // 3
    seqs, pairs = rows // SEQ, width // LANES
    tile = lambda f: pl.BlockSpec((SEQ, LANES), f)
    table = tile(lambda s, p: (s, 0))
    return pl.pallas_call(
        attention_body,
        grid=(seqs, pairs),
        in_specs=[
            tile(lambda s, p: (s, p)),
            tile(lambda s, p: (s, pairs + p)),
            tile(lambda s, p: (s, 2 * pairs + p)),
            tile(lambda s, p: (s, p)),
            pl.BlockSpec((8, LANES), lambda s, p: (0, p)),
            table, table, table,
            pl.BlockSpec((SEQ, 1), lambda s, p: (s, 0)),
            pl.BlockSpec((1, 1, SEQ), lambda s, p: (s, 0, 0)),
        ],
        out_specs=[
            tile(lambda s, p: (s, p)),
            pl.BlockSpec((3, SEQ, LANES), lambda s, p: (0, s, p)),
            pl.BlockSpec((1, 8, LANES), lambda s, p: (s, 0, p)),
        ],
        out_shape=[
            jax.ShapeDtypeStruct((rows, width), BF16),
            jax.ShapeDtypeStruct((3, rows, width), BF16),
            jax.ShapeDtypeStruct((seqs, 8, width), F32),
        ],
        scratch_shapes=[pltpu.VMEM((SEQ, SEQ), F32)],
        compiler_params=pltpu.CompilerParams(dimension_semantics=("arbitrary", "arbitrary")),
        cost_estimate=pl.CostEstimate(
            flops=14 * rows * SEQ * width, bytes_accessed=24 * rows * width,
            transcendentals=rows * SEQ * width // HEAD,
        ),
        name="attention",
    )(
        projected, projected, projected, grad_mixed, bias, *tables,
        segments.reshape(rows, 1), segments.reshape(seqs, 1, SEQ),
    )


ROW_TILE = 512
COL_TILE = 256


def flip(index, bit):
    return index + bit - 2 * bit * ((index // bit) % 2)


def link_bits(count):
    bits = []
    bit = count // 2
    while bit >= 2:
        bits.append(bit)
        bit //= 2
    return bits


class Unit:
    def __init__(self, share, whole, axis, rows, cols):
        self.share, self.whole, self.axis = share, whole, axis
        self.row0, self.rows = rows
        self.col0, self.cols = cols

    def own(self, half=None):
        start, size = (self.row0, self.rows) if half is None else (
            self.row0 + half * (self.rows // 2), self.rows // 2)
        return self.share.at[pl.ds(start, size), pl.ds(self.col0, self.cols)]

    def block(self, which, half=None):
        start, size = (0, self.rows) if half is None else (half * (self.rows // 2), self.rows // 2)
        if self.axis == 0:
            rows = pl.ds(pl.multiple_of(which * self.rows + start, size), size)
            return self.whole.at[rows, pl.ds(self.col0, self.cols)]
        cols = pl.ds(pl.multiple_of(which * self.cols, self.cols), self.cols)
        return self.whole.at[pl.ds(self.row0 + start, size), cols]


def front_body(
    x_hbm, cot_hbm, qkv_hbm, dense_hbm, up_hbm, down_hbm, small_ref, cos_ref, sa_ref, sb_ref,
    segc_ref, segr_ref,
    wqkv_out, wdense_out, wup_out, wdown_out, low_out, act_out, gh_out, gp_out, mixed_out,
    upg_ref, bsum_ref, vec_ref,
    wqkv, wdense, wup, wdown, low, cot, act, gh, qkv, mixed, gm, mask, vec_in,
    send, recv, vsend, vrecv, local, out_sem,
):
    count = lax.axis_size("dp")
    me = lax.axis_index("dp")
    bits = link_bits(count)
    orders = (bits, bits[::-1])
    rows, width = low.shape
    local_width = mixed.shape[1]
    units_here = act.shape[1]
    half_units = units_here // 2
    block_rows = up_hbm.shape[0]
    block_cols = down_hbm.shape[1]

    barrier = pltpu.get_barrier_semaphore()
    for bit in bits + [1]:
        pl.semaphore_signal(
            barrier, inc=1, device_id={"dp": flip(me, bit)}, device_id_type=pl.DeviceIdType.MESH)
    pl.semaphore_wait(barrier, len(bits) + 1)

    units = [
        Unit(qkv_hbm, wqkv, 0, (0, block_rows), (0, wqkv.shape[1])),
        Unit(dense_hbm, wdense, 1, (0, wdense.shape[0]), (0, block_cols)),
        Unit(up_hbm, wup, 0, (0, block_rows), (0, half_units)),
        Unit(down_hbm, wdown, 1, (0, half_units), (0, block_cols)),
        Unit(up_hbm, wup, 0, (0, block_rows), (half_units, half_units)),
        Unit(down_hbm, wdown, 1, (half_units, half_units), (0, block_cols)),
    ]

    def remote(src, dst, u, slot, bit):
        return pltpu.make_async_remote_copy(
            src_ref=src, dst_ref=dst, send_sem=send.at[u, slot], recv_sem=recv.at[u, slot],
            device_id={"dp": flip(me, bit)}, device_id_type=pl.DeviceIdType.MESH)

    def held(order, stage):
        owners = [me]
        for bit in order[:stage]:
            owners = owners + [flip(o, bit) for o in owners]
        return owners

    stages = len(bits)
    per_path = 2 ** stages - 1

    def stage_copies(u, stage):
        copies = []
        for path, order in enumerate(orders):
            for q, owner in enumerate(held(order, stage)):
                slot = path * per_path + 2 ** stage - 1 + q
                dst = units[u].block(owner, path)
                src = units[u].own(path) if stage == 0 else dst
                copies.append(remote(src, dst, u, slot, order[stage]))
        return copies

    def core_copies(u, lo=0, hi=2 ** stages):
        copies = []
        for q, owner in list(enumerate(held(bits, stages)))[lo:hi]:
            dst = units[u].block(owner)
            src = units[u].own() if q == 0 else dst
            copies.append(remote(src, dst, u, 2 * per_path + q, 1))
        return copies

    def own_copy(u):
        return pltpu.make_async_copy(units[u].own(), units[u].block(me), local.at[u])

    def start(u):
        own_copy(u).start()
        for c in stage_copies(u, 0):
            c.start()
        core_copies(u, 0, 1)[0].start()

    def advance(u, stage):
        if stage == 1:
            own_copy(u).wait()
        for c in stage_copies(u, stage - 1):
            c.wait_recv()
        if stage < stages:
            for c in stage_copies(u, stage):
                c.start()
        else:
            for c in core_copies(u, 1):
                c.start()

    def finish(u):
        for c in core_copies(u):
            c.wait_recv()

    def drain(u):
        for stage in range(stages):
            for c in stage_copies(u, stage):
                c.wait_send()
        for c in core_copies(u):
            c.wait_send()

    def save(src, dst, slot):
        return pltpu.make_async_copy(src, dst, out_sem.at[slot])

    x_copy = pltpu.make_async_copy(x_hbm, act, local.at[len(units)])
    x_copy.start()
    cot_copy = pltpu.make_async_copy(cot_hbm, cot, local.at[len(units) + 1])
    cot_copy.start()

    def vector_copies(i):
        copies = []
        for q, owner in enumerate(held(bits + [1], i)):
            copies.append(pltpu.make_async_remote_copy(
                src_ref=small_ref if q == 0 else vec_in.at[owner], dst_ref=vec_in.at[owner],
                send_sem=vsend.at[2 ** i - 1 + q], recv_sem=vrecv.at[2 ** i - 1 + q],
                device_id={"dp": flip(me, (bits + [1])[i])},
                device_id_type=pl.DeviceIdType.MESH))
        return copies

    vec_in[me] = small_ref[...]
    for i in range(stages + 1):
        for c in vector_copies(i):
            c.start()
        if i == 0:
            start(0)
            start(1)
        for c in vector_copies(i):
            c.wait_recv()
    total = vec_in[0]
    for owner in range(1, count):
        total = total + vec_in[owner]
    vec_ref[...] = total

    x_copy.wait()
    gain = vec_ref[0:1, :]
    shift = vec_ref[1:2, :]
    norm_rows = 32

    def norm_step(i, carry):
        at = pl.ds(pl.multiple_of(i * norm_rows, norm_rows), norm_rows)
        wide = act[at, :].astype(F32)
        mean = jnp.mean(wide, axis=1, keepdims=True)
        centred = wide - mean
        var = jnp.mean(centred * centred, axis=1, keepdims=True)
        normed = centred * lax.rsqrt(var + EPSILON)
        low[at, :] = (normed * gain + shift).astype(BF16)
        return carry

    lax.fori_loop(0, rows // norm_rows, norm_step, 0)
    save(low, low_out, 0).start()

    advance(0, 1)
    start(2)
    advance(1, 1)
    start(3)
    advance(0, 2)
    cot_copy.wait()
    finish(0)
    save(wqkv, wqkv_out, 1).start()

    half = ROT // 2
    row_tiles = rows // ROW_TILE

    def qkv_step(i, carry):
        @pl.when(i == 1)
        def _():
            advance(2, 1)
            start(4)

        @pl.when(i == 6)
        def _():
            advance(1, 2)

        tile = i // row_tiles
        at = pl.ds(pl.multiple_of((i % row_tiles) * ROW_TILE, ROW_TILE), ROW_TILE)
        cols = pl.ds(pl.multiple_of(tile * COL_TILE, COL_TILE), COL_TILE)
        t = dot(low[at, :], wqkv[:, cols]) + vec_ref[3:4, cols]
        wide = lambda r: jnp.concatenate([r[at, :]] * (COL_TILE // LANES), axis=1)
        turned = (
            t * wide(cos_ref)
            + pltpu.roll(t, COL_TILE - half, 1) * wide(sa_ref)
            + pltpu.roll(t, half, 1) * wide(sb_ref)
        )
        is_value = tile >= 2 * local_width // COL_TILE
        qkv[at, cols] = jnp.where(is_value, t, turned).astype(BF16)
        return carry

    lax.fori_loop(0, row_tiles * 3 * local_width // COL_TILE, qkv_step, 0)
    advance(3, 1)
    start(5)
    finish(1)
    save(wdense, wdense_out, 2).start()

    def mixed_step(i, carry):
        at = pl.ds(pl.multiple_of((i % row_tiles) * ROW_TILE, ROW_TILE), ROW_TILE)
        cols = pl.ds(pl.multiple_of((i // row_tiles) * COL_TILE, COL_TILE), COL_TILE)
        gm[at, cols] = dot(cot[at, :], wdense[cols, :], 1, 1).astype(BF16)
        return carry

    lax.fori_loop(0, row_tiles * local_width // COL_TILE, mixed_step, 0)

    bsum_ref[...] = jnp.zeros_like(bsum_ref)
    upg_ref[...] = jnp.zeros_like(upg_ref)
    pairs = local_width // LANES

    def attention_step(i, carry):
        s, p = i // pairs, i % pairs
        at = pl.ds(pl.multiple_of(s * SEQ, SEQ), SEQ)
        lanes = [
            pl.ds(pl.multiple_of(j * local_width + p * LANES, LANES), LANES) for j in range(3)
        ]

        @pl.when(i == 3)
        def _():
            advance(2, 2)

        @pl.when(i == 5)
        def _():
            advance(4, 1)

        @pl.when(p == 0)
        def _():
            across = lax.broadcasted_iota(jnp.int32, (SEQ, SEQ), 1)
            down = lax.broadcasted_iota(jnp.int32, (SEQ, SEQ), 0)
            allowed = (segc_ref[at, :] == segr_ref[s]) & (down >= across)
            mask[...] = jnp.where(allowed, 0.0, NEGATIVE)

        q, k, v = [qkv[at, l] for l in lanes]
        go = gm[at, lanes[0]]
        lane = lax.broadcasted_iota(jnp.int32, (SEQ, LANES), 1)
        zero = jnp.zeros((), BF16)
        total = None
        for h in range(LANES // HEAD):
            mine = (lane // HEAD) == h
            kh, vh, qh, gh_ = [jnp.where(mine, t, zero) for t in (k, v, q, go)]
            scores = dot(q, kh, 1, 1) * SCALE + mask[...]
            top = jnp.max(scores, axis=1, keepdims=True)
            e = jnp.exp(scores - top)
            probs = e / jnp.sum(e, axis=1, keepdims=True)
            probs_low = probs.astype(BF16)
            gprobs = dot(go, vh, 1, 1)
            delta = jnp.sum(probs * gprobs, axis=1, keepdims=True)
            gs = (probs * (gprobs - delta) * SCALE).astype(BF16)
            terms = (dot(probs_low, vh), dot(gs, kh), dot(gs, qh, 0, 0), dot(probs_low, gh_, 0, 0))
            total = terms if total is None else [a + b for a, b in zip(total, terms)]
        mixed[at, lanes[0]] = total[0].astype(BF16)

        def back(t):
            return (
                t * cos_ref[at, :]
                - pltpu.roll(t, LANES - half, 1) * sa_ref[at, :]
                - pltpu.roll(t, half, 1) * sb_ref[at, :]
            )

        grads = (back(total[1]), back(total[2]), total[3])
        for j, g in enumerate(grads):
            qkv[at, lanes[j]] = g.astype(BF16)
            bsum_ref[j : j + 1, lanes[0]] += jnp.sum(g, axis=0, keepdims=True)
        return carry

    lax.fori_loop(0, (rows // SEQ) * pairs, attention_step, 0)
    save(qkv, gp_out, 3).start()
    save(mixed, mixed_out, 4).start()
    advance(3, 2)
    finish(2)
    finish(3)
    tiles = units_here // COL_TILE

    def ffn_step(i, carry):
        @pl.when(i == 1)
        def _():
            advance(5, 1)

        @pl.when(i == row_tiles * tiles // 2 - 2)
        def _():
            advance(4, 2)

        @pl.when(i == row_tiles * tiles // 2)
        def _():
            advance(5, 2)
            finish(4)
            finish(5)
            save(wup, wup_out, 5).start()
            save(wdown, wdown_out, 6).start()

        at = pl.ds(pl.multiple_of((i % row_tiles) * ROW_TILE, ROW_TILE), ROW_TILE)
        cols = pl.ds(pl.multiple_of((i // row_tiles) * COL_TILE, COL_TILE), COL_TILE)
        hidden = dot(low[at, :], wup[:, cols]) + vec_ref[2:3, cols]
        grad = dot(cot[at, :], wdown[cols, :], 1, 1)
        square = hidden * hidden
        th = jnp.tanh(GELU_A * hidden * (1.0 + GELU_B * square))
        act[at, cols] = (0.5 * hidden * (1.0 + th)).astype(BF16)
        slope = 0.5 * (1.0 + th) + 0.5 * hidden * (1.0 - th * th) * (
            GELU_A * (1.0 + 3.0 * GELU_B * square))
        grad = grad * slope
        gh[at, cols] = grad.astype(BF16)
        upg_ref[0:1, cols] += jnp.sum(grad, axis=0, keepdims=True)
        return carry

    lax.fori_loop(0, row_tiles * tiles, ffn_step, 0)
    save(act, act_out, 7).start()
    save(gh, gh_out, 8).start()
    for u in range(len(units)):
        drain(u)
    for i in range(stages + 1):
        for c in vector_copies(i):
            c.wait_send()
    for i, (src, dst) in enumerate((
        (low, low_out), (wqkv, wqkv_out), (wdense, wdense_out), (qkv, gp_out), (mixed, mixed_out),
        (wup, wup_out), (wdown, wdown_out), (act, act_out), (gh, gh_out),
    )):
        save(src, dst, i).wait()


GELU_A = 0.7978845608028654
GELU_B = 0.044715


def front(x, cot, qkv_share, dense_share, up_share, down_share, small, tables, segments):
    rows, width = x.shape
    count = lax.axis_size("dp")
    local_width = dense_share.shape[0]
    units_here = up_share.shape[1]
    seqs = rows // SEQ
    links = len(link_bits(count))
    slots = 2 * (2 ** links - 1) + 2 ** links
    any_ = pl.BlockSpec(memory_space=pl.ANY)
    vmem = pl.BlockSpec(memory_space=pltpu.VMEM)
    b16 = lambda *s: jax.ShapeDtypeStruct(s, BF16)
    f32 = lambda *s: jax.ShapeDtypeStruct(s, F32)
    big = [
        (width, 3 * local_width), (local_width, width), (width, units_here), (units_here, width),
        (rows, width), (rows, units_here), (rows, units_here), (rows, 3 * local_width),
        (rows, local_width),
    ]
    return pl.pallas_call(
        front_body,
        in_specs=[any_] * 6 + [vmem] * 6,
        out_specs=[any_] * 9 + [vmem] * 3,
        out_shape=[b16(*s) for s in big] + [f32(8, units_here), f32(8, local_width), f32(8, width)],
        scratch_shapes=[
            pltpu.VMEM(big[0], BF16), pltpu.VMEM(big[1], BF16), pltpu.VMEM(big[2], BF16),
            pltpu.VMEM(big[3], BF16), pltpu.VMEM((rows, width), BF16), pltpu.VMEM((rows, width), BF16),
            pltpu.VMEM((rows, units_here), BF16), pltpu.VMEM((rows, units_here), BF16),
            pltpu.VMEM((rows, 3 * local_width), BF16), pltpu.VMEM((rows, local_width), BF16),
            pltpu.VMEM((rows, local_width), BF16), pltpu.VMEM((SEQ, SEQ), F32),
            pltpu.VMEM((count, 8, width), F32),
            pltpu.SemaphoreType.DMA((6, slots)), pltpu.SemaphoreType.DMA((6, slots)),
            pltpu.SemaphoreType.DMA((count - 1,)), pltpu.SemaphoreType.DMA((count - 1,)),
            pltpu.SemaphoreType.DMA((8,)), pltpu.SemaphoreType.DMA((9,)),
        ],
        compiler_params=pltpu.CompilerParams(
            collective_id=0, has_side_effects=True, vmem_limit_bytes=66_000_000),
        cost_estimate=pl.CostEstimate(
            flops=12 * rows * width * (local_width + units_here), bytes_accessed=80_000_000,
            transcendentals=rows * units_here),
        name="layer_front",
    )(
        x, cot, qkv_share, dense_share, up_share, down_share, small, *tables,
        segments.reshape(rows, 1), segments.reshape(seqs, 1, SEQ),
    )


def gelu_tanh(inputs):
    return jax.nn.gelu(inputs, approximate=True)


def line_sum(part, finish):
    size = lax.axis_size("tensor")
    if size != 4:
        return finish(lax.psum(part, "tensor").astype(F32))
    index = lax.axis_index("tensor")
    inward = lax.ppermute(part, "tensor", [(0, 1), (3, 2)])
    pair = (part.astype(F32) + inward.astype(F32)).astype(BF16)
    other = lax.ppermute(pair, "tensor", [(1, 2), (2, 1)])
    done = finish(pair.astype(F32) + other.astype(F32))
    back = lax.ppermute(done, "tensor", [(1, 0), (2, 3)])
    return jnp.where((index == 0) | (index == size - 1), back, done)


def local(
    block_input, segments, norm_gain, norm_bias, qkv_weight, query_value_bias, key_bias,
    dense_weight, dense_bias, up_weight, up_bias, down_weight, down_bias, cotangent,
):
    rows, width = block_input.shape
    local_width = qkv_weight.shape[2]
    heads = local_width // HEAD
    seqs = rows // SEQ
    shards = lax.axis_size("dp")
    wide = block_input.astype(F32)
    mean = jnp.mean(wide, axis=1, keepdims=True)
    centred = wide - mean
    inv_std = lax.rsqrt(jnp.mean(centred * centred, axis=1, keepdims=True) + EPSILON)
    normed = centred * inv_std
    tables = rotary_tables(segments)
    fused = shards & (shards - 1) == 0 and shards >= 4 and down_weight.shape[1] % LANES == 0
    if fused:
        mine = lax.axis_index("dp")

        def spread(value):
            owner = lax.broadcasted_iota(jnp.int32, (1, shards, 1), 1)
            return jnp.where(owner == mine, value[:, None, :], 0.0).reshape(1, -1)

        wide_small = [t.astype(F32) for t in (
            norm_gain, norm_bias, up_bias, query_value_bias, key_bias, dense_bias, down_bias)]
        key_row = spread(wide_small[4]).reshape(heads, ROT)
        key_row = jnp.concatenate([key_row, jnp.zeros((heads, HEAD - ROT), F32)], axis=1)
        qkv_row = jnp.concatenate(
            [spread(wide_small[3][0]), key_row.reshape(1, -1), spread(wide_small[3][1]),
             jnp.zeros((1, width - 3 * local_width), F32)], axis=1)
        small = jnp.concatenate(
            [spread(wide_small[0][None]), spread(wide_small[1][None]), spread(wide_small[2]),
             qkv_row, spread(wide_small[5][None]), spread(wide_small[6][None]),
             jnp.zeros((2, width), F32)], axis=0)
        (qkv_all, dense_all, up_all, down_all, low, activated, grad_hidden_low, grad_projected,
         mixed, up_sums, bias_sums, vectors) = front(
            block_input, cotangent, qkv_weight.reshape(qkv_weight.shape[0], -1), dense_weight,
            up_weight, down_weight, small, tables, segments)
        gain, dense_shift, down_shift = vectors[0:1], vectors[4:5], vectors[5:6]
        grad_up_bias = up_sums[0]
        grad_joined = grad_projected
    else:
        smalls = (norm_gain, norm_bias, dense_bias, down_bias, up_bias, query_value_bias, key_bias)
        packed = jnp.concatenate([s.reshape(1, -1) for s in smalls], axis=1)
        packed = lax.all_gather(packed, "dp", axis=0, tiled=True)
        pieces = []
        at = 0
        for s in smalls:
            pieces.append(packed[:, at : at + s.size].reshape((shards,) + s.shape).astype(F32))
            at += s.size
        gain, shift, dense_shift, down_shift = [p.reshape(1, -1) for p in pieces[:4]]
        up_shift = pieces[4].transpose(1, 0, 2).reshape(1, -1)
        qv_bias = pieces[5].transpose(1, 2, 0, 3).reshape(2, local_width)
        key_part = pieces[6].transpose(1, 0, 2).reshape(heads, ROT)
        key_full = jnp.concatenate([key_part, jnp.zeros((heads, HEAD - ROT), F32)], axis=1)
        bias = jnp.concatenate(
            [qv_bias[0:1], key_full.reshape(1, -1), qv_bias[1:2], jnp.zeros((5, local_width), F32)], axis=0
        )

        dense_all = lax.all_gather(dense_weight, "dp", axis=1, tiled=True)
        qkv_all = lax.all_gather(qkv_weight.reshape(qkv_weight.shape[0], -1), "dp", axis=0, tiled=True)
        up_all = lax.all_gather(up_weight, "dp", axis=0, tiled=True)
        down_all = lax.all_gather(down_weight, "dp", axis=1, tiled=True)

        low = (normed * gain + shift).astype(BF16)

        grad_mixed = dot(cotangent, dense_all, 1, 1).astype(BF16)
        projected = dot(low, qkv_all)
        mixed, grad_projected, bias_sums = attention(projected, grad_mixed, bias, tables, segments)
        bias_sums = jnp.sum(bias_sums, axis=0)

        hidden = dot(low, up_all) + up_shift
        activated, gelu_back = jax.vjp(gelu_tanh, hidden)
        activated = activated.astype(BF16)
        grad_hidden = gelu_back(dot(cotangent, down_all, 1, 1))[0]
        grad_up_bias = jnp.sum(grad_hidden, axis=0)
        grad_hidden_low = grad_hidden.astype(BF16)
        grad_joined = jnp.concatenate([grad_projected[i] for i in range(3)], axis=1)

    branches = (dot(mixed, dense_all) + dot(activated, down_all)).astype(BF16)
    grad_part = (dot(grad_joined, qkv_all, 1, 1) + dot(grad_hidden_low, up_all, 1, 1)).astype(BF16)
    grad_dense = dot(mixed, cotangent, 0, 0).astype(BF16)
    grad_qkv = dot(low, grad_joined, 0, 0).astype(BF16)
    grad_down = dot(activated, cotangent, 0, 0).astype(BF16)
    grad_up = dot(low, grad_hidden_low, 0, 0).astype(BF16)

    outs, grads = [], []
    for s in range(seqs):
        at = slice(s * SEQ, (s + 1) * SEQ)
        outs.append(
            line_sum(
                branches[at],
                lambda t, at=at: (wide[at] + t + dense_shift + down_shift).astype(BF16),
            )
        )
    for s in range(seqs):
        at = slice(s * SEQ, (s + 1) * SEQ)
        grads.append(line_sum(grad_part[at], lambda t: t.astype(BF16)))
    block_output = jnp.concatenate(outs, axis=0)
    grad_normed = jnp.concatenate(grads, axis=0).astype(F32)

    grad_wide = cotangent.astype(F32)
    scaled = grad_normed * gain
    input_grad = (
        inv_std
        * (
            scaled
            - jnp.mean(scaled, axis=1, keepdims=True)
            - normed * jnp.mean(scaled * normed, axis=1, keepdims=True)
        )
        + grad_wide
    )

    def scatter(value, dim):
        return lax.psum_scatter(value, "dp", scatter_dimension=dim, tiled=True).astype(F32)

    qkv_out = scatter(grad_qkv, 0).reshape(qkv_weight.shape)
    dense_out = scatter(grad_dense, 1)
    up_out = scatter(grad_up, 0)
    down_out = scatter(grad_down, 1)

    key_sums = bias_sums[1].reshape(heads, HEAD)[:, :ROT]
    qv_sums = jnp.stack([bias_sums[0], bias_sums[2]]).reshape(2, heads, HEAD)
    small_sums = (
        jnp.sum(grad_normed * normed, axis=0).reshape(shards, -1),
        jnp.sum(grad_normed, axis=0).reshape(shards, -1),
        jnp.sum(grad_wide, axis=0).reshape(shards, -1),
        grad_up_bias.reshape(up_bias.shape[0], shards, -1).transpose(1, 0, 2).reshape(shards, -1),
        qv_sums.reshape(2, heads, shards, -1).transpose(2, 0, 1, 3).reshape(shards, -1),
        key_sums.reshape(heads, shards, -1).transpose(1, 0, 2).reshape(shards, -1),
    )
    total = lax.psum_scatter(
        jnp.concatenate(small_sums, axis=1), "dp", scatter_dimension=0, tiled=True
    ).reshape(-1)
    shapes = (norm_gain.shape, norm_bias.shape, dense_bias.shape, up_bias.shape,
              query_value_bias.shape, key_bias.shape)
    smalls_out = []
    at = 0
    for part, shape in zip(small_sums, shapes):
        smalls_out.append(total[at : at + part.shape[1]].reshape(shape))
        at += part.shape[1]
    gain_out, shift_out, bias_out, up_bias_out, qv_out, key_out = smalls_out
    return (
        block_output, input_grad, gain_out, shift_out, qkv_out, qv_out, key_out, dense_out,
        bias_out, up_out, up_bias_out, down_out, bias_out,
    )


def solution(mesh):
    in_specs = (
        P("dp", None),
        P("dp"),
        P("dp"),
        P("dp"),
        P("dp", None, "tensor"),
        P(None, "tensor", "dp"),
        P("tensor", "dp"),
        P("tensor", "dp"),
        P("dp"),
        P("dp", "tensor"),
        P("tensor", "dp"),
        P("tensor", "dp"),
        P("dp"),
        P("dp", None),
    )
    out_specs = (
        P("dp", None),
        P("dp", None),
        P("dp"),
        P("dp"),
        P("dp", None, "tensor"),
        P(None, "tensor", "dp"),
        P("tensor", "dp"),
        P("tensor", "dp"),
        P("dp"),
        P("dp", "tensor"),
        P("tensor", "dp"),
        P("tensor", "dp"),
        P("dp"),
    )
    return jax.shard_map(local, mesh=mesh, in_specs=in_specs, out_specs=out_specs, check_vma=False)
```

```python
import functools

import jax
import jax.numpy as jnp
from jax import lax
from jax.experimental import pallas as pl
from jax.experimental.pallas import tpu as pltpu
from jax.sharding import PartitionSpec as P

HEAD = 64
ROT = 32
SEQ = 512
LANES = 128
EPSILON = 1e-05
SCALE = 0.125
NEGATIVE = -1e30

F32 = jnp.float32
BF16 = jnp.bfloat16


def dot(a, b, ca=1, cb=0):
    return lax.dot_general(a, b, (((ca,), (cb,)), ((), ())), preferred_element_type=F32)


def rotary_tables(segments):
    seg_rows = segments.reshape(-1, SEQ)
    position = jnp.arange(SEQ, dtype=jnp.int32)
    starting = jnp.concatenate(
        [jnp.ones((seg_rows.shape[0], 1), dtype=jnp.bool_), seg_rows[:, 1:] != seg_rows[:, :-1]],
        axis=1,
    )
    starts = lax.cummax(jnp.where(starting, position[None, :], jnp.int32(0)), axis=1)
    offset = (position[None, :] - starts).astype(F32).reshape(-1, 1)
    half = ROT // 2
    lane = jnp.arange(LANES, dtype=jnp.int32) % HEAD
    inverse = 10000.0 ** (-((lane % half).astype(F32) * (2.0 / ROT)))
    angles = offset * inverse[None, :]
    cosine = jnp.where(lane < ROT, jnp.cos(angles), 1.0)
    sine = jnp.sin(angles)
    return (
        cosine,
        jnp.where(lane < half, -sine, 0.0),
        jnp.where((lane >= half) & (lane < ROT), sine, 0.0),
    )


def attention_body(
    q_ref, k_ref, v_ref, go_ref, bias_ref, cos_ref, sa_ref, sb_ref, segc_ref, segr_ref,
    mixed_ref, gp_ref, gb_ref, mask_ref,
):
    half = ROT // 2

    def rotate(t, direction):
        swapped = pltpu.roll(t, LANES - half, 1) * sa_ref[...]
        swapped = swapped + pltpu.roll(t, half, 1) * sb_ref[...]
        return t * cos_ref[...] + direction * swapped

    @pl.when(pl.program_id(1) == 0)
    def _():
        rows = lax.broadcasted_iota(jnp.int32, (SEQ, SEQ), 0)
        cols = lax.broadcasted_iota(jnp.int32, (SEQ, SEQ), 1)
        allowed = (segc_ref[...] == segr_ref[0]) & (rows >= cols)
        mask_ref[...] = jnp.where(allowed, 0.0, NEGATIVE)

    q = rotate(q_ref[...] + bias_ref[0:1, :], 1.0).astype(BF16)
    k = rotate(k_ref[...] + bias_ref[1:2, :], 1.0).astype(BF16)
    v = (v_ref[...] + bias_ref[2:3, :]).astype(BF16)
    go = go_ref[...]
    lane = lax.broadcasted_iota(jnp.int32, (SEQ, LANES), 1)
    mixed = gq = gk = gv = None
    for h in range(LANES // HEAD):
        mine = (lane // HEAD) == h
        zero = jnp.zeros((), BF16)
        kh = jnp.where(mine, k, zero)
        vh = jnp.where(mine, v, zero)
        qh = jnp.where(mine, q, zero)
        gh = jnp.where(mine, go, zero)
        s = dot(q, kh, 1, 1) * SCALE + mask_ref[...]
        top = jnp.max(s, axis=1, keepdims=True)
        e = jnp.exp(s - top)
        p = e / jnp.sum(e, axis=1, keepdims=True)
        low = p.astype(BF16)
        dp = dot(go, vh, 1, 1)
        delta = jnp.sum(p * dp, axis=1, keepdims=True)
        ds = (p * (dp - delta) * SCALE).astype(BF16)
        terms = (dot(low, vh), dot(ds, kh), dot(ds, qh, 0, 0), dot(low, gh, 0, 0))
        if h == 0:
            mixed, gq, gk, gv = terms
        else:
            mixed, gq, gk, gv = [a + b for a, b in zip((mixed, gq, gk, gv), terms)]
    mixed_ref[...] = mixed.astype(BF16)
    gq = rotate(gq, -1.0)
    gk = rotate(gk, -1.0)
    for i, g in enumerate((gq, gk, gv)):
        gp_ref[i] = g.astype(BF16)
        gb_ref[0, i : i + 1, :] = jnp.sum(g, axis=0, keepdims=True)


def attention(projected, grad_mixed, bias, tables, segments):
    rows = projected.shape[0]
    width = projected.shape[1] // 3
    seqs, pairs = rows // SEQ, width // LANES
    tile = lambda f: pl.BlockSpec((SEQ, LANES), f)
    table = tile(lambda s, p: (s, 0))
    return pl.pallas_call(
        attention_body,
        grid=(seqs, pairs),
        in_specs=[
            tile(lambda s, p: (s, p)),
            tile(lambda s, p: (s, pairs + p)),
            tile(lambda s, p: (s, 2 * pairs + p)),
            tile(lambda s, p: (s, p)),
            pl.BlockSpec((8, LANES), lambda s, p: (0, p)),
            table, table, table,
            pl.BlockSpec((SEQ, 1), lambda s, p: (s, 0)),
            pl.BlockSpec((1, 1, SEQ), lambda s, p: (s, 0, 0)),
        ],
        out_specs=[
            tile(lambda s, p: (s, p)),
            pl.BlockSpec((3, SEQ, LANES), lambda s, p: (0, s, p)),
            pl.BlockSpec((1, 8, LANES), lambda s, p: (s, 0, p)),
        ],
        out_shape=[
            jax.ShapeDtypeStruct((rows, width), BF16),
            jax.ShapeDtypeStruct((3, rows, width), BF16),
            jax.ShapeDtypeStruct((seqs, 8, width), F32),
        ],
        scratch_shapes=[pltpu.VMEM((SEQ, SEQ), F32)],
        compiler_params=pltpu.CompilerParams(dimension_semantics=("arbitrary", "arbitrary")),
        cost_estimate=pl.CostEstimate(
            flops=14 * rows * SEQ * width, bytes_accessed=24 * rows * width,
            transcendentals=rows * SEQ * width // HEAD,
        ),
        name="attention",
    )(
        projected, projected, projected, grad_mixed, bias, *tables,
        segments.reshape(rows, 1), segments.reshape(seqs, 1, SEQ),
    )


ROW_TILE = 512
QUERY_TILE = 256
COL_TILE = 256
GRAD_TILE = 512
CHUNK = 128
SLOTS = 8
NORM_ROWS = 32
BACK_ROWS = 16
GELU_A = 0.7978845608028654
GELU_B = 0.044715
MESH = pl.DeviceIdType.MESH


def flip(index, bit):
    return index + bit - 2 * bit * ((index // bit) % 2)


def link_bits(count):
    bits = []
    bit = count // 2
    while bit >= 2:
        bits.append(bit)
        bit //= 2
    return bits


def aligned(start, size):
    return pl.ds(pl.multiple_of(start, size), size)


class Unit:
    def __init__(self, share, whole, axis, rows, cols, row_at=0, col_at=0):
        self.share, self.whole, self.axis = share, whole, axis
        self.row0, self.rows = rows
        self.col0, self.cols = cols
        self.row_at, self.col_at = row_at, col_at

    def span(self, half):
        return (0, self.rows) if half is None else (half * (self.rows // 2), self.rows // 2)

    def own(self, half=None):
        start, size = self.span(half)
        return self.share.at[pl.ds(self.row0 + start, size), pl.ds(self.col0, self.cols)]

    def block(self, which, half=None):
        start, size = self.span(half)
        if self.axis == 0:
            rows = aligned(which * self.rows + start, size)
            return self.whole.at[rows, pl.ds(self.col_at, self.cols)]
        cols = aligned(which * self.cols, self.cols)
        return self.whole.at[pl.ds(self.row_at + start, size), cols]


def layer_body(
    x_hbm, cot_hbm, qkv_hbm, dense_hbm, up_hbm, down_hbm, small_ref, cos_ref, sin_ref, seg_ref,
    block_out, input_grad, qkv_out, dense_out, up_out, down_out, core_rx, link_rx, sums_ref,
    wqu, wdd, acts, low, cot, mask, vec_ref, vec_in, turned, gn, part, inbox, cross,
    send, recv, vsend, vrecv, local,
    a_send, a_recv, b_send, b_recv, c_send, c_recv, z_out, credit,
    core_send, core_recv, link_send, link_recv, fetch_sem, grad_sem, row_sem, sum_send, sum_recv,
):
    count = lax.axis_size("dp")
    me = lax.axis_index("dp")
    depth = lax.axis_size("tensor")
    level = lax.axis_index("tensor")
    outer = (level == 0) | (level == depth - 1)
    inner = jnp.logical_not(outer)
    bits = link_bits(count)
    orders = (bits, bits[::-1])
    stages = len(bits)
    per_path = 2 ** stages - 1
    rows, width = low.shape
    units_here = up_hbm.shape[1]
    local_width = dense_hbm.shape[0]
    qkv_cols = 3 * local_width
    half_units = units_here // 2
    block_rows = up_hbm.shape[0]
    block_cols = down_hbm.shape[1]
    gh_at = qkv_cols
    mix_at = qkv_cols + units_here
    act_at = mix_at + local_width
    row_tiles = rows // ROW_TILE

    barrier = pltpu.get_barrier_semaphore()
    for bit in bits + [1]:
        pl.semaphore_signal(barrier, inc=1, device_id={"dp": flip(me, bit)}, device_id_type=MESH)
    for other in (flip(level, 1), depth - 1 - level):
        pl.semaphore_signal(barrier, inc=1, device_id={"tensor": other}, device_id_type=MESH)
    pl.semaphore_wait(barrier, len(bits) + 3)

    units = [
        Unit(qkv_hbm, wqu, 0, (0, block_rows), (0, qkv_cols)),
        Unit(dense_hbm, wdd, 1, (0, local_width), (0, block_cols)),
        Unit(up_hbm, wqu, 0, (0, block_rows), (0, half_units), col_at=qkv_cols),
        Unit(down_hbm, wdd, 1, (0, half_units), (0, block_cols), row_at=local_width),
        Unit(up_hbm, wqu, 0, (0, block_rows), (half_units, half_units), col_at=qkv_cols + half_units),
        Unit(down_hbm, wdd, 1, (half_units, half_units), (0, block_cols),
             row_at=local_width + half_units),
    ]

    def remote_dp(src, dst, ssem, rsem, peer):
        return pltpu.make_async_remote_copy(
            src_ref=src, dst_ref=dst, send_sem=ssem, recv_sem=rsem,
            device_id={"dp": peer}, device_id_type=MESH)

    def held(order, stage):
        owners = [me]
        for bit in order[:stage]:
            owners = owners + [flip(o, bit) for o in owners]
        return owners

    def stage_copies(u, stage):
        copies = []
        for path, order in enumerate(orders):
            for q, owner in enumerate(held(order, stage)):
                slot = path * per_path + 2 ** stage - 1 + q
                dst = units[u].block(owner, path)
                src = units[u].own(path) if stage == 0 else dst
                copies.append(remote_dp(
                    src, dst, send.at[u, slot], recv.at[u, slot], flip(me, order[stage])))
        return copies

    def core_copies(u, lo=0, hi=2 ** stages):
        copies = []
        for q, owner in list(enumerate(held(bits, stages)))[lo:hi]:
            dst = units[u].block(owner)
            src = units[u].own() if q == 0 else dst
            slot = 2 * per_path + q
            copies.append(remote_dp(src, dst, send.at[u, slot], recv.at[u, slot], flip(me, 1)))
        return copies

    def own_copy(u):
        return pltpu.make_async_copy(units[u].own(), units[u].block(me), local.at[u])

    def start(u):
        own_copy(u).start()
        for c in stage_copies(u, 0):
            c.start()
        core_copies(u, 0, 1)[0].start()

    def advance(u, stage):
        if stage == 1:
            own_copy(u).wait()
        for c in stage_copies(u, stage - 1):
            c.wait_recv()
        for c in stage_copies(u, stage) if stage < stages else core_copies(u, 1):
            c.start()

    def finish(u):
        for c in core_copies(u):
            c.wait_recv()

    def drain(u):
        for stage in range(stages):
            for c in stage_copies(u, stage):
                c.wait_send()
        for c in core_copies(u):
            c.wait_send()

    x_at = acts.at[:, pl.ds(act_at, width)]

    def x_copy():
        return pltpu.make_async_copy(x_hbm, x_at, local.at[len(units)])

    cot_copy = pltpu.make_async_copy(cot_hbm, cot, local.at[len(units) + 1])
    x_copy().start()
    cot_copy.start()

    def vec_slot(i):
        return vec_in.at[aligned(i * 8, 8), :]

    def vector_copies(i):
        copies = []
        for q, owner in enumerate(held(bits + [1], i)):
            slot = 2 ** i - 1 + q
            copies.append(remote_dp(
                small_ref if q == 0 else vec_slot(owner), vec_slot(owner),
                vsend.at[slot], vrecv.at[slot], flip(me, (bits + [1])[i])))
        return copies

    vec_slot(me)[...] = small_ref[...]
    for i in range(stages + 1):
        for c in vector_copies(i):
            c.start()
        if i == 0:
            start(0)
            start(1)
        for c in vector_copies(i):
            c.wait_recv()
    total = vec_slot(0)[...]
    for owner in range(1, count):
        total = total + vec_slot(owner)[...]
    vec_ref[...] = total

    sums_ref[...] = jnp.zeros_like(sums_ref)
    x_copy().wait()
    cot_copy.wait()

    def normalised(at):
        wide = acts[at, pl.ds(act_at, width)].astype(F32)
        mean = jnp.mean(wide, axis=1, keepdims=True)
        centred = wide - mean
        var = jnp.mean(centred * centred, axis=1, keepdims=True)
        inv = lax.rsqrt(var + EPSILON)
        return centred * inv, inv

    def norm_step(i, total):
        at = aligned(i * NORM_ROWS, NORM_ROWS)
        normed, _ = normalised(at)
        low[at, :] = (normed * vec_ref[0:1, :] + vec_ref[1:2, :]).astype(BF16)
        sums_ref[2:3, :] += jnp.sum(cot[at, :].astype(F32), axis=0, keepdims=True)
        return total

    lax.fori_loop(0, rows // NORM_ROWS, norm_step, 0)

    advance(0, 1)
    start(2)
    advance(1, 1)
    start(3)
    for stage in range(2, stages + 1):
        advance(0, stage)
    finish(0)

    half = ROT // 2

    def lane_is_leading(shape):
        lane = lax.broadcasted_iota(jnp.int32, shape, 1)
        return (lane % HEAD) < half

    def swap(t):
        size = t.shape[1]
        return jnp.where(
            lane_is_leading(t.shape), pltpu.roll(t, size - half, 1), pltpu.roll(t, half, 1))

    def qkv_step(i, carry):
        @pl.when(i == 1)
        def _():
            advance(2, 1)
            start(4)

        @pl.when(i == 6)
        def _():
            for stage in range(2, stages + 1):
                advance(1, stage)

        tile = i // row_tiles
        at = aligned((i % row_tiles) * ROW_TILE, ROW_TILE)
        cols = aligned(tile * COL_TILE, COL_TILE)
        t = dot(low[at, :], wqu[:, cols]) + vec_ref[3:4, cols]
        wide = lambda r: jnp.concatenate([r[at, :]] * (COL_TILE // LANES), axis=1)
        rotated = t * wide(cos_ref) + swap(t) * wide(sin_ref)
        is_value = tile >= 2 * local_width // COL_TILE
        acts[at, cols] = jnp.where(is_value, t, rotated).astype(BF16)
        return carry

    lax.fori_loop(0, row_tiles * qkv_cols // COL_TILE, qkv_step, 0)
    advance(3, 1)
    start(5)
    finish(1)

    def mixed_step(i, carry):
        at = aligned((i % row_tiles) * ROW_TILE, ROW_TILE)
        tile = i // row_tiles
        g = dot(cot[at, :], wdd[aligned(tile * COL_TILE, COL_TILE), :], 1, 1).astype(BF16)
        for j in range(COL_TILE // LANES):
            part[tile * (COL_TILE // LANES) + j, at, :] = g[:, j * LANES : (j + 1) * LANES]
        return carry

    lax.fori_loop(0, row_tiles * local_width // COL_TILE, mixed_step, 0)
    pairs = local_width // LANES

    def attention_step(i, carry):
        s, p = i // pairs, i % pairs
        at = aligned(s * SEQ, SEQ)
        lanes = [aligned(j * local_width + p * LANES, LANES) for j in range(3)]

        @pl.when(i == 3)
        def _():
            for stage in range(2, stages + 1):
                advance(2, stage)

        @pl.when(i == 5)
        def _():
            advance(4, 1)

        @pl.when(p == 0)
        def _():
            across = lax.broadcasted_iota(jnp.int32, (SEQ, SEQ), 1)
            down = lax.broadcasted_iota(jnp.int32, (SEQ, SEQ), 0)
            row = seg_ref[s]
            column = jnp.transpose(jnp.broadcast_to(row, (LANES, SEQ)))[:, 0:1]
            allowed = (column == row) & (down >= across)
            mask[...] = jnp.where(allowed, 0.0, NEGATIVE)

        q, k, v = [acts[at, l] for l in lanes]
        go = part[p, at, :]
        lane = lax.broadcasted_iota(jnp.int32, (SEQ, LANES), 1)
        zero = jnp.zeros((), BF16)
        total = None
        for h in range(LANES // HEAD):
            mine = (lane // HEAD) == h
            kh, vh, qh, gh = [jnp.where(mine, t, zero) for t in (k, v, q, go)]
            by_row, by_key = [], []
            for r in range(SEQ // QUERY_TILE):
                seen = (r + 1) * QUERY_TILE
                here = slice(r * QUERY_TILE, seen)
                scores = dot(q[here], kh[:seen], 1, 1) * SCALE + mask[here, :seen]
                top = jnp.max(scores, axis=1, keepdims=True)
                e = jnp.exp(scores - top)
                probs = e / jnp.sum(e, axis=1, keepdims=True)
                probs_low = probs.astype(BF16)
                gprobs = dot(go[here], vh[:seen], 1, 1)
                delta = jnp.sum(probs * gprobs, axis=1, keepdims=True)
                gs = (probs * (gprobs - delta) * SCALE).astype(BF16)
                by_row.append((dot(probs_low, vh[:seen]), dot(gs, kh[:seen])))
                keyed = (dot(gs, qh[here], 0, 0), dot(probs_low, gh[here], 0, 0))
                if by_key:
                    keyed = tuple(
                        jnp.concatenate([old + new[: old.shape[0]], new[old.shape[0] :]], axis=0)
                        for old, new in zip(by_key, keyed))
                by_key = keyed
            terms = [jnp.concatenate(t, axis=0) for t in zip(*by_row)] + list(by_key)
            total = terms if total is None else [a + b for a, b in zip(total, terms)]
        acts[at, aligned(mix_at + p * LANES, LANES)] = total[0].astype(BF16)

        def back(t):
            return t * cos_ref[at, :] - swap(t) * sin_ref[at, :]

        for j, g in enumerate((back(total[1]), back(total[2]), total[3])):
            acts[at, lanes[j]] = g.astype(BF16)
            sums_ref[4:5, lanes[j]] += jnp.sum(g, axis=0, keepdims=True)
        return carry

    lax.fori_loop(0, (rows // SEQ) * pairs, attention_step, 0)
    for stage in range(2, stages + 1):
        advance(3, stage)
    finish(2)
    finish(3)

    tiles = units_here // COL_TILE

    def ffn_step(i, carry):
        @pl.when(i == 1)
        def _():
            advance(5, 1)

        @pl.when(i == row_tiles * tiles // 2 - 2)
        def _():
            for stage in range(2, stages + 1):
                advance(4, stage)

        @pl.when(i == row_tiles * tiles // 2)
        def _():
            for stage in range(2, stages + 1):
                advance(5, stage)
            finish(4)
            finish(5)

        at = aligned((i % row_tiles) * ROW_TILE, ROW_TILE)
        tile = i // row_tiles
        cols = aligned(tile * COL_TILE, COL_TILE)
        hidden = dot(low[at, :], wqu[:, aligned(qkv_cols + tile * COL_TILE, COL_TILE)])
        hidden = hidden + vec_ref[2:3, cols]
        grad = dot(cot[at, :], wdd[aligned(local_width + tile * COL_TILE, COL_TILE), :], 1, 1)
        square = hidden * hidden
        th = jnp.tanh(GELU_A * hidden * (1.0 + GELU_B * square))
        acts[at, aligned(act_at + tile * COL_TILE, COL_TILE)] = (
            0.5 * hidden * (1.0 + th)).astype(BF16)
        slope = 0.5 * (1.0 + th) + 0.5 * hidden * (1.0 - th * th) * (
            GELU_A * (1.0 + 3.0 * GELU_B * square))
        grad = grad * slope
        acts[at, aligned(gh_at + tile * COL_TILE, COL_TILE)] = grad.astype(BF16)
        sums_ref[3:4, cols] += jnp.sum(grad, axis=0, keepdims=True)
        return carry

    lax.fori_loop(0, row_tiles * tiles, ffn_step, 0)
    for u in range(len(units)):
        drain(u)
    for i in range(stages + 1):
        for c in vector_copies(i):
            c.wait_send()

    chunks = width // CHUNK
    every = 2 * chunks

    def remote_z(src, dst, ssem, rsem, peer):
        return pltpu.make_async_remote_copy(
            src_ref=src, dst_ref=dst, send_sem=ssem, recv_sem=rsem,
            device_id={"tensor": peer}, device_id_type=MESH)

    def columns(c):
        return aligned((c % chunks) * CHUNK, CHUNK)

    def copy_a(c):
        return remote_z(part.at[c % chunks], inbox.at[c % SLOTS], a_send.at[c % SLOTS],
                        a_recv.at[c % SLOTS], flip(level, 1))

    def copy_b(c):
        return remote_z(part.at[c % chunks], cross.at[c % SLOTS], b_send.at[c % SLOTS],
                        b_recv.at[c % SLOTS], depth - 1 - level)

    def copy_c_out(c):
        return remote_z(cross.at[c % SLOTS], inbox.at[c % SLOTS], c_send.at[c % SLOTS],
                        c_recv.at[c % SLOTS], flip(level, 1))

    def copy_c_grad(c):
        return remote_z(gn.at[:, columns(c)], gn.at[:, columns(c)], c_send.at[c % SLOTS],
                        c_recv.at[c % SLOTS], flip(level, 1))

    def out_copy(src, c):
        return pltpu.make_async_copy(src.at[c % SLOTS], block_out.at[:, columns(c)],
                                     z_out.at[c % SLOTS])

    gn_copy = pltpu.make_async_copy(x_hbm, gn, local.at[len(units) + 2])

    @pl.when(inner)
    def _():
        gn_copy.start()
        gn_copy.wait()

    add_rows = 256

    def by_rows(step):
        def body(i, carry):
            step(aligned(i * add_rows, add_rows))
            return carry
        lax.fori_loop(0, rows // add_rows, body, 0)

    def tick(k):
        @pl.when(inner & (k < every))
        def _():
            copy_a(k).wait_recv()

            def add(at):
                part[k % chunks, at, :] = (
                    part[k % chunks, at, :].astype(F32) + inbox[k % SLOTS, at, :].astype(F32)
                ).astype(BF16)

            by_rows(add)

            @pl.when(k >= SLOTS)
            def _():
                pl.semaphore_wait(credit, 1)

            copy_b(k).start()

        @pl.when(inner & (k >= 2) & (k < every + 2))
        def _():
            j = k - 2
            copy_b(j).wait_recv()
            copy_b(j).wait_send()

            @pl.when(j < chunks)
            def _():
                def add(at):
                    pair = part[j % chunks, at, :].astype(F32) + cross[j % SLOTS, at, :].astype(F32)
                    shifts = vec_ref[5:6, columns(j)], vec_ref[6:7, columns(j)]
                    wide = gn[at, columns(j)].astype(F32)
                    cross[j % SLOTS, at, :] = (wide + pair + shifts[0] + shifts[1]).astype(BF16)

                by_rows(add)
                copy_c_out(j).start()
                out_copy(cross, j).start()

            @pl.when(j >= chunks)
            def _():
                def add(at):
                    gn[at, columns(j)] = (
                        part[j % chunks, at, :].astype(F32) + cross[j % SLOTS, at, :].astype(F32)
                    ).astype(BF16)

                by_rows(add)
                copy_c_grad(j).start()

        @pl.when(inner & (k >= 4) & (k < every + 4))
        def _():
            i = k - 4

            @pl.when(i < chunks)
            def _():
                copy_c_out(i).wait_send()
                out_copy(cross, i).wait()

            @pl.when(i >= chunks)
            def _():
                copy_c_grad(i).wait_send()

            @pl.when(i < every - SLOTS)
            def _():
                pl.semaphore_signal(
                    credit, inc=1, device_id={"tensor": depth - 1 - level}, device_id_type=MESH)

        @pl.when(outer & (k >= 4) & (k < every + 4))
        def _():
            i = k - 4
            copy_a(i).wait_send()

            @pl.when(i < chunks)
            def _():
                copy_c_out(i).wait_recv()
                out_copy(inbox, i).start()
                out_copy(inbox, i).wait()

            @pl.when(i >= chunks)
            def _():
                copy_c_grad(i).wait_recv()

            @pl.when(i + SLOTS < every)
            def _():
                copy_a(i + SLOTS).start()

    def ticks(lo, hi):
        def body(k, carry):
            tick(k)
            return carry
        lax.fori_loop(lo, hi, body, 0)

    def produce(first, tile, r, t):
        at = aligned(r * ROW_TILE, ROW_TILE)
        for j in range(COL_TILE // CHUNK):
            part[(first + tile * (COL_TILE // CHUNK) + j) % chunks, at, :] = (
                t[:, j * CHUNK : (j + 1) * CHUNK].astype(BF16))

    per_tile = COL_TILE // CHUNK

    def branch_step(i, carry):
        tile, r = i // row_tiles, i % row_tiles
        at = aligned(r * ROW_TILE, ROW_TILE)
        cols = aligned(tile * COL_TILE, COL_TILE)
        produce(0, tile, r, dot(acts[at, pl.ds(mix_at, local_width + units_here)], wdd[:, cols]))

        @pl.when(r == row_tiles - 1)
        def _():
            for j in range(per_tile):
                @pl.when(outer & (tile * per_tile + j < SLOTS))
                def _():
                    copy_a(tile * per_tile + j).start()

            @pl.when(tile % 2 == 1)
            def _():
                tick(tile // 2)

        return carry

    lax.fori_loop(0, row_tiles * width // COL_TILE, branch_step, 0)
    done_ticks = width // COL_TILE // 2

    grad_tiles = acts.shape[1] // GRAD_TILE
    low_tiles = mix_at // GRAD_TILE
    across = width // GRAD_TILE
    blocks = 2 ** stages
    staged = wdd.shape[0] // block_rows * across // grad_tiles * grad_tiles

    def stage_at(k, p=None):
        start, size = (0, block_rows) if p is None else (p * (block_rows // 2), block_rows // 2)
        at = aligned((k // across) * block_rows + start, size)
        return wdd.at[at, aligned((k % across) * GRAD_TILE, GRAD_TILE)]

    def relative(base, v):
        for i, bit in enumerate(bits):
            has = (v // 2 ** (stages - 1 - i)) % 2
            base = base + has * (bit - 2 * bit * ((base // bit) % 2))
        return base

    def turn(block):
        cols = aligned(block * block_rows, block_rows)
        turned[0] = jnp.transpose(low[:, cols])
        turned[1] = jnp.transpose(cot[:, cols])

    def grad_tile(n):
        return dot(turned[n // low_tiles], acts[:, aligned(n * GRAD_TILE, GRAD_TILE)])

    def core_copy(i):
        return remote_dp(stage_at(i % staged), core_rx.at[i], core_send.at[i % staged],
                         core_recv.at[i], flip(me, 1))

    def other_step(i, carry):
        n = i % grad_tiles

        @pl.when(n == 0)
        def _():
            turn(relative(flip(me, 1), blocks - 1 - i // grad_tiles))

        @pl.when(i >= staged)
        def _():
            core_copy(i - staged).wait_send()

        stage_at(i % staged)[...] = grad_tile(n).astype(BF16)
        core_copy(i).start()

        @pl.when(n == grad_tiles - 1)
        def _():
            tick(done_ticks + i // grad_tiles)

        return carry

    lax.fori_loop(0, blocks * grad_tiles, other_step, 0)
    done_ticks += blocks

    def first_bit(v, order):
        for s, bit in enumerate(order):
            if v // 2 ** (stages - 1 - bits.index(bit)) % 2:
                return s
        return len(order)

    pieces = {}
    for v in range(blocks):
        for p, order in enumerate(orders):
            for s in range(first_bit(v, order)):
                pieces[(v, p, s)] = len(pieces)
    spare = staged

    def link_copy(v, p, n):
        order = orders[p]
        s = first_bit(v, order)
        left = v - 2 ** (stages - 1 - bits.index(order[s]))
        piece = pieces[(left, p, s)]
        return remote_dp(
            stage_at((blocks - 1 - v) * grad_tiles + n, p), link_rx.at[piece, n],
            link_send.at[2 * (v - 1) + p, n], link_recv.at[piece, n], flip(me, order[s]))

    def arrival(v, p, s, n):
        piece = pieces[(v, p, s)]
        return remote_dp(
            stage_at(0, p), link_rx.at[piece, n], link_send.at[0, 0], link_recv.at[piece, n],
            flip(me, orders[p][s]))

    def own_block(v):
        q = blocks - 1 - v
        mine = [key for key in pieces if key[0] == v]

        def core_fetch(n):
            return pltpu.make_async_copy(
                core_rx.at[q * grad_tiles + n], stage_at(spare + n % 2), fetch_sem.at[n % 2, 0])

        def slot(s, n):
            return (n % 2) * stages + s if v == 0 else spare + 2 + n % 2

        def piece_fetch(key, n):
            _, p, s = key
            return pltpu.make_async_copy(
                link_rx.at[pieces[key], n], stage_at(slot(s, n), p),
                fetch_sem.at[n % 2, 1 + mine.index(key)])

        def fetch(n):
            core_copy(q * grad_tiles + n).wait_recv()
            core_fetch(n).start()
            for key in mine:
                arrival(*key, n).wait_recv()
                piece_fetch(key, n).start()

        def grad_out(n):
            at = aligned((n % 2) * block_rows, block_rows)
            flat, tall = mask.at[at, :], mask.at[:, at]
            sem = grad_sem.at[n % 2]
            first = qkv_cols // GRAD_TILE
            last = low_tiles + local_width // GRAD_TILE
            cases = (
                (n < first, flat, lambda: qkv_out.at[:, aligned(n * GRAD_TILE, GRAD_TILE)]),
                ((n >= first) & (n < low_tiles), flat,
                 lambda: up_out.at[:, aligned((n - first) * GRAD_TILE, GRAD_TILE)]),
                ((n >= low_tiles) & (n < last), tall,
                 lambda: dense_out.at[aligned((n - low_tiles) * GRAD_TILE, GRAD_TILE), :]),
                (n >= last, tall,
                 lambda: down_out.at[aligned((n - last) * GRAD_TILE, GRAD_TILE), :]),
            )
            return [(c, pltpu.make_async_copy(src, dst(), sem)) for c, src, dst in cases]

        def for_out(n, act):
            for cond, copy in grad_out(n):
                @pl.when(cond)
                def _():
                    act(copy)

        turn(relative(me, v))
        if v == 0:
            for n in range(2 * stages):
                for p in range(2):
                    link_copy(blocks - 1, p, n).wait_send()
        fetch(0)

        def step(n, carry):
            t = grad_tile(n)
            core_fetch(n).wait()
            t = t + stage_at(spare + n % 2)[...].astype(F32)
            for key in mine:
                piece_fetch(key, n).wait()
            for s in sorted({key[2] for key in mine}):
                sides = []
                for p in range(2):
                    rows_p = slice(p * (block_rows // 2), (p + 1) * (block_rows // 2))
                    side = t[rows_p]
                    if (v, p, s) in pieces:
                        side = side + stage_at(slot(s, n), p)[...].astype(F32)
                    sides.append(side)
                t = jnp.concatenate(sides, axis=0)
            if v:
                k = (blocks - 1 - v) * grad_tiles + n
                core_copy(k if v < blocks - 1 else k + staged).wait_send()
                stage_at(k)[...] = t.astype(BF16)
                for p in range(2):
                    link_copy(v, p, n).start()
            else:
                @pl.when((n >= 2) & (n != low_tiles + 1))
                def _():
                    for_out(n - 2, lambda c: c.wait())

                @pl.when(n == low_tiles)
                def _():
                    for_out(n - 1, lambda c: c.wait())

                @pl.when(n < low_tiles)
                def _():
                    mask[aligned((n % 2) * block_rows, block_rows), :] = t

                @pl.when(n >= low_tiles)
                def _():
                    mask[:, aligned((n % 2) * block_rows, block_rows)] = jnp.transpose(t)

                for_out(n, lambda c: c.start())

            @pl.when(n + 1 < grad_tiles)
            def _():
                fetch(n + 1)

            return carry

        lax.fori_loop(0, grad_tiles, step, 0)
        if v == 0:
            for n in (grad_tiles - 2, grad_tiles - 1):
                for cond, copy in grad_out(n):
                    if bool(cond):
                        copy.wait()

    own_block(blocks - 1)
    ticks(done_ticks, done_ticks + 1)
    done_ticks += 1
    before = done_ticks
    lag = SLOTS - 2 - per_tile

    def grad_step(i, carry):
        tile, r = i // row_tiles, i % row_tiles

        @pl.when(r == 0)
        def _():
            ticks(
                jnp.maximum(before, lag + per_tile * tile),
                jnp.maximum(before, lag + per_tile * (tile + 1)),
            )

            for v in range(1, blocks - 1):
                @pl.when(tile == width // COL_TILE // 2 + blocks - 2 - v)
                def _():
                    own_block(v)

        at = aligned(r * ROW_TILE, ROW_TILE)
        t = dot(acts[at, pl.ds(0, mix_at)], wqu[aligned(tile * COL_TILE, COL_TILE), :], 1, 1)
        produce(chunks, tile, r, t)
        return carry

    lax.fori_loop(0, row_tiles * width // COL_TILE, grad_step, 0)
    done_ticks = lag + per_tile * (width // COL_TILE)
    last_block = every - 4

    ticks(done_ticks, last_block)
    own_block(0)
    x_copy().start()
    ticks(last_block, every + 4)
    for v in range(1, blocks):
        for p in range(2):
            for n in range(grad_tiles):
                if v == blocks - 1 and n < 2 * stages:
                    continue
                link_copy(v, p, n).wait_send()
    x_copy().wait()

    def row_slot(i):
        return vec_in.at[aligned((i % 2) * BACK_ROWS, BACK_ROWS), :]

    def row_copy(i):
        return pltpu.make_async_copy(
            row_slot(i), input_grad.at[aligned(i * BACK_ROWS, BACK_ROWS), :], row_sem.at[i % 2])

    def back_step(i, carry):
        at = aligned(i * BACK_ROWS, BACK_ROWS)
        normed, inv = normalised(at)
        g = gn[at, :].astype(F32)
        product = g * normed
        sums_ref[0:1, :] += jnp.sum(product, axis=0, keepdims=True)
        sums_ref[1:2, :] += jnp.sum(g, axis=0, keepdims=True)
        gain = vec_ref[0:1, :]
        scaled = g * gain
        first = jnp.mean(scaled, axis=1, keepdims=True)
        second = jnp.mean(product * gain, axis=1, keepdims=True)

        @pl.when(i >= 2)
        def _():
            row_copy(i - 2).wait()

        row_slot(i)[...] = inv * (scaled - first - normed * second) + cot[at, :].astype(F32)
        row_copy(i).start()
        return carry

    norm_steps = rows // BACK_ROWS
    lax.fori_loop(0, norm_steps, back_step, 0)

    row_copy(norm_steps - 2).wait()
    row_copy(norm_steps - 1).wait()

    first_slot = 2 * BACK_ROWS // 8

    def sum_copy(i, bit):
        return remote_dp(sums_ref, vec_slot(first_slot + i), sum_send.at[i], sum_recv.at[i],
                         flip(me, bit))

    for i, bit in enumerate(bits + [1]):
        copy = sum_copy(i, bit)
        copy.start()
        copy.wait()
        sums_ref[...] = sums_ref[...] + vec_slot(first_slot + i)[...]


def fits(shards, depth, local_width, block_cols):
    return (
        shards & (shards - 1) == 0 and len(link_bits(shards)) == 2 and depth == 4
        and block_cols % COL_TILE == 0 and local_width % GRAD_TILE == 0
    )


def layer(x, cot, qkv_share, dense_share, up_share, down_share, small, tables, segments):
    rows, width = x.shape
    count = lax.axis_size("dp")
    local_width = dense_share.shape[0]
    units_here = up_share.shape[1]
    block_rows = up_share.shape[0]
    seqs = rows // SEQ
    links = len(link_bits(count))
    blocks = 2 ** links
    slots = 2 * (blocks - 1) + blocks
    acts_cols = 4 * local_width + 2 * units_here
    grad_tiles = acts_cols // GRAD_TILE
    pieces = 0
    for order in range(2):
        pieces += sum(blocks // 2 ** (s + 1) for s in range(links))
    staged = (local_width + units_here) // block_rows * (width // GRAD_TILE) // grad_tiles * grad_tiles
    chunks = width // CHUNK
    any_ = pl.BlockSpec(memory_space=pl.ANY)
    vmem = pl.BlockSpec(memory_space=pltpu.VMEM)
    b16 = lambda *s: jax.ShapeDtypeStruct(s, BF16)
    f32 = lambda *s: jax.ShapeDtypeStruct(s, F32)
    dma = lambda *s: pltpu.SemaphoreType.DMA(s)
    outs = pl.pallas_call(
        layer_body,
        in_specs=[any_] * 6 + [vmem] * 4,
        out_specs=[any_] * 8 + [vmem],
        out_shape=[
            b16(rows, width), f32(rows, width), f32(block_rows, 3 * local_width),
            f32(local_width, block_rows), f32(block_rows, units_here), f32(units_here, block_rows),
            b16(blocks * grad_tiles, block_rows, GRAD_TILE),
            b16(pieces, grad_tiles, block_rows // 2, GRAD_TILE), f32(8, width),
        ],
        scratch_shapes=[
            pltpu.VMEM((width, 3 * local_width + units_here), BF16),
            pltpu.VMEM((local_width + units_here, width), BF16),
            pltpu.VMEM((rows, acts_cols), BF16), pltpu.VMEM((rows, width), BF16),
            pltpu.VMEM((rows, width), BF16), pltpu.VMEM((SEQ, SEQ), F32),
            pltpu.VMEM((8, width), F32), pltpu.VMEM((8 * count, width), F32),
            pltpu.VMEM((2, block_rows, rows), BF16), pltpu.VMEM((rows, width), BF16),
            pltpu.VMEM((chunks, rows, CHUNK), BF16), pltpu.VMEM((SLOTS, rows, CHUNK), BF16),
            pltpu.VMEM((SLOTS, rows, CHUNK), BF16),
            dma(6, slots), dma(6, slots), dma(count - 1), dma(count - 1), dma(9),
            dma(SLOTS), dma(SLOTS), dma(SLOTS), dma(SLOTS), dma(SLOTS), dma(SLOTS), dma(SLOTS),
            pltpu.SemaphoreType.REGULAR,
            dma(staged), dma(blocks * grad_tiles), dma(2 * (blocks - 1), grad_tiles),
            dma(pieces, grad_tiles), dma(2, 1 + 2 * links), dma(2), dma(2),
            dma(links + 1), dma(links + 1),
        ],
        compiler_params=pltpu.CompilerParams(
            collective_id=0, has_side_effects=True, vmem_limit_bytes=67_043_328),
        cost_estimate=pl.CostEstimate(
            flops=18 * rows * width * (local_width + units_here), bytes_accessed=80_000_000,
            transcendentals=rows * units_here),
        name="layer",
    )(
        x, cot, qkv_share, dense_share, up_share, down_share, small, *tables,
        segments.astype(F32).reshape(seqs, 1, SEQ),
    )
    return outs[:6] + outs[8:]


def gelu_tanh(inputs):
    return jax.nn.gelu(inputs, approximate=True)


def line_sum(part, finish):
    size = lax.axis_size("tensor")
    if size != 4:
        return finish(lax.psum(part, "tensor").astype(F32))
    index = lax.axis_index("tensor")
    inward = lax.ppermute(part, "tensor", [(0, 1), (3, 2)])
    pair = (part.astype(F32) + inward.astype(F32)).astype(BF16)
    other = lax.ppermute(pair, "tensor", [(1, 2), (2, 1)])
    done = finish(pair.astype(F32) + other.astype(F32))
    back = lax.ppermute(done, "tensor", [(1, 0), (2, 3)])
    return jnp.where((index == 0) | (index == size - 1), back, done)


def local(
    block_input, segments, norm_gain, norm_bias, qkv_weight, query_value_bias, key_bias,
    dense_weight, dense_bias, up_weight, up_bias, down_weight, down_bias, cotangent,
):
    rows, width = block_input.shape
    local_width = qkv_weight.shape[2]
    heads = local_width // HEAD
    seqs = rows // SEQ
    shards = lax.axis_size("dp")
    tables = rotary_tables(segments)
    fused = fits(shards, lax.axis_size("tensor"), local_width, down_weight.shape[1])
    if fused:
        mine = lax.axis_index("dp")

        def spread(value):
            owner = lax.broadcasted_iota(jnp.int32, (1, shards, 1), 1)
            return jnp.where(owner == mine, value[:, None, :], 0.0).reshape(1, -1)

        wide_small = [t.astype(F32) for t in (
            norm_gain, norm_bias, up_bias, query_value_bias, key_bias, dense_bias, down_bias)]
        key_row = spread(wide_small[4]).reshape(heads, ROT)
        key_row = jnp.concatenate([key_row, jnp.zeros((heads, HEAD - ROT), F32)], axis=1)
        qkv_row = jnp.concatenate(
            [spread(wide_small[3][0]), key_row.reshape(1, -1), spread(wide_small[3][1]),
             jnp.zeros((1, width - 3 * local_width), F32)], axis=1)
        small = jnp.concatenate(
            [spread(wide_small[0][None]), spread(wide_small[1][None]), spread(wide_small[2]),
             qkv_row, jnp.zeros((1, width), F32), spread(wide_small[5][None]),
             spread(wide_small[6][None]), jnp.zeros((1, width), F32)], axis=0)
        cosine, leading, trailing = tables
        block_output, input_grad, qkv_out, dense_out, up_out, down_out, total = layer(
            block_input, cotangent, qkv_weight.reshape(qkv_weight.shape[0], -1), dense_weight,
            up_weight, down_weight, small, (cosine, leading + trailing), segments)

        def mine_of(value, lead):
            return lax.dynamic_index_in_dim(
                value.reshape(lead, shards, -1), mine, axis=1, keepdims=False)

        sums = total[4]
        qv_sums = jnp.stack([sums[:local_width], sums[2 * local_width : 3 * local_width]])
        key_sums = sums[local_width : 2 * local_width].reshape(heads, HEAD)[:, :ROT]
        bias_out = mine_of(total[2], 1).reshape(-1)
        return (
            block_output, input_grad, mine_of(total[0], 1).reshape(-1),
            mine_of(total[1], 1).reshape(-1), qkv_out.reshape(qkv_weight.shape),
            mine_of(qv_sums, 2 * heads).reshape(query_value_bias.shape),
            mine_of(key_sums, heads), dense_out, bias_out, up_out,
            mine_of(total[3], up_bias.shape[0]), down_out, bias_out,
        )
    smalls = (norm_gain, norm_bias, dense_bias, down_bias, up_bias, query_value_bias, key_bias)
    packed = jnp.concatenate([s.reshape(1, -1) for s in smalls], axis=1)
    packed = lax.all_gather(packed, "dp", axis=0, tiled=True)
    pieces = []
    at = 0
    for s in smalls:
        pieces.append(packed[:, at : at + s.size].reshape((shards,) + s.shape).astype(F32))
        at += s.size
    gain, shift, dense_shift, down_shift = [p.reshape(1, -1) for p in pieces[:4]]
    up_shift = pieces[4].transpose(1, 0, 2).reshape(1, -1)
    qv_bias = pieces[5].transpose(1, 2, 0, 3).reshape(2, local_width)
    key_part = pieces[6].transpose(1, 0, 2).reshape(heads, ROT)
    key_full = jnp.concatenate([key_part, jnp.zeros((heads, HEAD - ROT), F32)], axis=1)
    bias = jnp.concatenate(
        [qv_bias[0:1], key_full.reshape(1, -1), qv_bias[1:2], jnp.zeros((5, local_width), F32)], axis=0
    )

    dense_all = lax.all_gather(dense_weight, "dp", axis=1, tiled=True)
    qkv_all = lax.all_gather(qkv_weight.reshape(qkv_weight.shape[0], -1), "dp", axis=0, tiled=True)
    up_all = lax.all_gather(up_weight, "dp", axis=0, tiled=True)
    down_all = lax.all_gather(down_weight, "dp", axis=1, tiled=True)

    wide = block_input.astype(F32)
    mean = jnp.mean(wide, axis=1, keepdims=True)
    centred = wide - mean
    inv_std = lax.rsqrt(jnp.mean(centred * centred, axis=1, keepdims=True) + EPSILON)
    normed = centred * inv_std
    low = (normed * gain + shift).astype(BF16)

    grad_mixed = dot(cotangent, dense_all, 1, 1).astype(BF16)
    projected = dot(low, qkv_all)
    mixed, grad_projected, bias_sums = attention(projected, grad_mixed, bias, tables, segments)
    bias_sums = jnp.sum(bias_sums, axis=0)

    hidden = dot(low, up_all) + up_shift
    activated, gelu_back = jax.vjp(gelu_tanh, hidden)
    activated = activated.astype(BF16)
    grad_hidden = gelu_back(dot(cotangent, down_all, 1, 1))[0]
    grad_up_bias = jnp.sum(grad_hidden, axis=0)
    grad_hidden_low = grad_hidden.astype(BF16)
    grad_joined = jnp.concatenate([grad_projected[i] for i in range(3)], axis=1)

    branches = (dot(mixed, dense_all) + dot(activated, down_all)).astype(BF16)
    grad_part = (dot(grad_joined, qkv_all, 1, 1) + dot(grad_hidden_low, up_all, 1, 1)).astype(BF16)
    grad_dense = dot(mixed, cotangent, 0, 0).astype(BF16)
    grad_qkv = dot(low, grad_joined, 0, 0).astype(BF16)
    grad_down = dot(activated, cotangent, 0, 0).astype(BF16)
    grad_up = dot(low, grad_hidden_low, 0, 0).astype(BF16)

    outs, grads = [], []
    for s in range(seqs):
        at = slice(s * SEQ, (s + 1) * SEQ)
        outs.append(
            line_sum(
                branches[at],
                lambda t, at=at: (wide[at] + t + dense_shift + down_shift).astype(BF16),
            )
        )
    for s in range(seqs):
        at = slice(s * SEQ, (s + 1) * SEQ)
        grads.append(line_sum(grad_part[at], lambda t: t.astype(BF16)))
    block_output = jnp.concatenate(outs, axis=0)
    grad_normed = jnp.concatenate(grads, axis=0).astype(F32)

    grad_wide = cotangent.astype(F32)
    scaled = grad_normed * gain
    input_grad = (
        inv_std
        * (
            scaled
            - jnp.mean(scaled, axis=1, keepdims=True)
            - normed * jnp.mean(scaled * normed, axis=1, keepdims=True)
        )
        + grad_wide
    )

    def scatter(value, dim):
        return lax.psum_scatter(value, "dp", scatter_dimension=dim, tiled=True).astype(F32)

    qkv_out = scatter(grad_qkv, 0).reshape(qkv_weight.shape)
    dense_out = scatter(grad_dense, 1)
    up_out = scatter(grad_up, 0)
    down_out = scatter(grad_down, 1)

    key_sums = bias_sums[1].reshape(heads, HEAD)[:, :ROT]
    qv_sums = jnp.stack([bias_sums[0], bias_sums[2]]).reshape(2, heads, HEAD)
    small_sums = (
        jnp.sum(grad_normed * normed, axis=0).reshape(shards, -1),
        jnp.sum(grad_normed, axis=0).reshape(shards, -1),
        jnp.sum(grad_wide, axis=0).reshape(shards, -1),
        grad_up_bias.reshape(up_bias.shape[0], shards, -1).transpose(1, 0, 2).reshape(shards, -1),
        qv_sums.reshape(2, heads, shards, -1).transpose(2, 0, 1, 3).reshape(shards, -1),
        key_sums.reshape(heads, shards, -1).transpose(1, 0, 2).reshape(shards, -1),
    )
    total = lax.psum_scatter(
        jnp.concatenate(small_sums, axis=1), "dp", scatter_dimension=0, tiled=True
    ).reshape(-1)
    shapes = (norm_gain.shape, norm_bias.shape, dense_bias.shape, up_bias.shape,
              query_value_bias.shape, key_bias.shape)
    smalls_out = []
    at = 0
    for part, shape in zip(small_sums, shapes):
        smalls_out.append(total[at : at + part.shape[1]].reshape(shape))
        at += part.shape[1]
    gain_out, shift_out, bias_out, up_bias_out, qv_out, key_out = smalls_out
    return (
        block_output, input_grad, gain_out, shift_out, qkv_out, qv_out, key_out, dense_out,
        bias_out, up_out, up_bias_out, down_out, bias_out,
    )


def solution(mesh):
    in_specs = (
        P("dp", None),
        P("dp"),
        P("dp"),
        P("dp"),
        P("dp", None, "tensor"),
        P(None, "tensor", "dp"),
        P("tensor", "dp"),
        P("tensor", "dp"),
        P("dp"),
        P("dp", "tensor"),
        P("tensor", "dp"),
        P("tensor", "dp"),
        P("dp"),
        P("dp", None),
    )
    out_specs = (
        P("dp", None),
        P("dp", None),
        P("dp"),
        P("dp"),
        P("dp", None, "tensor"),
        P(None, "tensor", "dp"),
        P("tensor", "dp"),
        P("tensor", "dp"),
        P("dp"),
        P("dp", "tensor"),
        P("tensor", "dp"),
        P("tensor", "dp"),
        P("dp"),
    )
    return jax.shard_map(local, mesh=mesh, in_specs=in_specs, out_specs=out_specs, check_vma=False)
```

```python
import functools

import jax
import jax.numpy as jnp
import numpy as np
from jax import lax
from jax.experimental import pallas as pl
from jax.experimental.pallas import tpu as pltpu
from jax.sharding import PartitionSpec as P

HEAD = 64
ROT = 32
SEQ = 512
LANES = 128
EPSILON = 1e-05
SCALE = 0.125
NEGATIVE = -1e30

F32 = jnp.float32
BF16 = jnp.bfloat16


def dot(a, b, ca=1, cb=0):
    return lax.dot_general(a, b, (((ca,), (cb,)), ((), ())), preferred_element_type=F32)


def rotary_tables(segments):
    seg_rows = segments.reshape(-1, SEQ)
    position = jnp.arange(SEQ, dtype=jnp.int32)
    starting = jnp.concatenate(
        [jnp.ones((seg_rows.shape[0], 1), dtype=jnp.bool_), seg_rows[:, 1:] != seg_rows[:, :-1]],
        axis=1,
    )
    starts = lax.cummax(jnp.where(starting, position[None, :], jnp.int32(0)), axis=1)
    offset = (position[None, :] - starts).astype(F32).reshape(-1, 1)
    half = ROT // 2
    lane = jnp.arange(LANES, dtype=jnp.int32) % HEAD
    inverse = 10000.0 ** (-((lane % half).astype(F32) * (2.0 / ROT)))
    angles = offset * inverse[None, :]
    cosine = jnp.where(lane < ROT, jnp.cos(angles), 1.0)
    sine = jnp.sin(angles)
    return (
        cosine,
        jnp.where(lane < half, -sine, 0.0),
        jnp.where((lane >= half) & (lane < ROT), sine, 0.0),
    )


def attention_body(
    q_ref, k_ref, v_ref, go_ref, bias_ref, cos_ref, sa_ref, sb_ref, segc_ref, segr_ref,
    mixed_ref, gp_ref, gb_ref, mask_ref,
):
    half = ROT // 2

    def rotate(t, direction):
        swapped = pltpu.roll(t, LANES - half, 1) * sa_ref[...]
        swapped = swapped + pltpu.roll(t, half, 1) * sb_ref[...]
        return t * cos_ref[...] + direction * swapped

    @pl.when(pl.program_id(1) == 0)
    def _():
        rows = lax.broadcasted_iota(jnp.int32, (SEQ, SEQ), 0)
        cols = lax.broadcasted_iota(jnp.int32, (SEQ, SEQ), 1)
        allowed = (segc_ref[...] == segr_ref[0]) & (rows >= cols)
        mask_ref[...] = jnp.where(allowed, 0.0, NEGATIVE)

    q = rotate(q_ref[...] + bias_ref[0:1, :], 1.0).astype(BF16)
    k = rotate(k_ref[...] + bias_ref[1:2, :], 1.0).astype(BF16)
    v = (v_ref[...] + bias_ref[2:3, :]).astype(BF16)
    go = go_ref[...]
    lane = lax.broadcasted_iota(jnp.int32, (SEQ, LANES), 1)
    mixed = gq = gk = gv = None
    for h in range(LANES // HEAD):
        mine = (lane // HEAD) == h
        zero = jnp.zeros((), BF16)
        kh = jnp.where(mine, k, zero)
        vh = jnp.where(mine, v, zero)
        qh = jnp.where(mine, q, zero)
        gh = jnp.where(mine, go, zero)
        s = dot(q, kh, 1, 1) * SCALE + mask_ref[...]
        top = jnp.max(s, axis=1, keepdims=True)
        e = jnp.exp(s - top)
        p = e / jnp.sum(e, axis=1, keepdims=True)
        low = p.astype(BF16)
        dp = dot(go, vh, 1, 1)
        delta = jnp.sum(p * dp, axis=1, keepdims=True)
        ds = (p * (dp - delta) * SCALE).astype(BF16)
        terms = (dot(low, vh), dot(ds, kh), dot(ds, qh, 0, 0), dot(low, gh, 0, 0))
        if h == 0:
            mixed, gq, gk, gv = terms
        else:
            mixed, gq, gk, gv = [a + b for a, b in zip((mixed, gq, gk, gv), terms)]
    mixed_ref[...] = mixed.astype(BF16)
    gq = rotate(gq, -1.0)
    gk = rotate(gk, -1.0)
    for i, g in enumerate((gq, gk, gv)):
        gp_ref[i] = g.astype(BF16)
        gb_ref[0, i : i + 1, :] = jnp.sum(g, axis=0, keepdims=True)


def attention(projected, grad_mixed, bias, tables, segments):
    rows = projected.shape[0]
    width = projected.shape[1] // 3
    seqs, pairs = rows // SEQ, width // LANES
    tile = lambda f: pl.BlockSpec((SEQ, LANES), f)
    table = tile(lambda s, p: (s, 0))
    return pl.pallas_call(
        attention_body,
        grid=(seqs, pairs),
        in_specs=[
            tile(lambda s, p: (s, p)),
            tile(lambda s, p: (s, pairs + p)),
            tile(lambda s, p: (s, 2 * pairs + p)),
            tile(lambda s, p: (s, p)),
            pl.BlockSpec((8, LANES), lambda s, p: (0, p)),
            table, table, table,
            pl.BlockSpec((SEQ, 1), lambda s, p: (s, 0)),
            pl.BlockSpec((1, 1, SEQ), lambda s, p: (s, 0, 0)),
        ],
        out_specs=[
            tile(lambda s, p: (s, p)),
            pl.BlockSpec((3, SEQ, LANES), lambda s, p: (0, s, p)),
            pl.BlockSpec((1, 8, LANES), lambda s, p: (s, 0, p)),
        ],
        out_shape=[
            jax.ShapeDtypeStruct((rows, width), BF16),
            jax.ShapeDtypeStruct((3, rows, width), BF16),
            jax.ShapeDtypeStruct((seqs, 8, width), F32),
        ],
        scratch_shapes=[pltpu.VMEM((SEQ, SEQ), F32)],
        compiler_params=pltpu.CompilerParams(dimension_semantics=("arbitrary", "arbitrary")),
        cost_estimate=pl.CostEstimate(
            flops=14 * rows * SEQ * width, bytes_accessed=24 * rows * width,
            transcendentals=rows * SEQ * width // HEAD,
        ),
        name="attention",
    )(
        projected, projected, projected, grad_mixed, bias, *tables,
        segments.reshape(rows, 1), segments.reshape(seqs, 1, SEQ),
    )


ROW_TILE = 512
QUERY_TILE = 256
COL_TILE = 256
GRAD_TILE = 512
CHUNK = 128
SLOTS = 8
NORM_ROWS = 32
NORM_EVENTS = (8, 16)
BACK_ROWS = 32
PARTS = 4
DEPTH = 4
TICK_TILES = 8
GELU_A = 0.7978845608028654
GELU_B = 0.044715
MESH = pl.DeviceIdType.MESH
INVERSE = np.asarray(
    10000.0 ** (-(np.arange(LANES) % (ROT // 2)) * (2.0 / ROT)), np.float32).reshape(1, LANES)


def flip(index, bit):
    return index + bit - 2 * bit * ((index // bit) % 2)


def link_bits(count):
    bits = []
    bit = count // 2
    while bit >= 2:
        bits.append(bit)
        bit //= 2
    return bits


def aligned(start, size):
    return pl.ds(pl.multiple_of(start, size), size)


class Unit:
    def __init__(self, share, whole, axis, rows, cols, row_at=0, col_at=0):
        self.share, self.whole, self.axis = share, whole, axis
        self.row0, self.rows = rows
        self.col0, self.cols = cols
        self.row_at, self.col_at = row_at, col_at

    def span(self, half):
        return (0, self.rows) if half is None else (half * (self.rows // 2), self.rows // 2)

    def own(self, half=None):
        start, size = self.span(half)
        return self.share.at[pl.ds(self.row0 + start, size), pl.ds(self.col0, self.cols)]

    def block(self, which, half=None):
        start, size = self.span(half)
        if self.axis == 0:
            rows = aligned(which * self.rows + start, size)
            return self.whole.at[rows, pl.ds(self.col_at, self.cols)]
        cols = aligned(which * self.cols, self.cols)
        return self.whole.at[pl.ds(self.row_at + start, size), cols]


def layer_body(
    x_hbm, cot_hbm, qkv_hbm, dense_hbm, up_hbm, down_hbm, rows_ref, up_shift_ref, qv_ref, key_ref, inverse_ref, seg_ref,
    block_out, input_grad, qkv_out, dense_out, up_out, down_out, core_rx, link_rx, sums_ref,
    wqu, wdd, acts, low, cot, mask, vec_ref, vec_in, turned, gn, part, inbox, cross,
    tables, stats, spare_tiles, sum_in,
    send, recv, vsend, vrecv, local,
    a_send, a_recv, b_send, b_recv, c_send, c_recv, z_out, credit,
    core_send, core_recv, link_send, link_recv, fetch_sem, grad_sem, row_sem, sum_send, sum_recv,
):
    count = lax.axis_size("dp")
    me = lax.axis_index("dp")
    depth = lax.axis_size("tensor")
    level = lax.axis_index("tensor")
    outer = (level == 0) | (level == depth - 1)
    inner = jnp.logical_not(outer)
    bits = link_bits(count)
    orders = (bits, bits[::-1])
    stages = len(bits)
    per_path = 2 ** stages - 1
    rows, width = low.shape
    units_here = up_hbm.shape[1]
    local_width = dense_hbm.shape[0]
    qkv_cols = 3 * local_width
    part_units = units_here // PARTS
    block_rows = up_hbm.shape[0]
    block_cols = down_hbm.shape[1]
    gh_at = qkv_cols
    mix_at = qkv_cols + units_here
    act_at = mix_at + local_width
    row_tiles = rows // ROW_TILE

    barrier = pltpu.get_barrier_semaphore()
    for bit in bits + [1]:
        pl.semaphore_signal(barrier, inc=1, device_id={"dp": flip(me, bit)}, device_id_type=MESH)
    for other in (flip(level, 1), depth - 1 - level):
        pl.semaphore_signal(barrier, inc=1, device_id={"tensor": other}, device_id_type=MESH)
    pl.semaphore_wait(barrier, len(bits) + 3)

    units = [
        Unit(None, wqu, 0, (0, block_rows), (0, qkv_cols)),
        Unit(dense_hbm, wdd, 1, (0, local_width), (0, block_cols)),
    ]
    for q in range(PARTS):
        at = q * part_units
        units.append(Unit(up_hbm, wqu, 0, (0, block_rows), (at, part_units), col_at=qkv_cols + at))
        units.append(Unit(down_hbm, wdd, 1, (at, part_units), (0, block_cols),
                          row_at=local_width + at))

    def remote_dp(src, dst, ssem, rsem, peer):
        return pltpu.make_async_remote_copy(
            src_ref=src, dst_ref=dst, send_sem=ssem, recv_sem=rsem,
            device_id={"dp": peer}, device_id_type=MESH)

    def held(order, stage):
        owners = [me]
        for bit in order[:stage]:
            owners = owners + [flip(o, bit) for o in owners]
        return owners

    def stage_copies(u, stage):
        copies = []
        for path, order in enumerate(orders):
            for q, owner in enumerate(held(order, stage)):
                slot = path * per_path + 2 ** stage - 1 + q
                dst = units[u].block(owner, path)
                src = units[u].own(path) if stage == 0 and u else dst
                copies.append(remote_dp(
                    src, dst, send.at[u, slot], recv.at[u, slot], flip(me, order[stage])))
        return copies

    def core_copies(u, lo=0, hi=2 ** stages):
        copies = []
        for q, owner in list(enumerate(held(bits, stages)))[lo:hi]:
            dst = units[u].block(owner)
            src = units[u].own() if q == 0 and u else dst
            slot = 2 * per_path + q
            copies.append(remote_dp(src, dst, send.at[u, slot], recv.at[u, slot], flip(me, 1)))
        return copies

    def own_copies(u):
        if u:
            return [pltpu.make_async_copy(units[u].own(), units[u].block(me), local.at[u])]
        at = aligned(me * block_rows, block_rows)
        sems = [local.at[0], local.at[len(units) + 3], local.at[len(units) + 4]]
        return [
            pltpu.make_async_copy(
                qkv_hbm.at[j], wqu.at[at, pl.ds(j * local_width, local_width)], sems[j])
            for j in range(3)
        ]

    def start(u):
        for c in own_copies(u):
            c.start()
        if u == 0:
            for c in own_copies(u):
                c.wait()
        for c in stage_copies(u, 0):
            c.start()
        core_copies(u, 0, 1)[0].start()

    def advance(u, stage):
        if stage == 1 and u:
            for c in own_copies(u):
                c.wait()
        for c in stage_copies(u, stage - 1):
            c.wait_recv()
        for c in stage_copies(u, stage) if stage < stages else core_copies(u, 1):
            c.start()

    order_of_events = [(0, 1), (1, 1)]
    for u in range(len(units)):
        order_of_events.append((u, 2))
        if u + 2 < len(units):
            order_of_events.append((u + 2, 1))

    def event(e):
        u, stage = order_of_events[e]
        if stage == 1:
            advance(u, 1)
            if u + 2 < len(units):
                start(u + 2)
        else:
            for later in range(2, stages + 1):
                advance(u, later)

    def events_at(i, table):
        for when, which in table:
            @pl.when(i == when)
            def _():
                for e in which:
                    event(e)

    def finish(u):
        for c in core_copies(u):
            c.wait_recv()

    def drain(u):
        for stage in range(stages):
            for c in stage_copies(u, stage):
                c.wait_send()
        for c in core_copies(u):
            c.wait_send()

    x_at = acts.at[:, pl.ds(act_at, width)]

    def x_copy():
        return pltpu.make_async_copy(x_hbm, x_at, local.at[len(units)])

    cot_copy = pltpu.make_async_copy(cot_hbm, cot, local.at[len(units) + 1])
    x_copy().start()
    cot_copy.start()

    def vec_slot(i):
        return vec_in.at[aligned(i * 8, 8), :]

    def vector_copies(i):
        copies = []
        for q, owner in enumerate(held(bits + [1], i)):
            slot = 2 ** i - 1 + q
            copies.append(remote_dp(
                vec_slot(owner), vec_slot(owner),
                vsend.at[slot], vrecv.at[slot], flip(me, (bits + [1])[i])))
        return copies

    def chosen(shape, test):
        at, lane = (lax.broadcasted_iota(jnp.int32, shape, d) for d in (0, 1))
        return test(at, lane)

    start(1)
    start(0)
    vec_ref[...] = jnp.zeros_like(vec_ref)
    at = aligned(me * block_rows, block_rows)
    wide_rows = rows_ref[...].astype(F32)
    for j, row in enumerate((0, 1, 5, 6)):
        vec_ref[row : row + 1, at] = wide_rows[j : j + 1]
    step = HEAD // count
    key_step = ROT // count
    by_head = lambda r, lane: lane // HEAD == r
    up = up_shift_ref[...]
    near = jnp.where(chosen((up.shape[1], units_here), by_head), 1.0, 0.0).astype(BF16)
    spread = dot(up, near)
    keep = chosen(spread.shape, lambda r, lane: lane % HEAD == me * step + r)
    vec_ref[2:3, pl.ds(0, units_here)] = jnp.sum(jnp.where(keep, spread, 0.0), axis=0, keepdims=True)
    near = jnp.where(
        chosen((step, local_width), lambda r, lane: lane % HEAD == me * step + r), 1.0, 0.0
    ).astype(BF16)
    for j in range(2):
        spread = dot(qv_ref[j], near)
        kept = jnp.where(chosen(spread.shape, by_head), spread, 0.0)
        vec_ref[3:4, pl.ds(2 * j * local_width, local_width)] = jnp.sum(kept, axis=0, keepdims=True)
    keys = key_ref[...]
    near = jnp.where(chosen((keys.shape[1], local_width), by_head), 1.0, 0.0).astype(BF16)
    spread = dot(keys, near)
    keep = chosen(spread.shape, lambda r, lane: lane % HEAD == me * key_step + r)
    vec_ref[3:4, pl.ds(local_width, local_width)] = jnp.sum(
        jnp.where(keep, spread, 0.0), axis=0, keepdims=True)

    vec_slot(me)[...] = vec_ref[...]
    for i in range(stages + 1):
        for c in vector_copies(i):
            c.start()
        for c in vector_copies(i):
            c.wait_recv()
    total = vec_slot(0)[...]
    for owner in range(1, count):
        total = total + vec_slot(owner)[...]
    vec_ref[...] = total

    sums_ref[...] = jnp.zeros_like(sums_ref)
    x_copy().wait()
    cot_copy.wait()

    def norm_step(i, total):
        events_at(i, ((NORM_EVENTS[0], (0,)), (NORM_EVENTS[1], (1,))))
        at = aligned(i * NORM_ROWS, NORM_ROWS)
        wide = acts[at, pl.ds(act_at, width)].astype(F32)
        mean = jnp.mean(wide, axis=1, keepdims=True)
        centred = wide - mean
        var = jnp.mean(centred * centred, axis=1, keepdims=True)
        inv = lax.rsqrt(var + EPSILON)
        stats[at, 0:1] = mean
        stats[at, 1:2] = inv
        normed = centred * inv
        low[at, :] = (normed * vec_ref[0:1, :] + vec_ref[1:2, :]).astype(BF16)
        sums_ref[2:3, :] += jnp.sum(cot[at, :].astype(F32), axis=0, keepdims=True)
        return total

    lax.fori_loop(0, rows // NORM_ROWS, norm_step, 0)

    half = ROT // 2
    lane_in_head = lax.broadcasted_iota(jnp.int32, (SEQ, LANES), 1) % HEAD

    def segments_of(s):
        row = seg_ref[s].astype(F32)
        return row, jnp.transpose(jnp.broadcast_to(row, (LANES, SEQ)))[:, 0:1]

    def table_step(s, carry):
        row, column = segments_of(s)
        starts = jnp.sum(jnp.where(row < column, 1.0, 0.0), axis=1, keepdims=True)
        place = lax.broadcasted_iota(jnp.int32, (SEQ, 1), 0).astype(F32)
        angles = (place - starts) * inverse_ref[...]
        at = aligned(s * SEQ, SEQ)
        sine = jnp.sin(angles)
        tables[0, at, :] = jnp.where(lane_in_head < ROT, jnp.cos(angles), 1.0)
        tables[1, at, :] = jnp.where(
            lane_in_head < half, -sine, jnp.where(lane_in_head < ROT, sine, 0.0))
        return carry

    lax.fori_loop(0, rows // SEQ, table_step, 0)
    event(2)
    event(3)
    finish(0)


    def lane_is_leading(shape):
        lane = lax.broadcasted_iota(jnp.int32, shape, 1)
        return (lane % HEAD) < half

    def swap(t):
        size = t.shape[1]
        return jnp.where(
            lane_is_leading(t.shape), pltpu.roll(t, size - half, 1), pltpu.roll(t, half, 1))

    def qkv_step(i, carry):
        events_at(i, ((3, (4,)), (6, (5,)), (11, (6,))))
        tile = i // row_tiles
        at = aligned((i % row_tiles) * ROW_TILE, ROW_TILE)
        cols = aligned(tile * COL_TILE, COL_TILE)
        t = dot(low[at, :], wqu[:, cols]) + vec_ref[3:4, cols]
        wide = lambda j: jnp.concatenate([tables[j, at, :]] * (COL_TILE // LANES), axis=1)
        rotated = t * wide(0) + swap(t) * wide(1)
        is_value = tile >= 2 * local_width // COL_TILE
        acts[at, cols] = jnp.where(is_value, t, rotated).astype(BF16)
        return carry

    lax.fori_loop(0, row_tiles * qkv_cols // COL_TILE, qkv_step, 0)
    finish(1)

    def mixed_step(i, carry):
        at = aligned((i % row_tiles) * ROW_TILE, ROW_TILE)
        tile = i // row_tiles
        g = dot(cot[at, :], wdd[aligned(tile * COL_TILE, COL_TILE), :], 1, 1).astype(BF16)
        for j in range(COL_TILE // LANES):
            part[tile * (COL_TILE // LANES) + j, at, :] = g[:, j * LANES : (j + 1) * LANES]
        return carry

    lax.fori_loop(0, row_tiles * local_width // COL_TILE, mixed_step, 0)
    pairs = local_width // LANES
    event(7)

    def attention_step(i, carry):
        s, p = i // pairs, i % pairs
        at = aligned(s * SEQ, SEQ)
        lanes = [aligned(j * local_width + p * LANES, LANES) for j in range(3)]

        events_at(i, ((2, (8,)), (3, (9,)), (5, (10,)), (6, (11,)), (7, (12,))))

        @pl.when(p == 0)
        def _():
            across = lax.broadcasted_iota(jnp.int32, (SEQ, SEQ), 1)
            down = lax.broadcasted_iota(jnp.int32, (SEQ, SEQ), 0)
            row, column = segments_of(s)
            allowed = (column == row) & (down >= across)
            mask[...] = jnp.where(allowed, 0.0, NEGATIVE)

        q, k, v = [acts[at, l] for l in lanes]
        go = part[p, at, :]
        lane = lax.broadcasted_iota(jnp.int32, (SEQ, LANES), 1)
        zero = jnp.zeros((), BF16)
        total = None
        for h in range(LANES // HEAD):
            mine = (lane // HEAD) == h
            kh, vh, qh, gh = [jnp.where(mine, t, zero) for t in (k, v, q, go)]
            by_row, by_key = [], []
            for r in range(SEQ // QUERY_TILE):
                seen = (r + 1) * QUERY_TILE
                here = slice(r * QUERY_TILE, seen)
                scores = dot(q[here], kh[:seen], 1, 1) * SCALE + mask[here, :seen]
                top = jnp.max(scores, axis=1, keepdims=True)
                e = jnp.exp(scores - top)
                probs = e / jnp.sum(e, axis=1, keepdims=True)
                probs_low = probs.astype(BF16)
                gprobs = dot(go[here], vh[:seen], 1, 1)
                delta = jnp.sum(probs * gprobs, axis=1, keepdims=True)
                gs = (probs * (gprobs - delta) * SCALE).astype(BF16)
                by_row.append((dot(probs_low, vh[:seen]), dot(gs, kh[:seen])))
                keyed = (dot(gs, qh[here], 0, 0), dot(probs_low, gh[here], 0, 0))
                if by_key:
                    keyed = tuple(
                        jnp.concatenate([old + new[: old.shape[0]], new[old.shape[0] :]], axis=0)
                        for old, new in zip(by_key, keyed))
                by_key = keyed
            terms = [jnp.concatenate(t, axis=0) for t in zip(*by_row)] + list(by_key)
            total = terms if total is None else [a + b for a, b in zip(total, terms)]
        acts[at, aligned(mix_at + p * LANES, LANES)] = total[0].astype(BF16)

        def back(t):
            return t * tables[0, at, :] - swap(t) * tables[1, at, :]

        for j, g in enumerate((back(total[1]), back(total[2]), total[3])):
            acts[at, lanes[j]] = g.astype(BF16)
            sums_ref[4:5, lanes[j]] += jnp.sum(g, axis=0, keepdims=True)
        return carry

    lax.fori_loop(0, (rows // SEQ) * pairs, attention_step, 0)
    event(13)
    finish(2)
    finish(3)

    tiles = units_here // COL_TILE
    per_part = row_tiles * tiles // PARTS

    def ffn_step(i, carry):
        events_at(i, (
            (per_part, (14,)), (per_part + 2, (15,)), (2 * per_part, (16,)),
            (2 * per_part + 1, (17,)), (3 * per_part - 1, (18,)), (3 * per_part, (19,)),
        ))
        for q in range(1, PARTS):
            @pl.when(i == q * per_part)
            def _():
                finish(2 + 2 * q)
                finish(3 + 2 * q)

        at = aligned((i % row_tiles) * ROW_TILE, ROW_TILE)
        tile = i // row_tiles
        cols = aligned(tile * COL_TILE, COL_TILE)
        hidden = dot(low[at, :], wqu[:, aligned(qkv_cols + tile * COL_TILE, COL_TILE)])
        hidden = hidden + vec_ref[2:3, cols]
        grad = dot(cot[at, :], wdd[aligned(local_width + tile * COL_TILE, COL_TILE), :], 1, 1)
        square = hidden * hidden
        th = jnp.tanh(GELU_A * hidden * (1.0 + GELU_B * square))
        acts[at, aligned(act_at + tile * COL_TILE, COL_TILE)] = (
            0.5 * hidden * (1.0 + th)).astype(BF16)
        slope = 0.5 * (1.0 + th) + 0.5 * hidden * (1.0 - th * th) * (
            GELU_A * (1.0 + 3.0 * GELU_B * square))
        grad = grad * slope
        acts[at, aligned(gh_at + tile * COL_TILE, COL_TILE)] = grad.astype(BF16)
        sums_ref[3:4, cols] += jnp.sum(grad, axis=0, keepdims=True)
        return carry

    lax.fori_loop(0, row_tiles * tiles, ffn_step, 0)
    for u in range(len(units)):
        drain(u)
    for i in range(stages + 1):
        for c in vector_copies(i):
            c.wait_send()

    chunks = width // CHUNK
    every = 2 * chunks

    def remote_z(src, dst, ssem, rsem, peer):
        return pltpu.make_async_remote_copy(
            src_ref=src, dst_ref=dst, send_sem=ssem, recv_sem=rsem,
            device_id={"tensor": peer}, device_id_type=MESH)

    def columns(c):
        return aligned((c % chunks) * CHUNK, CHUNK)

    def copy_a(c):
        return remote_z(part.at[c % chunks], inbox.at[c % SLOTS], a_send.at[c % SLOTS],
                        a_recv.at[c % SLOTS], flip(level, 1))

    def copy_b(c):
        return remote_z(part.at[c % chunks], cross.at[c % SLOTS], b_send.at[c % SLOTS],
                        b_recv.at[c % SLOTS], depth - 1 - level)

    def copy_c_out(c):
        return remote_z(cross.at[c % SLOTS], inbox.at[c % SLOTS], c_send.at[c % SLOTS],
                        c_recv.at[c % SLOTS], flip(level, 1))

    def copy_c_grad(c):
        return remote_z(gn.at[:, columns(c)], gn.at[:, columns(c)], c_send.at[c % SLOTS],
                        c_recv.at[c % SLOTS], flip(level, 1))

    def out_copy(src, c):
        return pltpu.make_async_copy(src.at[c % SLOTS], block_out.at[:, columns(c)],
                                     z_out.at[c % SLOTS])

    gn_copy = pltpu.make_async_copy(x_hbm, gn, local.at[len(units) + 2])

    @pl.when(inner)
    def _():
        gn_copy.start()
        gn_copy.wait()

    add_rows = 256
    x_late = wqu.at[pl.ds(0, rows), pl.ds(0, width)]

    def by_rows(step):
        def body(i, carry):
            step(aligned(i * add_rows, add_rows))
            return carry
        lax.fori_loop(0, rows // add_rows, body, 0)

    def tick(k):
        @pl.when(inner & (k < every))
        def _():
            copy_a(k).wait_recv()

            def add(at):
                part[k % chunks, at, :] = (
                    part[k % chunks, at, :].astype(F32) + inbox[k % SLOTS, at, :].astype(F32)
                ).astype(BF16)

            by_rows(add)

            @pl.when(k >= SLOTS)
            def _():
                pl.semaphore_wait(credit, 1)

            copy_b(k).start()

        @pl.when(inner & (k >= 2) & (k < every + 2))
        def _():
            j = k - 2
            copy_b(j).wait_recv()
            copy_b(j).wait_send()

            @pl.when(j < chunks)
            def _():
                def add(at):
                    pair = part[j % chunks, at, :].astype(F32) + cross[j % SLOTS, at, :].astype(F32)
                    shifts = vec_ref[5:6, columns(j)], vec_ref[6:7, columns(j)]
                    wide = gn[at, columns(j)].astype(F32)
                    cross[j % SLOTS, at, :] = (wide + pair + shifts[0] + shifts[1]).astype(BF16)

                by_rows(add)
                copy_c_out(j).start()
                out_copy(cross, j).start()

            @pl.when(j >= chunks)
            def _():
                def add(at):
                    gn[at, columns(j)] = (
                        part[j % chunks, at, :].astype(F32) + cross[j % SLOTS, at, :].astype(F32)
                    ).astype(BF16)

                by_rows(add)
                copy_c_grad(j).start()

        @pl.when(inner & (k >= 4) & (k < every + 4))
        def _():
            i = k - 4

            @pl.when(i < chunks)
            def _():
                copy_c_out(i).wait_send()
                out_copy(cross, i).wait()

            @pl.when(i >= chunks)
            def _():
                copy_c_grad(i).wait_send()

            @pl.when(i < every - SLOTS)
            def _():
                pl.semaphore_signal(
                    credit, inc=1, device_id={"tensor": depth - 1 - level}, device_id_type=MESH)

        @pl.when(outer & (k >= 4) & (k < every + 4))
        def _():
            i = k - 4
            copy_a(i).wait_send()

            @pl.when(i < chunks)
            def _():
                copy_c_out(i).wait_recv()
                out_copy(inbox, i).start()
                out_copy(inbox, i).wait()

            @pl.when(i >= chunks)
            def _():
                copy_c_grad(i).wait_recv()

            @pl.when(i + SLOTS < every)
            def _():
                copy_a(i + SLOTS).start()

        @pl.when((k >= chunks + 4) & (k < every + 4))
        def _():
            cols = columns(k - 4)

            def gather_sums(at):
                g = gn[at, cols].astype(F32)
                normed = (x_late[at, cols].astype(F32) - stats[at, 0:1]) * stats[at, 1:2]
                product = g * normed
                gain = vec_ref[0:1, cols]
                tables[0, at, :] += g * gain
                tables[1, at, :] += product * gain
                sums_ref[0:1, cols] += jnp.sum(product, axis=0, keepdims=True)
                sums_ref[1:2, cols] += jnp.sum(g, axis=0, keepdims=True)

            by_rows(gather_sums)

    def ticks(lo, hi):
        def body(k, carry):
            tick(k)
            return carry
        lax.fori_loop(lo, hi, body, 0)

    def produce(first, tile, r, t):
        at = aligned(r * ROW_TILE, ROW_TILE)
        for j in range(COL_TILE // CHUNK):
            part[(first + tile * (COL_TILE // CHUNK) + j) % chunks, at, :] = (
                t[:, j * CHUNK : (j + 1) * CHUNK].astype(BF16))

    per_tile = COL_TILE // CHUNK

    def branch_step(i, carry):
        tile, r = i // row_tiles, i % row_tiles
        at = aligned(r * ROW_TILE, ROW_TILE)
        cols = aligned(tile * COL_TILE, COL_TILE)
        produce(0, tile, r, dot(acts[at, pl.ds(mix_at, local_width + units_here)], wdd[:, cols]))

        @pl.when(r == row_tiles - 1)
        def _():
            for j in range(per_tile):
                @pl.when(outer & (tile * per_tile + j < SLOTS))
                def _():
                    copy_a(tile * per_tile + j).start()

            @pl.when(tile % 2 == 1)
            def _():
                tick(tile // 2)

        return carry

    lax.fori_loop(0, row_tiles * width // COL_TILE, branch_step, 0)
    done_ticks = width // COL_TILE // 2

    grad_tiles = acts.shape[1] // GRAD_TILE
    low_tiles = mix_at // GRAD_TILE
    across = width // GRAD_TILE
    blocks = 2 ** stages
    staged = wdd.shape[0] // block_rows * across // grad_tiles * grad_tiles

    def stage_at(k, p=None):
        start, size = (0, block_rows) if p is None else (p * (block_rows // 2), block_rows // 2)
        at = aligned((k // across) * block_rows + start, size)
        return wdd.at[at, aligned((k % across) * GRAD_TILE, GRAD_TILE)]

    def relative(base, v):
        for i, bit in enumerate(bits):
            has = (v // 2 ** (stages - 1 - i)) % 2
            base = base + has * (bit - 2 * bit * ((base // bit) % 2))
        return base

    def turn(block):
        cols = aligned(block * block_rows, block_rows)
        turned[0] = jnp.transpose(low[:, cols])
        turned[1] = jnp.transpose(cot[:, cols])

    def grad_tile(n):
        return dot(turned[n // low_tiles], acts[:, aligned(n * GRAD_TILE, GRAD_TILE)])

    def core_copy(i):
        return remote_dp(stage_at(i % staged), core_rx.at[i], core_send.at[i % staged],
                         core_recv.at[i], flip(me, 1))

    def other_step(i, carry):
        n = i % grad_tiles

        @pl.when(n == 0)
        def _():
            turn(relative(flip(me, 1), blocks - 1 - i // grad_tiles))

        @pl.when(i >= staged)
        def _():
            core_copy(i - staged).wait_send()

        stage_at(i % staged)[...] = grad_tile(n).astype(BF16)
        core_copy(i).start()

        @pl.when(i % TICK_TILES == TICK_TILES - 1)
        def _():
            tick(done_ticks + i // TICK_TILES)

        return carry

    lax.fori_loop(0, blocks * grad_tiles, other_step, 0)
    done_ticks += blocks * grad_tiles // TICK_TILES

    def first_bit(v, order):
        for s, bit in enumerate(order):
            if v // 2 ** (stages - 1 - bits.index(bit)) % 2:
                return s
        return len(order)

    pieces = {}
    for v in range(blocks):
        for p, order in enumerate(orders):
            for s in range(first_bit(v, order)):
                pieces[(v, p, s)] = len(pieces)
    spare = staged

    def link_copy(v, p, n):
        order = orders[p]
        s = first_bit(v, order)
        left = v - 2 ** (stages - 1 - bits.index(order[s]))
        piece = pieces[(left, p, s)]
        return remote_dp(
            stage_at((blocks - 1 - v) * grad_tiles + n, p), link_rx.at[piece, n],
            link_send.at[2 * (v - 1) + p, n], link_recv.at[piece, n], flip(me, order[s]))

    def arrival(v, p, s, n):
        piece = pieces[(v, p, s)]
        return remote_dp(
            stage_at(0, p), link_rx.at[piece, n], link_send.at[0, 0], link_recv.at[piece, n],
            flip(me, orders[p][s]))

    def own_block(v):
        q = blocks - 1 - v
        mine = [key for key in pieces if key[0] == v]
        assert v == 0 or len(mine) < 2

        def core_slot(n):
            return stage_at(spare + n % DEPTH)

        def core_fetch(n):
            return pltpu.make_async_copy(
                core_rx.at[q * grad_tiles + n], core_slot(n), fetch_sem.at[n % DEPTH, 0])

        def piece_slot(key, n):
            _, p, s = key
            if v == 0:
                return stage_at((n % DEPTH) * stages + s, p)
            return spare_tiles.at[n % DEPTH]

        def piece_fetch(key, n):
            return pltpu.make_async_copy(
                link_rx.at[pieces[key], n], piece_slot(key, n),
                fetch_sem.at[n % DEPTH, 1 + mine.index(key)])

        def fetch(n):
            core_copy(q * grad_tiles + n).wait_recv()
            core_fetch(n).start()
            for key in mine:
                arrival(*key, n).wait_recv()
                piece_fetch(key, n).start()

        def grad_out(n):
            at = aligned((n % 2) * block_rows, block_rows)
            flat, tall = mask.at[at, :], mask.at[:, at]
            sem = grad_sem.at[n % 2]
            first = qkv_cols // GRAD_TILE
            each = local_width // GRAD_TILE
            last = low_tiles + local_width // GRAD_TILE
            cases = (
                (n < first, flat, lambda: qkv_out.at[n // each].at[
                    :, aligned((n % each) * GRAD_TILE, GRAD_TILE)]),
                ((n >= first) & (n < low_tiles), flat,
                 lambda: up_out.at[:, aligned((n - first) * GRAD_TILE, GRAD_TILE)]),
                ((n >= low_tiles) & (n < last), tall,
                 lambda: dense_out.at[aligned((n - low_tiles) * GRAD_TILE, GRAD_TILE), :]),
                (n >= last, tall,
                 lambda: down_out.at[aligned((n - last) * GRAD_TILE, GRAD_TILE), :]),
            )
            return [(c, pltpu.make_async_copy(src, dst(), sem)) for c, src, dst in cases]

        def for_out(n, act):
            for cond, copy in grad_out(n):
                @pl.when(cond)
                def _():
                    act(copy)

        turn(relative(me, v))
        if v == 0:
            for n in range(DEPTH * stages):
                for p in range(2):
                    link_copy(blocks - 1, p, n).wait_send()
        for n in range(DEPTH - 1):
            fetch(n)

        def step(n, carry):
            t = grad_tile(n)
            core_fetch(n).wait()
            t = t + core_slot(n)[...].astype(F32)
            for key in mine:
                piece_fetch(key, n).wait()
            for s in sorted({key[2] for key in mine}):
                sides = []
                for p in range(2):
                    rows_p = slice(p * (block_rows // 2), (p + 1) * (block_rows // 2))
                    side = t[rows_p]
                    if (v, p, s) in pieces:
                        side = side + piece_slot((v, p, s), n)[...].astype(F32)
                    sides.append(side)
                t = jnp.concatenate(sides, axis=0)
            if v:
                k = (blocks - 1 - v) * grad_tiles + n
                core_copy(k if v < blocks - 1 else k + staged).wait_send()
                stage_at(k)[...] = t.astype(BF16)
                for p in range(2):
                    link_copy(v, p, n).start()
            else:
                @pl.when((n >= 2) & (n != low_tiles + 1))
                def _():
                    for_out(n - 2, lambda c: c.wait())

                @pl.when(n == low_tiles)
                def _():
                    for_out(n - 1, lambda c: c.wait())

                @pl.when(n < low_tiles)
                def _():
                    mask[aligned((n % 2) * block_rows, block_rows), :] = t

                @pl.when(n >= low_tiles)
                def _():
                    mask[:, aligned((n % 2) * block_rows, block_rows)] = jnp.transpose(t)

                for_out(n, lambda c: c.start())

            @pl.when(n + DEPTH - 1 < grad_tiles)
            def _():
                fetch(n + DEPTH - 1)

            return carry

        lax.fori_loop(0, grad_tiles, step, 0)
        if v == 0:
            for n in (grad_tiles - 2, grad_tiles - 1):
                for cond, copy in grad_out(n):
                    if bool(cond):
                        copy.wait()

    own_block(blocks - 1)
    ticks(done_ticks, done_ticks + 1)
    done_ticks += 1
    before = done_ticks
    lag = SLOTS - 2 - per_tile

    def grad_step(i, carry):
        tile, r = i // row_tiles, i % row_tiles

        @pl.when(r == 0)
        def _():
            ticks(
                jnp.maximum(before, lag + per_tile * tile),
                jnp.maximum(before, lag + per_tile * (tile + 1)),
            )

            for v in range(1, blocks - 1):
                @pl.when(tile == width // COL_TILE // 2 + blocks - 2 - v)
                def _():
                    own_block(v)

        at = aligned(r * ROW_TILE, ROW_TILE)
        t = dot(acts[at, pl.ds(0, mix_at)], wqu[aligned(tile * COL_TILE, COL_TILE), :], 1, 1)
        produce(chunks, tile, r, t)
        return carry

    lax.fori_loop(0, row_tiles * width // COL_TILE, grad_step, 0)
    done_ticks = lag + per_tile * (width // COL_TILE)
    last_block = every - 4
    late_copy = pltpu.make_async_copy(x_hbm, x_late, local.at[len(units)])
    late_copy.start()
    tables[...] = jnp.zeros_like(tables)
    late_copy.wait()

    ticks(done_ticks, last_block)
    own_block(0)
    ticks(last_block, every + 4)
    for v in range(1, blocks):
        for p in range(2):
            for n in range(grad_tiles):
                if v == blocks - 1 and n < DEPTH * stages:
                    continue
                link_copy(v, p, n).wait_send()

    def row_slot(i):
        return vec_in.at[aligned((i % 2) * BACK_ROWS, BACK_ROWS), :]

    def row_copy(i):
        return pltpu.make_async_copy(
            row_slot(i), input_grad.at[aligned(i * BACK_ROWS, BACK_ROWS), :], row_sem.at[i % 2])

    def back_step(i, carry):
        at = aligned(i * BACK_ROWS, BACK_ROWS)
        mean, inv = stats[at, 0:1], stats[at, 1:2]
        first = jnp.sum(tables[0, at, :], axis=1, keepdims=True) * (inv / width)
        second = jnp.sum(tables[1, at, :], axis=1, keepdims=True) * (inv * inv / width)
        scaled = gn[at, :].astype(F32) * vec_ref[0:1, :]
        grad = scaled * inv - (x_late[at, :].astype(F32) - mean) * second - first

        @pl.when(i >= 2)
        def _():
            row_copy(i - 2).wait()

        row_slot(i)[...] = grad + cot[at, :].astype(F32)
        row_copy(i).start()
        return carry

    back_steps = rows // BACK_ROWS

    def sum_copy(i, bit):
        return remote_dp(sums_ref, sum_in.at[i], sum_send.at[i], sum_recv.at[i], flip(me, bit))

    trips = bits + [1]
    for i, bit in enumerate(trips):
        copy = sum_copy(i, bit)
        copy.start()
        lax.fori_loop(back_steps * i // len(trips), back_steps * (i + 1) // len(trips), back_step, 0)
        copy.wait()
        sums_ref[...] = sums_ref[...] + sum_in[i]
    row_copy(back_steps - 2).wait()
    row_copy(back_steps - 1).wait()


def fits(shards, depth, local_width, block_cols):
    return (
        shards & (shards - 1) == 0 and len(link_bits(shards)) == 2 and depth == 4
        and block_cols % COL_TILE == 0 and local_width % GRAD_TILE == 0
    )


def layer(x, cot, qkv_share, dense_share, up_share, down_share, vectors, segments):
    rows, width = x.shape
    count = lax.axis_size("dp")
    local_width = dense_share.shape[0]
    units_here = up_share.shape[1]
    block_rows = up_share.shape[0]
    seqs = rows // SEQ
    links = len(link_bits(count))
    blocks = 2 ** links
    slots = 2 * (blocks - 1) + blocks
    acts_cols = 4 * local_width + 2 * units_here
    grad_tiles = acts_cols // GRAD_TILE
    pieces = 0
    for order in range(2):
        pieces += sum(blocks // 2 ** (s + 1) for s in range(links))
    staged = (local_width + units_here) // block_rows * (width // GRAD_TILE) // grad_tiles * grad_tiles
    chunks = width // CHUNK
    any_ = pl.BlockSpec(memory_space=pl.ANY)
    vmem = pl.BlockSpec(memory_space=pltpu.VMEM)
    b16 = lambda *s: jax.ShapeDtypeStruct(s, BF16)
    f32 = lambda *s: jax.ShapeDtypeStruct(s, F32)
    dma = lambda *s: pltpu.SemaphoreType.DMA(s)
    outs = pl.pallas_call(
        layer_body,
        in_specs=[any_] * 6 + [vmem] * 6,
        out_specs=[any_] * 8 + [vmem],
        out_shape=[
            b16(rows, width), f32(rows, width), f32(3, block_rows, local_width),
            f32(local_width, block_rows), f32(block_rows, units_here), f32(units_here, block_rows),
            b16(blocks * grad_tiles, block_rows, GRAD_TILE),
            b16(pieces, grad_tiles, block_rows // 2, GRAD_TILE), f32(8, width),
        ],
        scratch_shapes=[
            pltpu.VMEM((width, 3 * local_width + units_here), BF16),
            pltpu.VMEM((local_width + units_here, width), BF16),
            pltpu.VMEM((rows, acts_cols), BF16), pltpu.VMEM((rows, width), BF16),
            pltpu.VMEM((rows, width), BF16), pltpu.VMEM((SEQ, SEQ), F32),
            pltpu.VMEM((8, width), F32), pltpu.VMEM((8 * count, width), F32),
            pltpu.VMEM((2, block_rows, rows), BF16), pltpu.VMEM((rows, width), BF16),
            pltpu.VMEM((chunks, rows, CHUNK), BF16), pltpu.VMEM((SLOTS, rows, CHUNK), BF16),
            pltpu.VMEM((SLOTS, rows, CHUNK), BF16),
            pltpu.VMEM((2, rows, LANES), F32), pltpu.VMEM((rows, LANES), F32),
            pltpu.VMEM((DEPTH, block_rows // 2, GRAD_TILE), BF16), pltpu.VMEM((links + 1, 8, width), F32),
            dma(2 + 2 * PARTS, slots), dma(2 + 2 * PARTS, slots), dma(count - 1), dma(count - 1),
            dma(7 + 2 * PARTS),
            dma(SLOTS), dma(SLOTS), dma(SLOTS), dma(SLOTS), dma(SLOTS), dma(SLOTS), dma(SLOTS),
            pltpu.SemaphoreType.REGULAR,
            dma(staged), dma(blocks * grad_tiles), dma(2 * (blocks - 1), grad_tiles),
            dma(pieces, grad_tiles), dma(DEPTH, 1 + 2 * links), dma(2), dma(2),
            dma(links + 1), dma(links + 1),
        ],
        compiler_params=pltpu.CompilerParams(
            collective_id=0, has_side_effects=True, vmem_limit_bytes=67_043_328),
        cost_estimate=pl.CostEstimate(
            flops=18 * rows * width * (local_width + units_here), bytes_accessed=80_000_000,
            transcendentals=rows * units_here),
        name="layer",
    )(
        x, cot, qkv_share, dense_share, up_share, down_share, *vectors, INVERSE,
        segments.reshape(seqs, 1, SEQ),
    )
    return outs[:6] + outs[8:]


def gelu_tanh(inputs):
    return jax.nn.gelu(inputs, approximate=True)


def line_sum(part, finish):
    size = lax.axis_size("tensor")
    if size != 4:
        return finish(lax.psum(part, "tensor").astype(F32))
    index = lax.axis_index("tensor")
    inward = lax.ppermute(part, "tensor", [(0, 1), (3, 2)])
    pair = (part.astype(F32) + inward.astype(F32)).astype(BF16)
    other = lax.ppermute(pair, "tensor", [(1, 2), (2, 1)])
    done = finish(pair.astype(F32) + other.astype(F32))
    back = lax.ppermute(done, "tensor", [(1, 0), (2, 3)])
    return jnp.where((index == 0) | (index == size - 1), back, done)


def local(
    block_input, segments, norm_gain, norm_bias, qkv_weight, query_value_bias, key_bias,
    dense_weight, dense_bias, up_weight, up_bias, down_weight, down_bias, cotangent,
):
    rows, width = block_input.shape
    local_width = qkv_weight.shape[2]
    heads = local_width // HEAD
    seqs = rows // SEQ
    shards = lax.axis_size("dp")
    fused = fits(shards, lax.axis_size("tensor"), local_width, down_weight.shape[1])
    if fused:
        mine = lax.axis_index("dp")
        four = jnp.stack([norm_gain, norm_bias, dense_bias, down_bias])
        block_output, input_grad, qkv_out, dense_out, up_out, down_out, total = layer(
            block_input, cotangent, qkv_weight.transpose(1, 0, 2), dense_weight, up_weight,
            down_weight, [four, up_bias.T, query_value_bias, key_bias.T], segments)

        def mine_of(value, lead):
            return lax.dynamic_index_in_dim(
                value.reshape(lead, shards, -1), mine, axis=1, keepdims=False)

        sums = total[4]
        qv_sums = jnp.stack([sums[:local_width], sums[2 * local_width : 3 * local_width]])
        key_sums = sums[local_width : 2 * local_width].reshape(heads, HEAD)[:, :ROT]
        bias_out = mine_of(total[2], 1).reshape(-1)
        return (
            block_output, input_grad, mine_of(total[0], 1).reshape(-1),
            mine_of(total[1], 1).reshape(-1), qkv_out.transpose(1, 0, 2),
            mine_of(qv_sums, 2 * heads).reshape(query_value_bias.shape),
            mine_of(key_sums, heads), dense_out, bias_out, up_out,
            mine_of(total[3], up_bias.shape[0]), down_out, bias_out,
        )
    smalls = (norm_gain, norm_bias, dense_bias, down_bias, up_bias, query_value_bias, key_bias)
    packed = jnp.concatenate([s.reshape(1, -1) for s in smalls], axis=1)
    packed = lax.all_gather(packed, "dp", axis=0, tiled=True)
    pieces = []
    at = 0
    for s in smalls:
        pieces.append(packed[:, at : at + s.size].reshape((shards,) + s.shape).astype(F32))
        at += s.size
    gain, shift, dense_shift, down_shift = [p.reshape(1, -1) for p in pieces[:4]]
    up_shift = pieces[4].transpose(1, 0, 2).reshape(1, -1)
    qv_bias = pieces[5].transpose(1, 2, 0, 3).reshape(2, local_width)
    key_part = pieces[6].transpose(1, 0, 2).reshape(heads, ROT)
    key_full = jnp.concatenate([key_part, jnp.zeros((heads, HEAD - ROT), F32)], axis=1)
    bias = jnp.concatenate(
        [qv_bias[0:1], key_full.reshape(1, -1), qv_bias[1:2], jnp.zeros((5, local_width), F32)], axis=0
    )

    dense_all = lax.all_gather(dense_weight, "dp", axis=1, tiled=True)
    qkv_all = lax.all_gather(qkv_weight.reshape(qkv_weight.shape[0], -1), "dp", axis=0, tiled=True)
    up_all = lax.all_gather(up_weight, "dp", axis=0, tiled=True)
    down_all = lax.all_gather(down_weight, "dp", axis=1, tiled=True)

    wide = block_input.astype(F32)
    mean = jnp.mean(wide, axis=1, keepdims=True)
    centred = wide - mean
    inv_std = lax.rsqrt(jnp.mean(centred * centred, axis=1, keepdims=True) + EPSILON)
    normed = centred * inv_std
    low = (normed * gain + shift).astype(BF16)

    tables = rotary_tables(segments)
    grad_mixed = dot(cotangent, dense_all, 1, 1).astype(BF16)
    projected = dot(low, qkv_all)
    mixed, grad_projected, bias_sums = attention(projected, grad_mixed, bias, tables, segments)
    bias_sums = jnp.sum(bias_sums, axis=0)

    hidden = dot(low, up_all) + up_shift
    activated, gelu_back = jax.vjp(gelu_tanh, hidden)
    activated = activated.astype(BF16)
    grad_hidden = gelu_back(dot(cotangent, down_all, 1, 1))[0]
    grad_up_bias = jnp.sum(grad_hidden, axis=0)
    grad_hidden_low = grad_hidden.astype(BF16)
    grad_joined = jnp.concatenate([grad_projected[i] for i in range(3)], axis=1)

    branches = (dot(mixed, dense_all) + dot(activated, down_all)).astype(BF16)
    grad_part = (dot(grad_joined, qkv_all, 1, 1) + dot(grad_hidden_low, up_all, 1, 1)).astype(BF16)
    grad_dense = dot(mixed, cotangent, 0, 0).astype(BF16)
    grad_qkv = dot(low, grad_joined, 0, 0).astype(BF16)
    grad_down = dot(activated, cotangent, 0, 0).astype(BF16)
    grad_up = dot(low, grad_hidden_low, 0, 0).astype(BF16)

    outs, grads = [], []
    for s in range(seqs):
        at = slice(s * SEQ, (s + 1) * SEQ)
        outs.append(
            line_sum(
                branches[at],
                lambda t, at=at: (wide[at] + t + dense_shift + down_shift).astype(BF16),
            )
        )
    for s in range(seqs):
        at = slice(s * SEQ, (s + 1) * SEQ)
        grads.append(line_sum(grad_part[at], lambda t: t.astype(BF16)))
    block_output = jnp.concatenate(outs, axis=0)
    grad_normed = jnp.concatenate(grads, axis=0).astype(F32)

    grad_wide = cotangent.astype(F32)
    scaled = grad_normed * gain
    input_grad = (
        inv_std
        * (
            scaled
            - jnp.mean(scaled, axis=1, keepdims=True)
            - normed * jnp.mean(scaled * normed, axis=1, keepdims=True)
        )
        + grad_wide
    )

    def scatter(value, dim):
        return lax.psum_scatter(value, "dp", scatter_dimension=dim, tiled=True).astype(F32)

    qkv_out = scatter(grad_qkv, 0).reshape(qkv_weight.shape)
    dense_out = scatter(grad_dense, 1)
    up_out = scatter(grad_up, 0)
    down_out = scatter(grad_down, 1)

    key_sums = bias_sums[1].reshape(heads, HEAD)[:, :ROT]
    qv_sums = jnp.stack([bias_sums[0], bias_sums[2]]).reshape(2, heads, HEAD)
    small_sums = (
        jnp.sum(grad_normed * normed, axis=0).reshape(shards, -1),
        jnp.sum(grad_normed, axis=0).reshape(shards, -1),
        jnp.sum(grad_wide, axis=0).reshape(shards, -1),
        grad_up_bias.reshape(up_bias.shape[0], shards, -1).transpose(1, 0, 2).reshape(shards, -1),
        qv_sums.reshape(2, heads, shards, -1).transpose(2, 0, 1, 3).reshape(shards, -1),
        key_sums.reshape(heads, shards, -1).transpose(1, 0, 2).reshape(shards, -1),
    )
    total = lax.psum_scatter(
        jnp.concatenate(small_sums, axis=1), "dp", scatter_dimension=0, tiled=True
    ).reshape(-1)
    shapes = (norm_gain.shape, norm_bias.shape, dense_bias.shape, up_bias.shape,
              query_value_bias.shape, key_bias.shape)
    smalls_out = []
    at = 0
    for part, shape in zip(small_sums, shapes):
        smalls_out.append(total[at : at + part.shape[1]].reshape(shape))
        at += part.shape[1]
    gain_out, shift_out, bias_out, up_bias_out, qv_out, key_out = smalls_out
    return (
        block_output, input_grad, gain_out, shift_out, qkv_out, qv_out, key_out, dense_out,
        bias_out, up_out, up_bias_out, down_out, bias_out,
    )


def solution(mesh):
    in_specs = (
        P("dp", None),
        P("dp"),
        P("dp"),
        P("dp"),
        P("dp", None, "tensor"),
        P(None, "tensor", "dp"),
        P("tensor", "dp"),
        P("tensor", "dp"),
        P("dp"),
        P("dp", "tensor"),
        P("tensor", "dp"),
        P("tensor", "dp"),
        P("dp"),
        P("dp", None),
    )
    out_specs = (
        P("dp", None),
        P("dp", None),
        P("dp"),
        P("dp"),
        P("dp", None, "tensor"),
        P(None, "tensor", "dp"),
        P("tensor", "dp"),
        P("tensor", "dp"),
        P("dp"),
        P("dp", "tensor"),
        P("tensor", "dp"),
        P("tensor", "dp"),
        P("dp"),
    )
    return jax.shard_map(local, mesh=mesh, in_specs=in_specs, out_specs=out_specs, check_vma=False)
```

```python
import functools

import jax
import jax.numpy as jnp
import numpy as np
from jax import lax
from jax.experimental import pallas as pl
from jax.experimental.pallas import tpu as pltpu
from jax.sharding import PartitionSpec as P

HEAD = 64
ROT = 32
SEQ = 512
LANES = 128
EPSILON = 1e-05
SCALE = 0.125
NEGATIVE = -1e30

F32 = jnp.float32
BF16 = jnp.bfloat16


def dot(a, b, ca=1, cb=0):
    return lax.dot_general(a, b, (((ca,), (cb,)), ((), ())), preferred_element_type=F32)


def rotary_tables(segments):
    seg_rows = segments.reshape(-1, SEQ)
    position = jnp.arange(SEQ, dtype=jnp.int32)
    starting = jnp.concatenate(
        [jnp.ones((seg_rows.shape[0], 1), dtype=jnp.bool_), seg_rows[:, 1:] != seg_rows[:, :-1]],
        axis=1,
    )
    starts = lax.cummax(jnp.where(starting, position[None, :], jnp.int32(0)), axis=1)
    offset = (position[None, :] - starts).astype(F32).reshape(-1, 1)
    half = ROT // 2
    lane = jnp.arange(LANES, dtype=jnp.int32) % HEAD
    inverse = 10000.0 ** (-((lane % half).astype(F32) * (2.0 / ROT)))
    angles = offset * inverse[None, :]
    cosine = jnp.where(lane < ROT, jnp.cos(angles), 1.0)
    sine = jnp.sin(angles)
    return (
        cosine,
        jnp.where(lane < half, -sine, 0.0),
        jnp.where((lane >= half) & (lane < ROT), sine, 0.0),
    )


def attention_body(
    q_ref, k_ref, v_ref, go_ref, bias_ref, cos_ref, sa_ref, sb_ref, segc_ref, segr_ref,
    mixed_ref, gp_ref, gb_ref, mask_ref,
):
    half = ROT // 2

    def rotate(t, direction):
        swapped = pltpu.roll(t, LANES - half, 1) * sa_ref[...]
        swapped = swapped + pltpu.roll(t, half, 1) * sb_ref[...]
        return t * cos_ref[...] + direction * swapped

    @pl.when(pl.program_id(1) == 0)
    def _():
        rows = lax.broadcasted_iota(jnp.int32, (SEQ, SEQ), 0)
        cols = lax.broadcasted_iota(jnp.int32, (SEQ, SEQ), 1)
        allowed = (segc_ref[...] == segr_ref[0]) & (rows >= cols)
        mask_ref[...] = jnp.where(allowed, 0.0, NEGATIVE)

    q = rotate(q_ref[...] + bias_ref[0:1, :], 1.0).astype(BF16)
    k = rotate(k_ref[...] + bias_ref[1:2, :], 1.0).astype(BF16)
    v = (v_ref[...] + bias_ref[2:3, :]).astype(BF16)
    go = go_ref[...]
    lane = lax.broadcasted_iota(jnp.int32, (SEQ, LANES), 1)
    mixed = gq = gk = gv = None
    for h in range(LANES // HEAD):
        mine = (lane // HEAD) == h
        zero = jnp.zeros((), BF16)
        kh = jnp.where(mine, k, zero)
        vh = jnp.where(mine, v, zero)
        qh = jnp.where(mine, q, zero)
        gh = jnp.where(mine, go, zero)
        s = dot(q, kh, 1, 1) * SCALE + mask_ref[...]
        top = jnp.max(s, axis=1, keepdims=True)
        e = jnp.exp(s - top)
        p = e / jnp.sum(e, axis=1, keepdims=True)
        low = p.astype(BF16)
        dp = dot(go, vh, 1, 1)
        delta = jnp.sum(p * dp, axis=1, keepdims=True)
        ds = (p * (dp - delta) * SCALE).astype(BF16)
        terms = (dot(low, vh), dot(ds, kh), dot(ds, qh, 0, 0), dot(low, gh, 0, 0))
        if h == 0:
            mixed, gq, gk, gv = terms
        else:
            mixed, gq, gk, gv = [a + b for a, b in zip((mixed, gq, gk, gv), terms)]
    mixed_ref[...] = mixed.astype(BF16)
    gq = rotate(gq, -1.0)
    gk = rotate(gk, -1.0)
    for i, g in enumerate((gq, gk, gv)):
        gp_ref[i] = g.astype(BF16)
        gb_ref[0, i : i + 1, :] = jnp.sum(g, axis=0, keepdims=True)


def attention(projected, grad_mixed, bias, tables, segments):
    rows = projected.shape[0]
    width = projected.shape[1] // 3
    seqs, pairs = rows // SEQ, width // LANES
    tile = lambda f: pl.BlockSpec((SEQ, LANES), f)
    table = tile(lambda s, p: (s, 0))
    return pl.pallas_call(
        attention_body,
        grid=(seqs, pairs),
        in_specs=[
            tile(lambda s, p: (s, p)),
            tile(lambda s, p: (s, pairs + p)),
            tile(lambda s, p: (s, 2 * pairs + p)),
            tile(lambda s, p: (s, p)),
            pl.BlockSpec((8, LANES), lambda s, p: (0, p)),
            table, table, table,
            pl.BlockSpec((SEQ, 1), lambda s, p: (s, 0)),
            pl.BlockSpec((1, 1, SEQ), lambda s, p: (s, 0, 0)),
        ],
        out_specs=[
            tile(lambda s, p: (s, p)),
            pl.BlockSpec((3, SEQ, LANES), lambda s, p: (0, s, p)),
            pl.BlockSpec((1, 8, LANES), lambda s, p: (s, 0, p)),
        ],
        out_shape=[
            jax.ShapeDtypeStruct((rows, width), BF16),
            jax.ShapeDtypeStruct((3, rows, width), BF16),
            jax.ShapeDtypeStruct((seqs, 8, width), F32),
        ],
        scratch_shapes=[pltpu.VMEM((SEQ, SEQ), F32)],
        compiler_params=pltpu.CompilerParams(dimension_semantics=("arbitrary", "arbitrary")),
        cost_estimate=pl.CostEstimate(
            flops=14 * rows * SEQ * width, bytes_accessed=24 * rows * width,
            transcendentals=rows * SEQ * width // HEAD,
        ),
        name="attention",
    )(
        projected, projected, projected, grad_mixed, bias, *tables,
        segments.reshape(rows, 1), segments.reshape(seqs, 1, SEQ),
    )


ROW_TILE = 512
QUERY_TILE = 256
COL_TILE = 256
GRAD_TILE = 512
CHUNK = 128
SLOTS = 8
NORM_ROWS = 32
NORM_EVENTS = (8, 16)
BACK_ROWS = 32
PARTS = 4
DEPTH = 4
TICK_TILES = 12
GELU_A = 0.7978845608028654
GELU_B = 0.044715
MESH = pl.DeviceIdType.MESH
INVERSE = np.asarray(
    10000.0 ** (-(np.arange(LANES) % (ROT // 2)) * (2.0 / ROT)), np.float32).reshape(1, LANES)


def flip(index, bit):
    return index + bit - 2 * bit * ((index // bit) % 2)


def link_bits(count):
    bits = []
    bit = count // 2
    while bit >= 2:
        bits.append(bit)
        bit //= 2
    return bits


def aligned(start, size):
    return pl.ds(pl.multiple_of(start, size), size)


class Unit:
    def __init__(self, share, whole, axis, rows, cols, row_at=0, col_at=0):
        self.share, self.whole, self.axis = share, whole, axis
        self.row0, self.rows = rows
        self.col0, self.cols = cols
        self.row_at, self.col_at = row_at, col_at

    def span(self, half):
        return (0, self.rows) if half is None else (half * (self.rows // 2), self.rows // 2)

    def own(self, half=None):
        start, size = self.span(half)
        return self.share.at[pl.ds(self.row0 + start, size), pl.ds(self.col0, self.cols)]

    def block(self, which, half=None):
        start, size = self.span(half)
        if self.axis == 0:
            rows = aligned(which * self.rows + start, size)
            return self.whole.at[rows, pl.ds(self.col_at, self.cols)]
        cols = aligned(which * self.cols, self.cols)
        return self.whole.at[pl.ds(self.row_at + start, size), cols]


def layer_body(
    x_hbm, cot_hbm, qkv_hbm, dense_hbm, up_hbm, down_hbm, rows_ref, up_shift_ref, qv_ref, key_ref, inverse_ref, seg_ref,
    block_out, input_grad, qkv_out, dense_out, up_out, down_out, core_rx, link_rx, sums_ref,
    wqu, wdd, acts, low, cot, mask, vec_ref, vec_in, turned, gn, part, inbox, cross,
    tables, stats, spare_tiles, sum_in,
    send, recv, vsend, vrecv, local,
    a_send, a_recv, b_send, b_recv, c_send, c_recv, z_out, credit,
    core_send, core_recv, link_send, link_recv, fetch_sem, grad_sem, row_sem, sum_send, sum_recv,
):
    count = lax.axis_size("dp")
    me = lax.axis_index("dp")
    depth = lax.axis_size("tensor")
    level = lax.axis_index("tensor")
    outer = (level == 0) | (level == depth - 1)
    inner = jnp.logical_not(outer)
    bits = link_bits(count)
    orders = (bits, bits[::-1])
    stages = len(bits)
    per_path = 2 ** stages - 1
    rows, width = low.shape
    units_here = up_hbm.shape[1]
    local_width = dense_hbm.shape[0]
    qkv_cols = 3 * local_width
    part_units = units_here // PARTS
    block_rows = up_hbm.shape[0]
    block_cols = down_hbm.shape[1]
    gh_at = qkv_cols
    mix_at = qkv_cols + units_here
    act_at = mix_at + local_width
    row_tiles = rows // ROW_TILE

    barrier = pltpu.get_barrier_semaphore()
    for bit in bits + [1]:
        pl.semaphore_signal(barrier, inc=1, device_id={"dp": flip(me, bit)}, device_id_type=MESH)
    for other in (flip(level, 1), depth - 1 - level):
        pl.semaphore_signal(barrier, inc=1, device_id={"tensor": other}, device_id_type=MESH)
    pl.semaphore_wait(barrier, len(bits) + 3)

    units = [
        Unit(None, wqu, 0, (0, block_rows), (0, qkv_cols)),
        Unit(dense_hbm, wdd, 1, (0, local_width), (0, block_cols)),
    ]
    for q in range(PARTS):
        at = q * part_units
        units.append(Unit(up_hbm, wqu, 0, (0, block_rows), (at, part_units), col_at=qkv_cols + at))
        units.append(Unit(down_hbm, wdd, 1, (at, part_units), (0, block_cols),
                          row_at=local_width + at))

    def remote_dp(src, dst, ssem, rsem, peer):
        return pltpu.make_async_remote_copy(
            src_ref=src, dst_ref=dst, send_sem=ssem, recv_sem=rsem,
            device_id={"dp": peer}, device_id_type=MESH)

    def held(order, stage):
        owners = [me]
        for bit in order[:stage]:
            owners = owners + [flip(o, bit) for o in owners]
        return owners

    def stage_copies(u, stage):
        copies = []
        for path, order in enumerate(orders):
            for q, owner in enumerate(held(order, stage)):
                slot = path * per_path + 2 ** stage - 1 + q
                dst = units[u].block(owner, path)
                src = units[u].own(path) if stage == 0 and u else dst
                copies.append(remote_dp(
                    src, dst, send.at[u, slot], recv.at[u, slot], flip(me, order[stage])))
        return copies

    def core_copies(u, lo=0, hi=2 ** stages):
        copies = []
        for q, owner in list(enumerate(held(bits, stages)))[lo:hi]:
            dst = units[u].block(owner)
            src = units[u].own() if q == 0 and u else dst
            slot = 2 * per_path + q
            copies.append(remote_dp(src, dst, send.at[u, slot], recv.at[u, slot], flip(me, 1)))
        return copies

    def own_copies(u):
        if u:
            return [pltpu.make_async_copy(units[u].own(), units[u].block(me), local.at[u])]
        at = aligned(me * block_rows, block_rows)
        sems = [local.at[0], local.at[len(units) + 3], local.at[len(units) + 4]]
        return [
            pltpu.make_async_copy(
                qkv_hbm.at[j], wqu.at[at, pl.ds(j * local_width, local_width)], sems[j])
            for j in range(3)
        ]

    def start(u):
        for c in own_copies(u):
            c.start()
        if u == 0:
            for c in own_copies(u):
                c.wait()
        for c in stage_copies(u, 0):
            c.start()
        core_copies(u, 0, 1)[0].start()

    def advance(u, stage):
        if stage == 1 and u:
            for c in own_copies(u):
                c.wait()
        for c in stage_copies(u, stage - 1):
            c.wait_recv()
        for c in stage_copies(u, stage) if stage < stages else core_copies(u, 1):
            c.start()

    order_of_events = [(0, 1), (1, 1)]
    for u in range(len(units)):
        order_of_events.append((u, 2))
        if u + 2 < len(units):
            order_of_events.append((u + 2, 1))

    def event(e):
        u, stage = order_of_events[e]
        if stage == 1:
            advance(u, 1)
            if u + 2 < len(units):
                start(u + 2)
        else:
            for later in range(2, stages + 1):
                advance(u, later)

    def events_at(i, table):
        for when, which in table:
            @pl.when(i == when)
            def _():
                for e in which:
                    event(e)

    def finish(u):
        for c in core_copies(u):
            c.wait_recv()

    def drain(u):
        for stage in range(stages):
            for c in stage_copies(u, stage):
                c.wait_send()
        for c in core_copies(u):
            c.wait_send()

    x_at = acts.at[:, pl.ds(act_at, width)]

    def x_copy():
        return pltpu.make_async_copy(x_hbm, x_at, local.at[len(units)])

    cot_copy = pltpu.make_async_copy(cot_hbm, cot, local.at[len(units) + 1])
    x_copy().start()
    cot_copy.start()

    def vec_slot(i):
        return vec_in.at[aligned(i * 8, 8), :]

    def vector_copies(i):
        copies = []
        for q, owner in enumerate(held(bits + [1], i)):
            slot = 2 ** i - 1 + q
            copies.append(remote_dp(
                vec_slot(owner), vec_slot(owner),
                vsend.at[slot], vrecv.at[slot], flip(me, (bits + [1])[i])))
        return copies

    def chosen(shape, test):
        at, lane = (lax.broadcasted_iota(jnp.int32, shape, d) for d in (0, 1))
        return test(at, lane)

    start(1)
    start(0)
    vec_ref[...] = jnp.zeros_like(vec_ref)
    at = aligned(me * block_rows, block_rows)
    wide_rows = rows_ref[...].astype(F32)
    for j, row in enumerate((0, 1, 5, 6)):
        vec_ref[row : row + 1, at] = wide_rows[j : j + 1]
    step = HEAD // count
    key_step = ROT // count
    by_head = lambda r, lane: lane // HEAD == r
    up = up_shift_ref[...]
    near = jnp.where(chosen((up.shape[1], units_here), by_head), 1.0, 0.0).astype(BF16)
    spread = dot(up, near)
    keep = chosen(spread.shape, lambda r, lane: lane % HEAD == me * step + r)
    vec_ref[2:3, pl.ds(0, units_here)] = jnp.sum(jnp.where(keep, spread, 0.0), axis=0, keepdims=True)
    near = jnp.where(
        chosen((step, local_width), lambda r, lane: lane % HEAD == me * step + r), 1.0, 0.0
    ).astype(BF16)
    for j in range(2):
        spread = dot(qv_ref[j], near)
        kept = jnp.where(chosen(spread.shape, by_head), spread, 0.0)
        vec_ref[3:4, pl.ds(2 * j * local_width, local_width)] = jnp.sum(kept, axis=0, keepdims=True)
    keys = key_ref[...]
    near = jnp.where(chosen((keys.shape[1], local_width), by_head), 1.0, 0.0).astype(BF16)
    spread = dot(keys, near)
    keep = chosen(spread.shape, lambda r, lane: lane % HEAD == me * key_step + r)
    vec_ref[3:4, pl.ds(local_width, local_width)] = jnp.sum(
        jnp.where(keep, spread, 0.0), axis=0, keepdims=True)

    vec_slot(me)[...] = vec_ref[...]
    for i in range(stages + 1):
        for c in vector_copies(i):
            c.start()
        for c in vector_copies(i):
            c.wait_recv()
    total = vec_slot(0)[...]
    for owner in range(1, count):
        total = total + vec_slot(owner)[...]
    vec_ref[...] = total

    sums_ref[...] = jnp.zeros_like(sums_ref)
    x_copy().wait()
    cot_copy.wait()

    def norm_step(i, total):
        events_at(i, ((NORM_EVENTS[0], (0,)), (NORM_EVENTS[1], (1,))))
        at = aligned(i * NORM_ROWS, NORM_ROWS)
        wide = acts[at, pl.ds(act_at, width)].astype(F32)
        mean = jnp.mean(wide, axis=1, keepdims=True)
        centred = wide - mean
        var = jnp.mean(centred * centred, axis=1, keepdims=True)
        inv = lax.rsqrt(var + EPSILON)
        stats[at, 0:1] = mean
        stats[at, 1:2] = inv
        normed = centred * inv
        low[at, :] = (normed * vec_ref[0:1, :] + vec_ref[1:2, :]).astype(BF16)
        sums_ref[2:3, :] += jnp.sum(cot[at, :].astype(F32), axis=0, keepdims=True)
        return total

    lax.fori_loop(0, rows // NORM_ROWS, norm_step, 0)

    half = ROT // 2
    lane_in_head = lax.broadcasted_iota(jnp.int32, (SEQ, LANES), 1) % HEAD

    def segments_of(s):
        row = seg_ref[s].astype(F32)
        return row, jnp.transpose(jnp.broadcast_to(row, (LANES, SEQ)))[:, 0:1]

    def table_step(s, carry):
        row, column = segments_of(s)
        starts = jnp.sum(jnp.where(row < column, 1.0, 0.0), axis=1, keepdims=True)
        place = lax.broadcasted_iota(jnp.int32, (SEQ, 1), 0).astype(F32)
        angles = (place - starts) * inverse_ref[...]
        at = aligned(s * SEQ, SEQ)
        sine = jnp.sin(angles)
        tables[0, at, :] = jnp.where(lane_in_head < ROT, jnp.cos(angles), 1.0)
        tables[1, at, :] = jnp.where(
            lane_in_head < half, -sine, jnp.where(lane_in_head < ROT, sine, 0.0))
        return carry

    lax.fori_loop(0, rows // SEQ, table_step, 0)
    event(2)
    event(3)
    finish(0)


    def lane_is_leading(shape):
        lane = lax.broadcasted_iota(jnp.int32, shape, 1)
        return (lane % HEAD) < half

    def swap(t):
        size = t.shape[1]
        return jnp.where(
            lane_is_leading(t.shape), pltpu.roll(t, size - half, 1), pltpu.roll(t, half, 1))

    def qkv_step(i, carry):
        events_at(i, ((3, (4,)), (6, (5,)), (11, (6,))))
        tile = i // row_tiles
        at = aligned((i % row_tiles) * ROW_TILE, ROW_TILE)
        cols = aligned(tile * COL_TILE, COL_TILE)
        t = dot(low[at, :], wqu[:, cols]) + vec_ref[3:4, cols]
        wide = lambda j: jnp.concatenate([tables[j, at, :]] * (COL_TILE // LANES), axis=1)
        rotated = t * wide(0) + swap(t) * wide(1)
        is_value = tile >= 2 * local_width // COL_TILE
        acts[at, cols] = jnp.where(is_value, t, rotated).astype(BF16)
        return carry

    lax.fori_loop(0, row_tiles * qkv_cols // COL_TILE, qkv_step, 0)
    finish(1)

    def mixed_step(i, carry):
        at = aligned((i % row_tiles) * ROW_TILE, ROW_TILE)
        tile = i // row_tiles
        g = dot(cot[at, :], wdd[aligned(tile * COL_TILE, COL_TILE), :], 1, 1).astype(BF16)
        for j in range(COL_TILE // LANES):
            part[tile * (COL_TILE // LANES) + j, at, :] = g[:, j * LANES : (j + 1) * LANES]
        return carry

    lax.fori_loop(0, row_tiles * local_width // COL_TILE, mixed_step, 0)
    pairs = local_width // LANES
    event(7)

    def attention_step(i, carry):
        s, p = i // pairs, i % pairs
        at = aligned(s * SEQ, SEQ)
        lanes = [aligned(j * local_width + p * LANES, LANES) for j in range(3)]

        events_at(i, ((2, (8,)), (3, (9,)), (5, (10,)), (6, (11,)), (7, (12,))))

        @pl.when(p == 0)
        def _():
            across = lax.broadcasted_iota(jnp.int32, (SEQ, SEQ), 1)
            down = lax.broadcasted_iota(jnp.int32, (SEQ, SEQ), 0)
            row, column = segments_of(s)
            allowed = (column == row) & (down >= across)
            mask[...] = jnp.where(allowed, 0.0, NEGATIVE)

        q, k, v = [acts[at, l] for l in lanes]
        go = part[p, at, :]
        lane = lax.broadcasted_iota(jnp.int32, (SEQ, LANES), 1)
        zero = jnp.zeros((), BF16)
        total = None
        for h in range(LANES // HEAD):
            mine = (lane // HEAD) == h
            kh, vh, qh, gh = [jnp.where(mine, t, zero) for t in (k, v, q, go)]
            by_row, by_key = [], []
            for r in range(SEQ // QUERY_TILE):
                seen = (r + 1) * QUERY_TILE
                here = slice(r * QUERY_TILE, seen)
                scores = dot(q[here], kh[:seen], 1, 1) * SCALE + mask[here, :seen]
                top = jnp.max(scores, axis=1, keepdims=True)
                e = jnp.exp(scores - top)
                probs = e / jnp.sum(e, axis=1, keepdims=True)
                probs_low = probs.astype(BF16)
                gprobs = dot(go[here], vh[:seen], 1, 1)
                delta = jnp.sum(probs * gprobs, axis=1, keepdims=True)
                gs = (probs * (gprobs - delta) * SCALE).astype(BF16)
                by_row.append((dot(probs_low, vh[:seen]), dot(gs, kh[:seen])))
                keyed = (dot(gs, qh[here], 0, 0), dot(probs_low, gh[here], 0, 0))
                if by_key:
                    keyed = tuple(
                        jnp.concatenate([old + new[: old.shape[0]], new[old.shape[0] :]], axis=0)
                        for old, new in zip(by_key, keyed))
                by_key = keyed
            terms = [jnp.concatenate(t, axis=0) for t in zip(*by_row)] + list(by_key)
            total = terms if total is None else [a + b for a, b in zip(total, terms)]
        acts[at, aligned(mix_at + p * LANES, LANES)] = total[0].astype(BF16)

        def back(t):
            return t * tables[0, at, :] - swap(t) * tables[1, at, :]

        for j, g in enumerate((back(total[1]), back(total[2]), total[3])):
            acts[at, lanes[j]] = g.astype(BF16)
            sums_ref[4:5, lanes[j]] += jnp.sum(g, axis=0, keepdims=True)
        return carry

    lax.fori_loop(0, (rows // SEQ) * pairs, attention_step, 0)
    event(13)
    finish(2)
    finish(3)

    tiles = units_here // COL_TILE
    per_part = row_tiles * tiles // PARTS

    def ffn_step(i, carry):
        events_at(i, (
            (per_part, (14,)), (per_part + 2, (15,)), (2 * per_part, (16,)),
            (2 * per_part + 1, (17,)), (3 * per_part - 1, (18,)), (3 * per_part, (19,)),
        ))
        for q in range(1, PARTS):
            @pl.when(i == q * per_part)
            def _():
                finish(2 + 2 * q)
                finish(3 + 2 * q)

        at = aligned((i % row_tiles) * ROW_TILE, ROW_TILE)
        tile = i // row_tiles
        cols = aligned(tile * COL_TILE, COL_TILE)
        hidden = dot(low[at, :], wqu[:, aligned(qkv_cols + tile * COL_TILE, COL_TILE)])
        hidden = hidden + vec_ref[2:3, cols]
        grad = dot(cot[at, :], wdd[aligned(local_width + tile * COL_TILE, COL_TILE), :], 1, 1)
        square = hidden * hidden
        th = jnp.tanh(GELU_A * hidden * (1.0 + GELU_B * square))
        acts[at, aligned(act_at + tile * COL_TILE, COL_TILE)] = (
            0.5 * hidden * (1.0 + th)).astype(BF16)
        slope = 0.5 * (1.0 + th) + 0.5 * hidden * (1.0 - th * th) * (
            GELU_A * (1.0 + 3.0 * GELU_B * square))
        grad = grad * slope
        acts[at, aligned(gh_at + tile * COL_TILE, COL_TILE)] = grad.astype(BF16)
        sums_ref[3:4, cols] += jnp.sum(grad, axis=0, keepdims=True)
        return carry

    lax.fori_loop(0, row_tiles * tiles, ffn_step, 0)
    for u in range(len(units)):
        drain(u)
    for i in range(stages + 1):
        for c in vector_copies(i):
            c.wait_send()

    chunks = width // CHUNK
    every = 2 * chunks

    def remote_z(src, dst, ssem, rsem, peer):
        return pltpu.make_async_remote_copy(
            src_ref=src, dst_ref=dst, send_sem=ssem, recv_sem=rsem,
            device_id={"tensor": peer}, device_id_type=MESH)

    def columns(c):
        return aligned((c % chunks) * CHUNK, CHUNK)

    def copy_a(c):
        return remote_z(part.at[c % chunks], inbox.at[c % SLOTS], a_send.at[c % SLOTS],
                        a_recv.at[c % SLOTS], flip(level, 1))

    def copy_b(c):
        return remote_z(part.at[c % chunks], cross.at[c % SLOTS], b_send.at[c % SLOTS],
                        b_recv.at[c % SLOTS], depth - 1 - level)

    def copy_c_out(c):
        return remote_z(cross.at[c % SLOTS], inbox.at[c % SLOTS], c_send.at[c % SLOTS],
                        c_recv.at[c % SLOTS], flip(level, 1))

    def copy_c_grad(c):
        return remote_z(gn.at[:, columns(c)], gn.at[:, columns(c)], c_send.at[c % SLOTS],
                        c_recv.at[c % SLOTS], flip(level, 1))

    def out_copy(src, c):
        return pltpu.make_async_copy(src.at[c % SLOTS], block_out.at[:, columns(c)],
                                     z_out.at[c % SLOTS])

    gn_copy = pltpu.make_async_copy(x_hbm, gn, local.at[len(units) + 2])

    @pl.when(inner)
    def _():
        gn_copy.start()
        gn_copy.wait()

    add_rows = 256
    x_late = wqu.at[pl.ds(0, rows), pl.ds(0, width)]

    def by_rows(step):
        def body(i, carry):
            step(aligned(i * add_rows, add_rows))
            return carry
        lax.fori_loop(0, rows // add_rows, body, 0)

    def tick(k):
        @pl.when(inner & (k < every))
        def _():
            copy_a(k).wait_recv()

            def add(at):
                part[k % chunks, at, :] = (
                    part[k % chunks, at, :].astype(F32) + inbox[k % SLOTS, at, :].astype(F32)
                ).astype(BF16)

            by_rows(add)

            @pl.when(k >= SLOTS)
            def _():
                pl.semaphore_wait(credit, 1)

            copy_b(k).start()

        @pl.when(inner & (k >= 2) & (k < every + 2))
        def _():
            j = k - 2
            copy_b(j).wait_recv()
            copy_b(j).wait_send()

            @pl.when(j < chunks)
            def _():
                def add(at):
                    pair = part[j % chunks, at, :].astype(F32) + cross[j % SLOTS, at, :].astype(F32)
                    shifts = vec_ref[5:6, columns(j)], vec_ref[6:7, columns(j)]
                    wide = gn[at, columns(j)].astype(F32)
                    cross[j % SLOTS, at, :] = (wide + pair + shifts[0] + shifts[1]).astype(BF16)

                by_rows(add)
                copy_c_out(j).start()
                out_copy(cross, j).start()

            @pl.when(j >= chunks)
            def _():
                def add(at):
                    gn[at, columns(j)] = (
                        part[j % chunks, at, :].astype(F32) + cross[j % SLOTS, at, :].astype(F32)
                    ).astype(BF16)

                by_rows(add)
                copy_c_grad(j).start()

        @pl.when(inner & (k >= 4) & (k < every + 4))
        def _():
            i = k - 4

            @pl.when(i < chunks)
            def _():
                copy_c_out(i).wait_send()
                out_copy(cross, i).wait()

            @pl.when(i >= chunks)
            def _():
                copy_c_grad(i).wait_send()

            @pl.when(i < every - SLOTS)
            def _():
                pl.semaphore_signal(
                    credit, inc=1, device_id={"tensor": depth - 1 - level}, device_id_type=MESH)

        @pl.when(outer & (k >= 4) & (k < every + 4))
        def _():
            i = k - 4
            copy_a(i).wait_send()

            @pl.when(i < chunks)
            def _():
                copy_c_out(i).wait_recv()
                out_copy(inbox, i).start()
                out_copy(inbox, i).wait()

            @pl.when(i >= chunks)
            def _():
                copy_c_grad(i).wait_recv()

            @pl.when(i + SLOTS < every)
            def _():
                copy_a(i + SLOTS).start()

        @pl.when((k >= chunks + 4) & (k < every + 4))
        def _():
            cols = columns(k - 4)

            def gather_sums(at):
                g = gn[at, cols].astype(F32)
                normed = (x_late[at, cols].astype(F32) - stats[at, 0:1]) * stats[at, 1:2]
                product = g * normed
                gain = vec_ref[0:1, cols]
                tables[0, at, :] += g * gain
                tables[1, at, :] += product * gain
                sums_ref[0:1, cols] += jnp.sum(product, axis=0, keepdims=True)
                sums_ref[1:2, cols] += jnp.sum(g, axis=0, keepdims=True)

            by_rows(gather_sums)

    def ticks(lo, hi):
        def body(k, carry):
            tick(k)
            return carry
        lax.fori_loop(lo, hi, body, 0)

    def produce(first, tile, r, t):
        at = aligned(r * ROW_TILE, ROW_TILE)
        for j in range(COL_TILE // CHUNK):
            part[(first + tile * (COL_TILE // CHUNK) + j) % chunks, at, :] = (
                t[:, j * CHUNK : (j + 1) * CHUNK].astype(BF16))

    per_tile = COL_TILE // CHUNK

    def branch_step(i, carry):
        tile, r = i // row_tiles, i % row_tiles
        at = aligned(r * ROW_TILE, ROW_TILE)
        cols = aligned(tile * COL_TILE, COL_TILE)
        produce(0, tile, r, dot(acts[at, pl.ds(mix_at, local_width + units_here)], wdd[:, cols]))

        @pl.when(r == row_tiles - 1)
        def _():
            for j in range(per_tile):
                @pl.when(outer & (tile * per_tile + j < SLOTS))
                def _():
                    copy_a(tile * per_tile + j).start()

            @pl.when(tile % 4 == 3)
            def _():
                tick(tile // 4)

        return carry

    lax.fori_loop(0, row_tiles * width // COL_TILE, branch_step, 0)
    done_ticks = width // COL_TILE // 4

    grad_tiles = acts.shape[1] // GRAD_TILE
    low_tiles = mix_at // GRAD_TILE
    across = width // GRAD_TILE
    blocks = 2 ** stages
    staged = wdd.shape[0] // block_rows * across // grad_tiles * grad_tiles

    def stage_at(k, p=None):
        start, size = (0, block_rows) if p is None else (p * (block_rows // 2), block_rows // 2)
        at = aligned((k // across) * block_rows + start, size)
        return wdd.at[at, aligned((k % across) * GRAD_TILE, GRAD_TILE)]

    def relative(base, v):
        for i, bit in enumerate(bits):
            has = (v // 2 ** (stages - 1 - i)) % 2
            base = base + has * (bit - 2 * bit * ((base // bit) % 2))
        return base

    def turn(block):
        cols = aligned(block * block_rows, block_rows)
        turned[0] = jnp.transpose(low[:, cols])
        turned[1] = jnp.transpose(cot[:, cols])

    def grad_tile(n):
        return dot(turned[n // low_tiles], acts[:, aligned(n * GRAD_TILE, GRAD_TILE)])

    def core_copy(i):
        return remote_dp(stage_at(i % staged), core_rx.at[i], core_send.at[i % staged],
                         core_recv.at[i], flip(me, 1))

    def other_step(i, carry):
        n = i % grad_tiles

        @pl.when(n == 0)
        def _():
            turn(relative(flip(me, 1), blocks - 1 - i // grad_tiles))

        @pl.when(i >= staged)
        def _():
            core_copy(i - staged).wait_send()

        stage_at(i % staged)[...] = grad_tile(n).astype(BF16)
        core_copy(i).start()

        @pl.when(i % TICK_TILES == TICK_TILES - 1)
        def _():
            tick(done_ticks + i // TICK_TILES)

        return carry

    lax.fori_loop(0, blocks * grad_tiles, other_step, 0)
    done_ticks += blocks * grad_tiles // TICK_TILES

    def first_bit(v, order):
        for s, bit in enumerate(order):
            if v // 2 ** (stages - 1 - bits.index(bit)) % 2:
                return s
        return len(order)

    pieces = {}
    for v in range(blocks):
        for p, order in enumerate(orders):
            for s in range(first_bit(v, order)):
                pieces[(v, p, s)] = len(pieces)
    spare = staged

    def link_copy(v, p, n):
        order = orders[p]
        s = first_bit(v, order)
        left = v - 2 ** (stages - 1 - bits.index(order[s]))
        piece = pieces[(left, p, s)]
        return remote_dp(
            stage_at((blocks - 1 - v) * grad_tiles + n, p), link_rx.at[piece, n],
            link_send.at[2 * (v - 1) + p, n], link_recv.at[piece, n], flip(me, order[s]))

    def arrival(v, p, s, n):
        piece = pieces[(v, p, s)]
        return remote_dp(
            stage_at(0, p), link_rx.at[piece, n], link_send.at[0, 0], link_recv.at[piece, n],
            flip(me, orders[p][s]))

    def own_block(v, ticks_at):
        q = blocks - 1 - v
        mine = [key for key in pieces if key[0] == v]
        assert v == 0 or len(mine) < 2

        def core_slot(n):
            return stage_at(spare + n % DEPTH)

        def core_fetch(n):
            return pltpu.make_async_copy(
                core_rx.at[q * grad_tiles + n], core_slot(n), fetch_sem.at[n % DEPTH, 0])

        def piece_slot(key, n):
            _, p, s = key
            if v == 0:
                return stage_at((n % DEPTH) * stages + s, p)
            return spare_tiles.at[n % DEPTH]

        def piece_fetch(key, n):
            return pltpu.make_async_copy(
                link_rx.at[pieces[key], n], piece_slot(key, n),
                fetch_sem.at[n % DEPTH, 1 + mine.index(key)])

        def fetch(n):
            core_copy(q * grad_tiles + n).wait_recv()
            core_fetch(n).start()
            for key in mine:
                arrival(*key, n).wait_recv()
                piece_fetch(key, n).start()

        def grad_out(n):
            at = aligned((n % 2) * block_rows, block_rows)
            flat, tall = mask.at[at, :], mask.at[:, at]
            sem = grad_sem.at[n % 2]
            first = qkv_cols // GRAD_TILE
            each = local_width // GRAD_TILE
            last = low_tiles + local_width // GRAD_TILE
            cases = (
                (n < first, flat, lambda: qkv_out.at[n // each].at[
                    :, aligned((n % each) * GRAD_TILE, GRAD_TILE)]),
                ((n >= first) & (n < low_tiles), flat,
                 lambda: up_out.at[:, aligned((n - first) * GRAD_TILE, GRAD_TILE)]),
                ((n >= low_tiles) & (n < last), tall,
                 lambda: dense_out.at[aligned((n - low_tiles) * GRAD_TILE, GRAD_TILE), :]),
                (n >= last, tall,
                 lambda: down_out.at[aligned((n - last) * GRAD_TILE, GRAD_TILE), :]),
            )
            return [(c, pltpu.make_async_copy(src, dst(), sem)) for c, src, dst in cases]

        def for_out(n, act):
            for cond, copy in grad_out(n):
                @pl.when(cond)
                def _():
                    act(copy)

        turn(relative(me, v))
        if v == 0:
            for n in range(DEPTH * stages):
                for p in range(2):
                    link_copy(blocks - 1, p, n).wait_send()
        for n in range(DEPTH - 1):
            fetch(n)

        def step(n, carry):
            for when, k in ticks_at:
                @pl.when(n == when)
                def _():
                    tick(k)

            t = grad_tile(n)
            core_fetch(n).wait()
            t = t + core_slot(n)[...].astype(F32)
            for key in mine:
                piece_fetch(key, n).wait()
            for s in sorted({key[2] for key in mine}):
                sides = []
                for p in range(2):
                    rows_p = slice(p * (block_rows // 2), (p + 1) * (block_rows // 2))
                    side = t[rows_p]
                    if (v, p, s) in pieces:
                        side = side + piece_slot((v, p, s), n)[...].astype(F32)
                    sides.append(side)
                t = jnp.concatenate(sides, axis=0)
            if v:
                k = (blocks - 1 - v) * grad_tiles + n
                core_copy(k if v < blocks - 1 else k + staged).wait_send()
                stage_at(k)[...] = t.astype(BF16)
                for p in range(2):
                    link_copy(v, p, n).start()
            else:
                @pl.when((n >= 2) & (n != low_tiles + 1))
                def _():
                    for_out(n - 2, lambda c: c.wait())

                @pl.when(n == low_tiles)
                def _():
                    for_out(n - 1, lambda c: c.wait())

                @pl.when(n < low_tiles)
                def _():
                    mask[aligned((n % 2) * block_rows, block_rows), :] = t

                @pl.when(n >= low_tiles)
                def _():
                    mask[:, aligned((n % 2) * block_rows, block_rows)] = jnp.transpose(t)

                for_out(n, lambda c: c.start())

            @pl.when(n + DEPTH - 1 < grad_tiles)
            def _():
                fetch(n + DEPTH - 1)

            return carry

        lax.fori_loop(0, grad_tiles, step, 0)
        if v == 0:
            for n in (grad_tiles - 2, grad_tiles - 1):
                for cond, copy in grad_out(n):
                    if bool(cond):
                        copy.wait()

    own_block(blocks - 1, ((grad_tiles // 2, done_ticks),))
    done_ticks += 1
    before = done_ticks
    lag = SLOTS - 2 - per_tile

    def grad_step(i, carry):
        tile, r = i // row_tiles, i % row_tiles

        @pl.when(r == 0)
        def _():
            mid = width // COL_TILE // 2
            taken = ((tile > mid) & (tile < mid + blocks - 1)).astype(jnp.int32)
            until = lag + per_tile * (tile + 1)
            ticks(
                jnp.maximum(before, until - per_tile + taken),
                jnp.maximum(before, until),
            )

            for v in range(1, blocks - 1):
                @pl.when(tile == mid + blocks - 2 - v)
                def _():
                    own_block(v, ((grad_tiles // 2, until),))

        at = aligned(r * ROW_TILE, ROW_TILE)
        t = dot(acts[at, pl.ds(0, mix_at)], wqu[aligned(tile * COL_TILE, COL_TILE), :], 1, 1)
        produce(chunks, tile, r, t)
        return carry

    lax.fori_loop(0, row_tiles * width // COL_TILE, grad_step, 0)
    done_ticks = lag + per_tile * (width // COL_TILE)
    last_block = every - 4
    late_copy = pltpu.make_async_copy(x_hbm, x_late, local.at[len(units)])
    late_copy.start()
    tables[...] = jnp.zeros_like(tables)
    late_copy.wait()

    ticks(done_ticks, last_block)
    own_block(0, ((grad_tiles // 4, last_block), (3 * grad_tiles // 4, last_block + 1)))
    ticks(last_block + 2, every + 4)
    for v in range(1, blocks):
        for p in range(2):
            for n in range(grad_tiles):
                if v == blocks - 1 and n < DEPTH * stages:
                    continue
                link_copy(v, p, n).wait_send()

    def row_slot(i):
        return vec_in.at[aligned((i % 2) * BACK_ROWS, BACK_ROWS), :]

    def row_copy(i):
        return pltpu.make_async_copy(
            row_slot(i), input_grad.at[aligned(i * BACK_ROWS, BACK_ROWS), :], row_sem.at[i % 2])

    def back_step(i, carry):
        at = aligned(i * BACK_ROWS, BACK_ROWS)
        mean, inv = stats[at, 0:1], stats[at, 1:2]
        first = jnp.sum(tables[0, at, :], axis=1, keepdims=True) * (inv / width)
        second = jnp.sum(tables[1, at, :], axis=1, keepdims=True) * (inv * inv / width)
        scaled = gn[at, :].astype(F32) * vec_ref[0:1, :]
        grad = scaled * inv - (x_late[at, :].astype(F32) - mean) * second - first

        @pl.when(i >= 2)
        def _():
            row_copy(i - 2).wait()

        row_slot(i)[...] = grad + cot[at, :].astype(F32)
        row_copy(i).start()
        return carry

    back_steps = rows // BACK_ROWS

    def sum_copy(i, bit):
        return remote_dp(sums_ref, sum_in.at[i], sum_send.at[i], sum_recv.at[i], flip(me, bit))

    trips = bits + [1]
    for i, bit in enumerate(trips):
        copy = sum_copy(i, bit)
        copy.start()
        lax.fori_loop(back_steps * i // len(trips), back_steps * (i + 1) // len(trips), back_step, 0)
        copy.wait()
        sums_ref[...] = sums_ref[...] + sum_in[i]
    row_copy(back_steps - 2).wait()
    row_copy(back_steps - 1).wait()


def fits(shards, depth, local_width, block_cols):
    return (
        shards & (shards - 1) == 0 and len(link_bits(shards)) == 2 and depth == 4
        and block_cols % COL_TILE == 0 and local_width % GRAD_TILE == 0
    )


def layer(x, cot, qkv_share, dense_share, up_share, down_share, vectors, segments):
    rows, width = x.shape
    count = lax.axis_size("dp")
    local_width = dense_share.shape[0]
    units_here = up_share.shape[1]
    block_rows = up_share.shape[0]
    seqs = rows // SEQ
    links = len(link_bits(count))
    blocks = 2 ** links
    slots = 2 * (blocks - 1) + blocks
    acts_cols = 4 * local_width + 2 * units_here
    grad_tiles = acts_cols // GRAD_TILE
    pieces = 0
    for order in range(2):
        pieces += sum(blocks // 2 ** (s + 1) for s in range(links))
    staged = (local_width + units_here) // block_rows * (width // GRAD_TILE) // grad_tiles * grad_tiles
    chunks = width // CHUNK
    any_ = pl.BlockSpec(memory_space=pl.ANY)
    vmem = pl.BlockSpec(memory_space=pltpu.VMEM)
    b16 = lambda *s: jax.ShapeDtypeStruct(s, BF16)
    f32 = lambda *s: jax.ShapeDtypeStruct(s, F32)
    dma = lambda *s: pltpu.SemaphoreType.DMA(s)
    outs = pl.pallas_call(
        layer_body,
        in_specs=[any_] * 6 + [vmem] * 6,
        out_specs=[any_] * 8 + [vmem],
        out_shape=[
            b16(rows, width), f32(rows, width), f32(3, block_rows, local_width),
            f32(local_width, block_rows), f32(block_rows, units_here), f32(units_here, block_rows),
            b16(blocks * grad_tiles, block_rows, GRAD_TILE),
            b16(pieces, grad_tiles, block_rows // 2, GRAD_TILE), f32(8, width),
        ],
        scratch_shapes=[
            pltpu.VMEM((width, 3 * local_width + units_here), BF16),
            pltpu.VMEM((local_width + units_here, width), BF16),
            pltpu.VMEM((rows, acts_cols), BF16), pltpu.VMEM((rows, width), BF16),
            pltpu.VMEM((rows, width), BF16), pltpu.VMEM((SEQ, SEQ), F32),
            pltpu.VMEM((8, width), F32), pltpu.VMEM((8 * count, width), F32),
            pltpu.VMEM((2, block_rows, rows), BF16), pltpu.VMEM((rows, width), BF16),
            pltpu.VMEM((chunks, rows, CHUNK), BF16), pltpu.VMEM((SLOTS, rows, CHUNK), BF16),
            pltpu.VMEM((SLOTS, rows, CHUNK), BF16),
            pltpu.VMEM((2, rows, LANES), F32), pltpu.VMEM((rows, LANES), F32),
            pltpu.VMEM((DEPTH, block_rows // 2, GRAD_TILE), BF16), pltpu.VMEM((links + 1, 8, width), F32),
            dma(2 + 2 * PARTS, slots), dma(2 + 2 * PARTS, slots), dma(count - 1), dma(count - 1),
            dma(7 + 2 * PARTS),
            dma(SLOTS), dma(SLOTS), dma(SLOTS), dma(SLOTS), dma(SLOTS), dma(SLOTS), dma(SLOTS),
            pltpu.SemaphoreType.REGULAR,
            dma(staged), dma(blocks * grad_tiles), dma(2 * (blocks - 1), grad_tiles),
            dma(pieces, grad_tiles), dma(DEPTH, 1 + 2 * links), dma(2), dma(2),
            dma(links + 1), dma(links + 1),
        ],
        compiler_params=pltpu.CompilerParams(
            collective_id=0, has_side_effects=True, vmem_limit_bytes=67_043_328),
        cost_estimate=pl.CostEstimate(
            flops=18 * rows * width * (local_width + units_here), bytes_accessed=80_000_000,
            transcendentals=rows * units_here),
        name="layer",
    )(
        x, cot, qkv_share, dense_share, up_share, down_share, *vectors, INVERSE,
        segments.reshape(seqs, 1, SEQ),
    )
    return outs[:6] + outs[8:]


def gelu_tanh(inputs):
    return jax.nn.gelu(inputs, approximate=True)


def line_sum(part, finish):
    size = lax.axis_size("tensor")
    if size != 4:
        return finish(lax.psum(part, "tensor").astype(F32))
    index = lax.axis_index("tensor")
    inward = lax.ppermute(part, "tensor", [(0, 1), (3, 2)])
    pair = (part.astype(F32) + inward.astype(F32)).astype(BF16)
    other = lax.ppermute(pair, "tensor", [(1, 2), (2, 1)])
    done = finish(pair.astype(F32) + other.astype(F32))
    back = lax.ppermute(done, "tensor", [(1, 0), (2, 3)])
    return jnp.where((index == 0) | (index == size - 1), back, done)


def local(
    block_input, segments, norm_gain, norm_bias, qkv_weight, query_value_bias, key_bias,
    dense_weight, dense_bias, up_weight, up_bias, down_weight, down_bias, cotangent,
):
    rows, width = block_input.shape
    local_width = qkv_weight.shape[2]
    heads = local_width // HEAD
    seqs = rows // SEQ
    shards = lax.axis_size("dp")
    fused = fits(shards, lax.axis_size("tensor"), local_width, down_weight.shape[1])
    if fused:
        mine = lax.axis_index("dp")
        four = jnp.stack([norm_gain, norm_bias, dense_bias, down_bias])
        block_output, input_grad, qkv_out, dense_out, up_out, down_out, total = layer(
            block_input, cotangent, qkv_weight.transpose(1, 0, 2), dense_weight, up_weight,
            down_weight, [four, up_bias.T, query_value_bias, key_bias.T], segments)

        def mine_of(value, lead):
            return lax.dynamic_index_in_dim(
                value.reshape(lead, shards, -1), mine, axis=1, keepdims=False)

        sums = total[4]
        qv_sums = jnp.stack([sums[:local_width], sums[2 * local_width : 3 * local_width]])
        key_sums = sums[local_width : 2 * local_width].reshape(heads, HEAD)[:, :ROT]
        bias_out = mine_of(total[2], 1).reshape(-1)
        return (
            block_output, input_grad, mine_of(total[0], 1).reshape(-1),
            mine_of(total[1], 1).reshape(-1), qkv_out.transpose(1, 0, 2),
            mine_of(qv_sums, 2 * heads).reshape(query_value_bias.shape),
            mine_of(key_sums, heads), dense_out, bias_out, up_out,
            mine_of(total[3], up_bias.shape[0]), down_out, bias_out,
        )
    smalls = (norm_gain, norm_bias, dense_bias, down_bias, up_bias, query_value_bias, key_bias)
    packed = jnp.concatenate([s.reshape(1, -1) for s in smalls], axis=1)
    packed = lax.all_gather(packed, "dp", axis=0, tiled=True)
    pieces = []
    at = 0
    for s in smalls:
        pieces.append(packed[:, at : at + s.size].reshape((shards,) + s.shape).astype(F32))
        at += s.size
    gain, shift, dense_shift, down_shift = [p.reshape(1, -1) for p in pieces[:4]]
    up_shift = pieces[4].transpose(1, 0, 2).reshape(1, -1)
    qv_bias = pieces[5].transpose(1, 2, 0, 3).reshape(2, local_width)
    key_part = pieces[6].transpose(1, 0, 2).reshape(heads, ROT)
    key_full = jnp.concatenate([key_part, jnp.zeros((heads, HEAD - ROT), F32)], axis=1)
    bias = jnp.concatenate(
        [qv_bias[0:1], key_full.reshape(1, -1), qv_bias[1:2], jnp.zeros((5, local_width), F32)], axis=0
    )

    dense_all = lax.all_gather(dense_weight, "dp", axis=1, tiled=True)
    qkv_all = lax.all_gather(qkv_weight.reshape(qkv_weight.shape[0], -1), "dp", axis=0, tiled=True)
    up_all = lax.all_gather(up_weight, "dp", axis=0, tiled=True)
    down_all = lax.all_gather(down_weight, "dp", axis=1, tiled=True)

    wide = block_input.astype(F32)
    mean = jnp.mean(wide, axis=1, keepdims=True)
    centred = wide - mean
    inv_std = lax.rsqrt(jnp.mean(centred * centred, axis=1, keepdims=True) + EPSILON)
    normed = centred * inv_std
    low = (normed * gain + shift).astype(BF16)

    tables = rotary_tables(segments)
    grad_mixed = dot(cotangent, dense_all, 1, 1).astype(BF16)
    projected = dot(low, qkv_all)
    mixed, grad_projected, bias_sums = attention(projected, grad_mixed, bias, tables, segments)
    bias_sums = jnp.sum(bias_sums, axis=0)

    hidden = dot(low, up_all) + up_shift
    activated, gelu_back = jax.vjp(gelu_tanh, hidden)
    activated = activated.astype(BF16)
    grad_hidden = gelu_back(dot(cotangent, down_all, 1, 1))[0]
    grad_up_bias = jnp.sum(grad_hidden, axis=0)
    grad_hidden_low = grad_hidden.astype(BF16)
    grad_joined = jnp.concatenate([grad_projected[i] for i in range(3)], axis=1)

    branches = (dot(mixed, dense_all) + dot(activated, down_all)).astype(BF16)
    grad_part = (dot(grad_joined, qkv_all, 1, 1) + dot(grad_hidden_low, up_all, 1, 1)).astype(BF16)
    grad_dense = dot(mixed, cotangent, 0, 0).astype(BF16)
    grad_qkv = dot(low, grad_joined, 0, 0).astype(BF16)
    grad_down = dot(activated, cotangent, 0, 0).astype(BF16)
    grad_up = dot(low, grad_hidden_low, 0, 0).astype(BF16)

    outs, grads = [], []
    for s in range(seqs):
        at = slice(s * SEQ, (s + 1) * SEQ)
        outs.append(
            line_sum(
                branches[at],
                lambda t, at=at: (wide[at] + t + dense_shift + down_shift).astype(BF16),
            )
        )
    for s in range(seqs):
        at = slice(s * SEQ, (s + 1) * SEQ)
        grads.append(line_sum(grad_part[at], lambda t: t.astype(BF16)))
    block_output = jnp.concatenate(outs, axis=0)
    grad_normed = jnp.concatenate(grads, axis=0).astype(F32)

    grad_wide = cotangent.astype(F32)
    scaled = grad_normed * gain
    input_grad = (
        inv_std
        * (
            scaled
            - jnp.mean(scaled, axis=1, keepdims=True)
            - normed * jnp.mean(scaled * normed, axis=1, keepdims=True)
        )
        + grad_wide
    )

    def scatter(value, dim):
        return lax.psum_scatter(value, "dp", scatter_dimension=dim, tiled=True).astype(F32)

    qkv_out = scatter(grad_qkv, 0).reshape(qkv_weight.shape)
    dense_out = scatter(grad_dense, 1)
    up_out = scatter(grad_up, 0)
    down_out = scatter(grad_down, 1)

    key_sums = bias_sums[1].reshape(heads, HEAD)[:, :ROT]
    qv_sums = jnp.stack([bias_sums[0], bias_sums[2]]).reshape(2, heads, HEAD)
    small_sums = (
        jnp.sum(grad_normed * normed, axis=0).reshape(shards, -1),
        jnp.sum(grad_normed, axis=0).reshape(shards, -1),
        jnp.sum(grad_wide, axis=0).reshape(shards, -1),
        grad_up_bias.reshape(up_bias.shape[0], shards, -1).transpose(1, 0, 2).reshape(shards, -1),
        qv_sums.reshape(2, heads, shards, -1).transpose(2, 0, 1, 3).reshape(shards, -1),
        key_sums.reshape(heads, shards, -1).transpose(1, 0, 2).reshape(shards, -1),
    )
    total = lax.psum_scatter(
        jnp.concatenate(small_sums, axis=1), "dp", scatter_dimension=0, tiled=True
    ).reshape(-1)
    shapes = (norm_gain.shape, norm_bias.shape, dense_bias.shape, up_bias.shape,
              query_value_bias.shape, key_bias.shape)
    smalls_out = []
    at = 0
    for part, shape in zip(small_sums, shapes):
        smalls_out.append(total[at : at + part.shape[1]].reshape(shape))
        at += part.shape[1]
    gain_out, shift_out, bias_out, up_bias_out, qv_out, key_out = smalls_out
    return (
        block_output, input_grad, gain_out, shift_out, qkv_out, qv_out, key_out, dense_out,
        bias_out, up_out, up_bias_out, down_out, bias_out,
    )


def solution(mesh):
    in_specs = (
        P("dp", None),
        P("dp"),
        P("dp"),
        P("dp"),
        P("dp", None, "tensor"),
        P(None, "tensor", "dp"),
        P("tensor", "dp"),
        P("tensor", "dp"),
        P("dp"),
        P("dp", "tensor"),
        P("tensor", "dp"),
        P("tensor", "dp"),
        P("dp"),
        P("dp", None),
    )
    out_specs = (
        P("dp", None),
        P("dp", None),
        P("dp"),
        P("dp"),
        P("dp", None, "tensor"),
        P(None, "tensor", "dp"),
        P("tensor", "dp"),
        P("tensor", "dp"),
        P("dp"),
        P("dp", "tensor"),
        P("tensor", "dp"),
        P("tensor", "dp"),
        P("dp"),
    )
    return jax.shard_map(local, mesh=mesh, in_specs=in_specs, out_specs=out_specs, check_vma=False)
```

```python
import functools

import jax
import jax.numpy as jnp
import numpy as np
from jax import lax
from jax.experimental import pallas as pl
from jax.experimental.pallas import tpu as pltpu
from jax.sharding import PartitionSpec as P

HEAD = 64
ROT = 32
SEQ = 512
LANES = 128
EPSILON = 1e-05
SCALE = 0.125
NEGATIVE = -1e30

F32 = jnp.float32
BF16 = jnp.bfloat16


def dot(a, b, ca=1, cb=0):
    return lax.dot_general(a, b, (((ca,), (cb,)), ((), ())), preferred_element_type=F32)


def rotary_tables(segments):
    seg_rows = segments.reshape(-1, SEQ)
    position = jnp.arange(SEQ, dtype=jnp.int32)
    starting = jnp.concatenate(
        [jnp.ones((seg_rows.shape[0], 1), dtype=jnp.bool_), seg_rows[:, 1:] != seg_rows[:, :-1]],
        axis=1,
    )
    starts = lax.cummax(jnp.where(starting, position[None, :], jnp.int32(0)), axis=1)
    offset = (position[None, :] - starts).astype(F32).reshape(-1, 1)
    half = ROT // 2
    lane = jnp.arange(LANES, dtype=jnp.int32) % HEAD
    inverse = 10000.0 ** (-((lane % half).astype(F32) * (2.0 / ROT)))
    angles = offset * inverse[None, :]
    cosine = jnp.where(lane < ROT, jnp.cos(angles), 1.0)
    sine = jnp.sin(angles)
    return (
        cosine,
        jnp.where(lane < half, -sine, 0.0),
        jnp.where((lane >= half) & (lane < ROT), sine, 0.0),
    )


def attention_body(
    q_ref, k_ref, v_ref, go_ref, bias_ref, cos_ref, sa_ref, sb_ref, segc_ref, segr_ref,
    mixed_ref, gp_ref, gb_ref, mask_ref,
):
    half = ROT // 2

    def rotate(t, direction):
        swapped = pltpu.roll(t, LANES - half, 1) * sa_ref[...]
        swapped = swapped + pltpu.roll(t, half, 1) * sb_ref[...]
        return t * cos_ref[...] + direction * swapped

    @pl.when(pl.program_id(1) == 0)
    def _():
        rows = lax.broadcasted_iota(jnp.int32, (SEQ, SEQ), 0)
        cols = lax.broadcasted_iota(jnp.int32, (SEQ, SEQ), 1)
        allowed = (segc_ref[...] == segr_ref[0]) & (rows >= cols)
        mask_ref[...] = jnp.where(allowed, 0.0, NEGATIVE)

    q = rotate(q_ref[...] + bias_ref[0:1, :], 1.0).astype(BF16)
    k = rotate(k_ref[...] + bias_ref[1:2, :], 1.0).astype(BF16)
    v = (v_ref[...] + bias_ref[2:3, :]).astype(BF16)
    go = go_ref[...]
    lane = lax.broadcasted_iota(jnp.int32, (SEQ, LANES), 1)
    mixed = gq = gk = gv = None
    for h in range(LANES // HEAD):
        mine = (lane // HEAD) == h
        zero = jnp.zeros((), BF16)
        kh = jnp.where(mine, k, zero)
        vh = jnp.where(mine, v, zero)
        qh = jnp.where(mine, q, zero)
        gh = jnp.where(mine, go, zero)
        s = dot(q, kh, 1, 1) * SCALE + mask_ref[...]
        top = jnp.max(s, axis=1, keepdims=True)
        e = jnp.exp(s - top)
        p = e / jnp.sum(e, axis=1, keepdims=True)
        low = p.astype(BF16)
        dp = dot(go, vh, 1, 1)
        delta = jnp.sum(p * dp, axis=1, keepdims=True)
        ds = (p * (dp - delta) * SCALE).astype(BF16)
        terms = (dot(low, vh), dot(ds, kh), dot(ds, qh, 0, 0), dot(low, gh, 0, 0))
        if h == 0:
            mixed, gq, gk, gv = terms
        else:
            mixed, gq, gk, gv = [a + b for a, b in zip((mixed, gq, gk, gv), terms)]
    mixed_ref[...] = mixed.astype(BF16)
    gq = rotate(gq, -1.0)
    gk = rotate(gk, -1.0)
    for i, g in enumerate((gq, gk, gv)):
        gp_ref[i] = g.astype(BF16)
        gb_ref[0, i : i + 1, :] = jnp.sum(g, axis=0, keepdims=True)


def attention(projected, grad_mixed, bias, tables, segments):
    rows = projected.shape[0]
    width = projected.shape[1] // 3
    seqs, pairs = rows // SEQ, width // LANES
    tile = lambda f: pl.BlockSpec((SEQ, LANES), f)
    table = tile(lambda s, p: (s, 0))
    return pl.pallas_call(
        attention_body,
        grid=(seqs, pairs),
        in_specs=[
            tile(lambda s, p: (s, p)),
            tile(lambda s, p: (s, pairs + p)),
            tile(lambda s, p: (s, 2 * pairs + p)),
            tile(lambda s, p: (s, p)),
            pl.BlockSpec((8, LANES), lambda s, p: (0, p)),
            table, table, table,
            pl.BlockSpec((SEQ, 1), lambda s, p: (s, 0)),
            pl.BlockSpec((1, 1, SEQ), lambda s, p: (s, 0, 0)),
        ],
        out_specs=[
            tile(lambda s, p: (s, p)),
            pl.BlockSpec((3, SEQ, LANES), lambda s, p: (0, s, p)),
            pl.BlockSpec((1, 8, LANES), lambda s, p: (s, 0, p)),
        ],
        out_shape=[
            jax.ShapeDtypeStruct((rows, width), BF16),
            jax.ShapeDtypeStruct((3, rows, width), BF16),
            jax.ShapeDtypeStruct((seqs, 8, width), F32),
        ],
        scratch_shapes=[pltpu.VMEM((SEQ, SEQ), F32)],
        compiler_params=pltpu.CompilerParams(dimension_semantics=("arbitrary", "arbitrary")),
        cost_estimate=pl.CostEstimate(
            flops=14 * rows * SEQ * width, bytes_accessed=24 * rows * width,
            transcendentals=rows * SEQ * width // HEAD,
        ),
        name="attention",
    )(
        projected, projected, projected, grad_mixed, bias, *tables,
        segments.reshape(rows, 1), segments.reshape(seqs, 1, SEQ),
    )


ROW_TILE = 512
QUERY_TILE = 256
COL_TILE = 256
GRAD_TILE = 512
CHUNK = 128
SLOTS = 8
NORM_ROWS = 32
NORM_EVENTS = (4, 10)
BACK_ROWS = 32
PARTS = 4
DEPTH = 4
TICK_TILES = 12
GELU_A = 0.7978845608028654
GELU_B = 0.044715
MESH = pl.DeviceIdType.MESH
INVERSE = np.asarray(
    10000.0 ** (-(np.arange(LANES) % (ROT // 2)) * (2.0 / ROT)), np.float32).reshape(1, LANES)


def flip(index, bit):
    return index + bit - 2 * bit * ((index // bit) % 2)


def link_bits(count):
    bits = []
    bit = count // 2
    while bit >= 2:
        bits.append(bit)
        bit //= 2
    return bits


def aligned(start, size):
    return pl.ds(pl.multiple_of(start, size), size)


class Unit:
    def __init__(self, share, whole, axis, rows, cols, row_at=0, col_at=0):
        self.share, self.whole, self.axis = share, whole, axis
        self.row0, self.rows = rows
        self.col0, self.cols = cols
        self.row_at, self.col_at = row_at, col_at

    def span(self, half):
        return (0, self.rows) if half is None else (half * (self.rows // 2), self.rows // 2)

    def own(self, half=None):
        start, size = self.span(half)
        return self.share.at[pl.ds(self.row0 + start, size), pl.ds(self.col0, self.cols)]

    def block(self, which, half=None):
        start, size = self.span(half)
        if self.axis == 0:
            rows = aligned(which * self.rows + start, size)
            return self.whole.at[rows, pl.ds(self.col_at, self.cols)]
        cols = aligned(which * self.cols, self.cols)
        return self.whole.at[pl.ds(self.row_at + start, size), cols]


def layer_body(
    x_hbm, cot_hbm, qkv_hbm, dense_hbm, up_hbm, down_hbm, rows_ref, up_shift_ref, qv_ref, key_ref, inverse_ref, seg_ref,
    block_out, input_grad, qkv_out, dense_out, up_out, down_out, core_rx, link_rx, sums_ref, mine_ref,
    wqu, wdd, acts, low, cot, mask, vec_ref, vec_in, turned, gn, part, inbox, cross,
    tables, stats, spare_tiles, sum_in,
    send, recv, vsend, vrecv, local,
    a_send, a_recv, b_send, b_recv, c_send, c_recv, z_out, credit,
    core_send, core_recv, link_send, link_recv, fetch_sem, grad_sem, row_sem, sum_send, sum_recv,
):
    count = lax.axis_size("dp")
    me = lax.axis_index("dp")
    depth = lax.axis_size("tensor")
    level = lax.axis_index("tensor")
    outer = (level == 0) | (level == depth - 1)
    inner = jnp.logical_not(outer)
    bits = link_bits(count)
    orders = (bits, bits[::-1])
    stages = len(bits)
    per_path = 2 ** stages - 1
    rows, width = low.shape
    units_here = up_hbm.shape[1]
    local_width = dense_hbm.shape[0]
    qkv_cols = 3 * local_width
    part_units = units_here // PARTS
    block_rows = up_hbm.shape[0]
    block_cols = down_hbm.shape[1]
    gh_at = qkv_cols
    mix_at = qkv_cols + units_here
    act_at = mix_at + local_width
    row_tiles = rows // ROW_TILE

    barrier = pltpu.get_barrier_semaphore()
    for bit in bits + [1]:
        pl.semaphore_signal(barrier, inc=1, device_id={"dp": flip(me, bit)}, device_id_type=MESH)
    for other in (flip(level, 1), depth - 1 - level):
        pl.semaphore_signal(barrier, inc=1, device_id={"tensor": other}, device_id_type=MESH)
    pl.semaphore_wait(barrier, len(bits) + 3)

    units = [
        Unit(None, wqu, 0, (0, block_rows), (0, qkv_cols)),
        Unit(dense_hbm, wdd, 1, (0, local_width), (0, block_cols)),
    ]
    for q in range(PARTS):
        at = q * part_units
        units.append(Unit(up_hbm, wqu, 0, (0, block_rows), (at, part_units), col_at=qkv_cols + at))
        units.append(Unit(down_hbm, wdd, 1, (at, part_units), (0, block_cols),
                          row_at=local_width + at))

    def remote_dp(src, dst, ssem, rsem, peer):
        return pltpu.make_async_remote_copy(
            src_ref=src, dst_ref=dst, send_sem=ssem, recv_sem=rsem,
            device_id={"dp": peer}, device_id_type=MESH)

    def held(order, stage):
        owners = [me]
        for bit in order[:stage]:
            owners = owners + [flip(o, bit) for o in owners]
        return owners

    def stage_copies(u, stage):
        copies = []
        for path, order in enumerate(orders):
            for q, owner in enumerate(held(order, stage)):
                slot = path * per_path + 2 ** stage - 1 + q
                dst = units[u].block(owner, path)
                src = units[u].own(path) if stage == 0 and u else dst
                copies.append(remote_dp(
                    src, dst, send.at[u, slot], recv.at[u, slot], flip(me, order[stage])))
        return copies

    def core_copies(u, lo=0, hi=2 ** stages):
        copies = []
        for q, owner in list(enumerate(held(bits, stages)))[lo:hi]:
            dst = units[u].block(owner)
            src = units[u].own() if q == 0 and u else dst
            slot = 2 * per_path + q
            copies.append(remote_dp(src, dst, send.at[u, slot], recv.at[u, slot], flip(me, 1)))
        return copies

    def own_copies(u):
        if u:
            return [pltpu.make_async_copy(units[u].own(), units[u].block(me), local.at[u])]
        at = aligned(me * block_rows, block_rows)
        sems = [local.at[0], local.at[len(units) + 3], local.at[len(units) + 4]]
        return [
            pltpu.make_async_copy(
                qkv_hbm.at[j], wqu.at[at, pl.ds(j * local_width, local_width)], sems[j])
            for j in range(3)
        ]

    def start(u):
        for c in own_copies(u):
            c.start()
        if u == 0:
            for c in own_copies(u):
                c.wait()
        for c in stage_copies(u, 0):
            c.start()
        core_copies(u, 0, 1)[0].start()

    def advance(u, stage):
        if stage == 1 and u:
            for c in own_copies(u):
                c.wait()
        for c in stage_copies(u, stage - 1):
            c.wait_recv()
        for c in stage_copies(u, stage) if stage < stages else core_copies(u, 1):
            c.start()

    order_of_events = [(0, 1), (1, 1)]
    for u in range(len(units)):
        order_of_events.append((u, 2))
        if u + 2 < len(units):
            order_of_events.append((u + 2, 1))

    def event(e):
        u, stage = order_of_events[e]
        if stage == 1:
            advance(u, 1)
            if u + 2 < len(units):
                start(u + 2)
        else:
            for later in range(2, stages + 1):
                advance(u, later)

    def events_at(i, table):
        for when, which in table:
            @pl.when(i == when)
            def _():
                for e in which:
                    event(e)

    def finish(u):
        for c in core_copies(u):
            c.wait_recv()

    def drain(u):
        for stage in range(stages):
            for c in stage_copies(u, stage):
                c.wait_send()
        for c in core_copies(u):
            c.wait_send()

    x_at = acts.at[:, pl.ds(act_at, width)]

    def x_copy():
        return pltpu.make_async_copy(x_hbm, x_at, local.at[len(units)])

    cot_copy = pltpu.make_async_copy(cot_hbm, cot, local.at[len(units) + 1])
    x_copy().start()
    cot_copy.start()

    def vec_slot(i):
        return vec_in.at[aligned(i * 8, 8), :]

    def vector_copies(i):
        copies = []
        for q, owner in enumerate(held(bits + [1], i)):
            slot = 2 ** i - 1 + q
            copies.append(remote_dp(
                vec_slot(owner), vec_slot(owner),
                vsend.at[slot], vrecv.at[slot], flip(me, (bits + [1])[i])))
        return copies

    def chosen(shape, test):
        at, lane = (lax.broadcasted_iota(jnp.int32, shape, d) for d in (0, 1))
        return test(at, lane)

    start(1)
    start(0)
    vec_ref[...] = jnp.zeros_like(vec_ref)
    at = aligned(me * block_rows, block_rows)
    wide_rows = rows_ref[...].astype(F32)
    for j, row in enumerate((0, 1, 5, 6)):
        vec_ref[row : row + 1, at] = wide_rows[j : j + 1]
    step = HEAD // count
    key_step = ROT // count
    by_head = lambda r, lane: lane // HEAD == r
    up = up_shift_ref[...]
    near = jnp.where(chosen((up.shape[1], units_here), by_head), 1.0, 0.0).astype(BF16)
    spread = dot(up, near)
    keep = chosen(spread.shape, lambda r, lane: lane % HEAD == me * step + r)
    vec_ref[2:3, pl.ds(0, units_here)] = jnp.sum(jnp.where(keep, spread, 0.0), axis=0, keepdims=True)
    near = jnp.where(
        chosen((step, local_width), lambda r, lane: lane % HEAD == me * step + r), 1.0, 0.0
    ).astype(BF16)
    for j in range(2):
        spread = dot(qv_ref[j], near)
        kept = jnp.where(chosen(spread.shape, by_head), spread, 0.0)
        vec_ref[3:4, pl.ds(2 * j * local_width, local_width)] = jnp.sum(kept, axis=0, keepdims=True)
    keys = key_ref[...]
    near = jnp.where(chosen((keys.shape[1], local_width), by_head), 1.0, 0.0).astype(BF16)
    spread = dot(keys, near)
    keep = chosen(spread.shape, lambda r, lane: lane % HEAD == me * key_step + r)
    vec_ref[3:4, pl.ds(local_width, local_width)] = jnp.sum(
        jnp.where(keep, spread, 0.0), axis=0, keepdims=True)

    vec_slot(me)[...] = vec_ref[...]
    for i in range(stages + 1):
        for c in vector_copies(i):
            c.start()
        for c in vector_copies(i):
            c.wait_recv()
    total = vec_slot(0)[...]
    for owner in range(1, count):
        total = total + vec_slot(owner)[...]
    vec_ref[...] = total

    sums_ref[...] = jnp.zeros_like(sums_ref)
    x_copy().wait()
    cot_copy.wait()

    def norm_step(i, total):
        events_at(i, ((NORM_EVENTS[0], (0,)), (NORM_EVENTS[1], (1,))))
        at = aligned(i * NORM_ROWS, NORM_ROWS)
        wide = acts[at, pl.ds(act_at, width)].astype(F32)
        mean = jnp.mean(wide, axis=1, keepdims=True)
        centred = wide - mean
        var = jnp.mean(centred * centred, axis=1, keepdims=True)
        inv = lax.rsqrt(var + EPSILON)
        stats[at, 0:1] = mean
        stats[at, 1:2] = inv
        normed = centred * inv
        low[at, :] = (normed * vec_ref[0:1, :] + vec_ref[1:2, :]).astype(BF16)
        sums_ref[2:3, :] += jnp.sum(cot[at, :].astype(F32), axis=0, keepdims=True)
        return total

    lax.fori_loop(0, rows // NORM_ROWS, norm_step, 0)

    half = ROT // 2
    lane_in_head = lax.broadcasted_iota(jnp.int32, (SEQ, LANES), 1) % HEAD

    def segments_of(s):
        row = seg_ref[s].astype(F32)
        return row, jnp.transpose(jnp.broadcast_to(row, (LANES, SEQ)))[:, 0:1]

    def table_step(s, carry):
        row, column = segments_of(s)
        starts = jnp.sum(jnp.where(row < column, 1.0, 0.0), axis=1, keepdims=True)
        place = lax.broadcasted_iota(jnp.int32, (SEQ, 1), 0).astype(F32)
        angles = (place - starts) * inverse_ref[...]
        at = aligned(s * SEQ, SEQ)
        sine = jnp.sin(angles)
        tables[0, at, :] = jnp.where(lane_in_head < ROT, jnp.cos(angles), 1.0)
        tables[1, at, :] = jnp.where(
            lane_in_head < half, -sine, jnp.where(lane_in_head < ROT, sine, 0.0))
        return carry

    lax.fori_loop(0, rows // SEQ, table_step, 0)
    event(2)
    event(3)
    finish(0)


    def lane_is_leading(shape):
        lane = lax.broadcasted_iota(jnp.int32, shape, 1)
        return (lane % HEAD) < half

    def swap(t):
        size = t.shape[1]
        return jnp.where(
            lane_is_leading(t.shape), pltpu.roll(t, size - half, 1), pltpu.roll(t, half, 1))

    def qkv_step(i, carry):
        events_at(i, ((3, (4,)), (6, (5,)), (11, (6,))))
        tile = i // row_tiles
        at = aligned((i % row_tiles) * ROW_TILE, ROW_TILE)
        cols = aligned(tile * COL_TILE, COL_TILE)
        t = dot(low[at, :], wqu[:, cols]) + vec_ref[3:4, cols]
        wide = lambda j: jnp.concatenate([tables[j, at, :]] * (COL_TILE // LANES), axis=1)
        rotated = t * wide(0) + swap(t) * wide(1)
        is_value = tile >= 2 * local_width // COL_TILE
        acts[at, cols] = jnp.where(is_value, t, rotated).astype(BF16)
        return carry

    lax.fori_loop(0, row_tiles * qkv_cols // COL_TILE, qkv_step, 0)
    finish(1)

    def mixed_step(i, carry):
        at = aligned((i % row_tiles) * ROW_TILE, ROW_TILE)
        tile = i // row_tiles
        g = dot(cot[at, :], wdd[aligned(tile * COL_TILE, COL_TILE), :], 1, 1).astype(BF16)
        for j in range(COL_TILE // LANES):
            part[tile * (COL_TILE // LANES) + j, at, :] = g[:, j * LANES : (j + 1) * LANES]
        return carry

    lax.fori_loop(0, row_tiles * local_width // COL_TILE, mixed_step, 0)
    pairs = local_width // LANES
    event(7)

    def attention_step(i, carry):
        s, p = i // pairs, i % pairs
        at = aligned(s * SEQ, SEQ)
        lanes = [aligned(j * local_width + p * LANES, LANES) for j in range(3)]

        events_at(i, ((2, (8,)), (3, (9,)), (5, (10,)), (6, (11,)), (7, (12,))))

        @pl.when(p == 0)
        def _():
            across = lax.broadcasted_iota(jnp.int32, (SEQ, SEQ), 1)
            down = lax.broadcasted_iota(jnp.int32, (SEQ, SEQ), 0)
            row, column = segments_of(s)
            allowed = (column == row) & (down >= across)
            mask[...] = jnp.where(allowed, 0.0, NEGATIVE)

        q, k, v = [acts[at, l] for l in lanes]
        go = part[p, at, :]
        lane = lax.broadcasted_iota(jnp.int32, (SEQ, LANES), 1)
        zero = jnp.zeros((), BF16)
        total = None
        for h in range(LANES // HEAD):
            mine = (lane // HEAD) == h
            kh, vh, qh, gh = [jnp.where(mine, t, zero) for t in (k, v, q, go)]
            by_row, by_key = [], []
            for r in range(SEQ // QUERY_TILE):
                seen = (r + 1) * QUERY_TILE
                here = slice(r * QUERY_TILE, seen)
                scores = dot(q[here], kh[:seen], 1, 1) * SCALE + mask[here, :seen]
                top = jnp.max(scores, axis=1, keepdims=True)
                e = jnp.exp(scores - top)
                probs = e / jnp.sum(e, axis=1, keepdims=True)
                probs_low = probs.astype(BF16)
                gprobs = dot(go[here], vh[:seen], 1, 1)
                delta = jnp.sum(probs * gprobs, axis=1, keepdims=True)
                gs = (probs * (gprobs - delta) * SCALE).astype(BF16)
                by_row.append((dot(probs_low, vh[:seen]), dot(gs, kh[:seen])))
                keyed = (dot(gs, qh[here], 0, 0), dot(probs_low, gh[here], 0, 0))
                if by_key:
                    keyed = tuple(
                        jnp.concatenate([old + new[: old.shape[0]], new[old.shape[0] :]], axis=0)
                        for old, new in zip(by_key, keyed))
                by_key = keyed
            terms = [jnp.concatenate(t, axis=0) for t in zip(*by_row)] + list(by_key)
            total = terms if total is None else [a + b for a, b in zip(total, terms)]
        acts[at, aligned(mix_at + p * LANES, LANES)] = total[0].astype(BF16)

        def back(t):
            return t * tables[0, at, :] - swap(t) * tables[1, at, :]

        for j, g in enumerate((back(total[1]), back(total[2]), total[3])):
            acts[at, lanes[j]] = g.astype(BF16)
            sums_ref[4:5, lanes[j]] += jnp.sum(g, axis=0, keepdims=True)
        return carry

    lax.fori_loop(0, (rows // SEQ) * pairs, attention_step, 0)
    event(13)
    finish(2)
    finish(3)

    tiles = units_here // COL_TILE
    per_part = row_tiles * tiles // PARTS

    def ffn_step(i, carry):
        events_at(i, (
            (per_part, (14,)), (per_part + 2, (15,)), (2 * per_part, (16,)),
            (2 * per_part + 1, (17,)), (3 * per_part - 1, (18,)), (3 * per_part, (19,)),
        ))
        for q in range(1, PARTS):
            @pl.when(i == q * per_part)
            def _():
                finish(2 + 2 * q)
                finish(3 + 2 * q)

        at = aligned((i % row_tiles) * ROW_TILE, ROW_TILE)
        tile = i // row_tiles
        cols = aligned(tile * COL_TILE, COL_TILE)
        hidden = dot(low[at, :], wqu[:, aligned(qkv_cols + tile * COL_TILE, COL_TILE)])
        hidden = hidden + vec_ref[2:3, cols]
        grad = dot(cot[at, :], wdd[aligned(local_width + tile * COL_TILE, COL_TILE), :], 1, 1)
        square = hidden * hidden
        th = jnp.tanh(GELU_A * hidden * (1.0 + GELU_B * square))
        acts[at, aligned(act_at + tile * COL_TILE, COL_TILE)] = (
            0.5 * hidden * (1.0 + th)).astype(BF16)
        slope = 0.5 * (1.0 + th) + 0.5 * hidden * (1.0 - th * th) * (
            GELU_A * (1.0 + 3.0 * GELU_B * square))
        grad = grad * slope
        acts[at, aligned(gh_at + tile * COL_TILE, COL_TILE)] = grad.astype(BF16)
        sums_ref[3:4, cols] += jnp.sum(grad, axis=0, keepdims=True)
        return carry

    lax.fori_loop(0, row_tiles * tiles, ffn_step, 0)
    for u in range(len(units)):
        drain(u)
    for i in range(stages + 1):
        for c in vector_copies(i):
            c.wait_send()

    chunks = width // CHUNK
    every = 2 * chunks

    def remote_z(src, dst, ssem, rsem, peer):
        return pltpu.make_async_remote_copy(
            src_ref=src, dst_ref=dst, send_sem=ssem, recv_sem=rsem,
            device_id={"tensor": peer}, device_id_type=MESH)

    def columns(c):
        return aligned((c % chunks) * CHUNK, CHUNK)

    def copy_a(c):
        return remote_z(part.at[c % chunks], inbox.at[c % SLOTS], a_send.at[c % SLOTS],
                        a_recv.at[c % SLOTS], flip(level, 1))

    def copy_b(c):
        return remote_z(part.at[c % chunks], cross.at[c % SLOTS], b_send.at[c % SLOTS],
                        b_recv.at[c % SLOTS], depth - 1 - level)

    def copy_c_out(c):
        return remote_z(cross.at[c % SLOTS], inbox.at[c % SLOTS], c_send.at[c % SLOTS],
                        c_recv.at[c % SLOTS], flip(level, 1))

    def copy_c_grad(c):
        return remote_z(gn.at[:, columns(c)], gn.at[:, columns(c)], c_send.at[c % SLOTS],
                        c_recv.at[c % SLOTS], flip(level, 1))

    def out_copy(src, c):
        return pltpu.make_async_copy(src.at[c % SLOTS], block_out.at[:, columns(c)],
                                     z_out.at[c % SLOTS])

    gn_copy = pltpu.make_async_copy(x_hbm, gn, local.at[len(units) + 2])

    @pl.when(inner)
    def _():
        gn_copy.start()
        gn_copy.wait()

    add_rows = 256
    x_late = wqu.at[pl.ds(0, rows), pl.ds(0, width)]

    def by_rows(step):
        def body(i, carry):
            step(aligned(i * add_rows, add_rows))
            return carry
        lax.fori_loop(0, rows // add_rows, body, 0)

    def tick(k):
        @pl.when(inner & (k < every))
        def _():
            copy_a(k).wait_recv()

            def add(at):
                part[k % chunks, at, :] = (
                    part[k % chunks, at, :].astype(F32) + inbox[k % SLOTS, at, :].astype(F32)
                ).astype(BF16)

            by_rows(add)

            @pl.when(k >= SLOTS)
            def _():
                pl.semaphore_wait(credit, 1)

            copy_b(k).start()

        @pl.when(inner & (k >= 2) & (k < every + 2))
        def _():
            j = k - 2
            copy_b(j).wait_recv()
            copy_b(j).wait_send()

            @pl.when(j < chunks)
            def _():
                def add(at):
                    pair = part[j % chunks, at, :].astype(F32) + cross[j % SLOTS, at, :].astype(F32)
                    shifts = vec_ref[5:6, columns(j)], vec_ref[6:7, columns(j)]
                    wide = gn[at, columns(j)].astype(F32)
                    cross[j % SLOTS, at, :] = (wide + pair + shifts[0] + shifts[1]).astype(BF16)

                by_rows(add)
                copy_c_out(j).start()
                out_copy(cross, j).start()

            @pl.when(j >= chunks)
            def _():
                def add(at):
                    gn[at, columns(j)] = (
                        part[j % chunks, at, :].astype(F32) + cross[j % SLOTS, at, :].astype(F32)
                    ).astype(BF16)

                by_rows(add)
                copy_c_grad(j).start()

        @pl.when(inner & (k >= 4) & (k < every + 4))
        def _():
            i = k - 4

            @pl.when(i < chunks)
            def _():
                copy_c_out(i).wait_send()
                out_copy(cross, i).wait()

            @pl.when(i >= chunks)
            def _():
                copy_c_grad(i).wait_send()

            @pl.when(i < every - SLOTS)
            def _():
                pl.semaphore_signal(
                    credit, inc=1, device_id={"tensor": depth - 1 - level}, device_id_type=MESH)

        @pl.when(outer & (k >= 4) & (k < every + 4))
        def _():
            i = k - 4
            copy_a(i).wait_send()

            @pl.when(i < chunks)
            def _():
                copy_c_out(i).wait_recv()
                out_copy(inbox, i).start()
                out_copy(inbox, i).wait()

            @pl.when(i >= chunks)
            def _():
                copy_c_grad(i).wait_recv()

            @pl.when(i + SLOTS < every)
            def _():
                copy_a(i + SLOTS).start()

        @pl.when((k >= chunks + 4) & (k < every + 4))
        def _():
            cols = columns(k - 4)

            def gather_sums(at):
                g = gn[at, cols].astype(F32)
                normed = (x_late[at, cols].astype(F32) - stats[at, 0:1]) * stats[at, 1:2]
                product = g * normed
                gain = vec_ref[0:1, cols]
                tables[0, at, :] += g * gain
                tables[1, at, :] += product * gain
                sums_ref[0:1, cols] += jnp.sum(product, axis=0, keepdims=True)
                sums_ref[1:2, cols] += jnp.sum(g, axis=0, keepdims=True)

            by_rows(gather_sums)

    def ticks(lo, hi):
        def body(k, carry):
            tick(k)
            return carry
        lax.fori_loop(lo, hi, body, 0)

    def produce(first, tile, r, t):
        at = aligned(r * ROW_TILE, ROW_TILE)
        for j in range(COL_TILE // CHUNK):
            part[(first + tile * (COL_TILE // CHUNK) + j) % chunks, at, :] = (
                t[:, j * CHUNK : (j + 1) * CHUNK].astype(BF16))

    per_tile = COL_TILE // CHUNK

    def branch_step(i, carry):
        tile, r = i // row_tiles, i % row_tiles
        at = aligned(r * ROW_TILE, ROW_TILE)
        cols = aligned(tile * COL_TILE, COL_TILE)
        produce(0, tile, r, dot(acts[at, pl.ds(mix_at, local_width + units_here)], wdd[:, cols]))

        @pl.when(r == row_tiles - 1)
        def _():
            for j in range(per_tile):
                @pl.when(outer & (tile * per_tile + j < SLOTS))
                def _():
                    copy_a(tile * per_tile + j).start()

            @pl.when(tile % 4 == 3)
            def _():
                tick(tile // 4)

        return carry

    lax.fori_loop(0, row_tiles * width // COL_TILE, branch_step, 0)
    done_ticks = width // COL_TILE // 4

    grad_tiles = acts.shape[1] // GRAD_TILE
    low_tiles = mix_at // GRAD_TILE
    across = width // GRAD_TILE
    blocks = 2 ** stages
    staged = wdd.shape[0] // block_rows * across // grad_tiles * grad_tiles

    def stage_at(k, p=None):
        start, size = (0, block_rows) if p is None else (p * (block_rows // 2), block_rows // 2)
        at = aligned((k // across) * block_rows + start, size)
        return wdd.at[at, aligned((k % across) * GRAD_TILE, GRAD_TILE)]

    def relative(base, v):
        for i, bit in enumerate(bits):
            has = (v // 2 ** (stages - 1 - i)) % 2
            base = base + has * (bit - 2 * bit * ((base // bit) % 2))
        return base

    def turn(block):
        cols = aligned(block * block_rows, block_rows)
        turned[0] = jnp.transpose(low[:, cols])
        turned[1] = jnp.transpose(cot[:, cols])

    def grad_tile(n):
        return dot(turned[n // low_tiles], acts[:, aligned(n * GRAD_TILE, GRAD_TILE)])

    def core_copy(i):
        return remote_dp(stage_at(i % staged), core_rx.at[i], core_send.at[i % staged],
                         core_recv.at[i], flip(me, 1))

    def other_step(i, carry):
        n = i % grad_tiles

        @pl.when(n == 0)
        def _():
            turn(relative(flip(me, 1), blocks - 1 - i // grad_tiles))

        @pl.when(i >= staged)
        def _():
            core_copy(i - staged).wait_send()

        stage_at(i % staged)[...] = grad_tile(n).astype(BF16)
        core_copy(i).start()

        @pl.when(i % TICK_TILES == TICK_TILES - 1)
        def _():
            tick(done_ticks + i // TICK_TILES)

        return carry

    lax.fori_loop(0, blocks * grad_tiles, other_step, 0)
    done_ticks += blocks * grad_tiles // TICK_TILES

    def first_bit(v, order):
        for s, bit in enumerate(order):
            if v // 2 ** (stages - 1 - bits.index(bit)) % 2:
                return s
        return len(order)

    pieces = {}
    for v in range(blocks):
        for p, order in enumerate(orders):
            for s in range(first_bit(v, order)):
                pieces[(v, p, s)] = len(pieces)
    spare = staged

    def link_copy(v, p, n):
        order = orders[p]
        s = first_bit(v, order)
        left = v - 2 ** (stages - 1 - bits.index(order[s]))
        piece = pieces[(left, p, s)]
        return remote_dp(
            stage_at((blocks - 1 - v) * grad_tiles + n, p), link_rx.at[piece, n],
            link_send.at[2 * (v - 1) + p, n], link_recv.at[piece, n], flip(me, order[s]))

    def arrival(v, p, s, n):
        piece = pieces[(v, p, s)]
        return remote_dp(
            stage_at(0, p), link_rx.at[piece, n], link_send.at[0, 0], link_recv.at[piece, n],
            flip(me, orders[p][s]))

    def own_block(v, ticks_at):
        q = blocks - 1 - v
        mine = [key for key in pieces if key[0] == v]
        assert v == 0 or len(mine) < 2

        def core_slot(n):
            return stage_at(spare + n % DEPTH)

        def core_fetch(n):
            return pltpu.make_async_copy(
                core_rx.at[q * grad_tiles + n], core_slot(n), fetch_sem.at[n % DEPTH, 0])

        def piece_slot(key, n):
            _, p, s = key
            if v == 0:
                return stage_at((n % DEPTH) * stages + s, p)
            return spare_tiles.at[n % DEPTH]

        def piece_fetch(key, n):
            return pltpu.make_async_copy(
                link_rx.at[pieces[key], n], piece_slot(key, n),
                fetch_sem.at[n % DEPTH, 1 + mine.index(key)])

        def fetch(n):
            core_copy(q * grad_tiles + n).wait_recv()
            core_fetch(n).start()
            for key in mine:
                arrival(*key, n).wait_recv()
                piece_fetch(key, n).start()

        def grad_out(n):
            at = aligned((n % 2) * block_rows, block_rows)
            flat, tall = mask.at[at, :], mask.at[:, at]
            sem = grad_sem.at[n % 2]
            first = qkv_cols // GRAD_TILE
            each = local_width // GRAD_TILE
            last = low_tiles + local_width // GRAD_TILE
            cases = (
                (n < first, flat, lambda: qkv_out.at[n // each].at[
                    :, aligned((n % each) * GRAD_TILE, GRAD_TILE)]),
                ((n >= first) & (n < low_tiles), flat,
                 lambda: up_out.at[:, aligned((n - first) * GRAD_TILE, GRAD_TILE)]),
                ((n >= low_tiles) & (n < last), tall,
                 lambda: dense_out.at[aligned((n - low_tiles) * GRAD_TILE, GRAD_TILE), :]),
                (n >= last, tall,
                 lambda: down_out.at[aligned((n - last) * GRAD_TILE, GRAD_TILE), :]),
            )
            return [(c, pltpu.make_async_copy(src, dst(), sem)) for c, src, dst in cases]

        def for_out(n, act):
            for cond, copy in grad_out(n):
                @pl.when(cond)
                def _():
                    act(copy)

        turn(relative(me, v))
        if v == 0:
            for n in range(DEPTH * stages):
                for p in range(2):
                    link_copy(blocks - 1, p, n).wait_send()
        for n in range(DEPTH - 1):
            fetch(n)

        def step(n, carry):
            for when, k in ticks_at:
                @pl.when(n == when)
                def _():
                    tick(k)

            t = grad_tile(n)
            core_fetch(n).wait()
            t = t + core_slot(n)[...].astype(F32)
            for key in mine:
                piece_fetch(key, n).wait()
            for s in sorted({key[2] for key in mine}):
                sides = []
                for p in range(2):
                    rows_p = slice(p * (block_rows // 2), (p + 1) * (block_rows // 2))
                    side = t[rows_p]
                    if (v, p, s) in pieces:
                        side = side + piece_slot((v, p, s), n)[...].astype(F32)
                    sides.append(side)
                t = jnp.concatenate(sides, axis=0)
            if v:
                k = (blocks - 1 - v) * grad_tiles + n
                core_copy(k if v < blocks - 1 else k + staged).wait_send()
                stage_at(k)[...] = t.astype(BF16)
                for p in range(2):
                    link_copy(v, p, n).start()
            else:
                @pl.when((n >= 2) & (n != low_tiles + 1))
                def _():
                    for_out(n - 2, lambda c: c.wait())

                @pl.when(n == low_tiles)
                def _():
                    for_out(n - 1, lambda c: c.wait())

                @pl.when(n < low_tiles)
                def _():
                    mask[aligned((n % 2) * block_rows, block_rows), :] = t

                @pl.when(n >= low_tiles)
                def _():
                    mask[:, aligned((n % 2) * block_rows, block_rows)] = jnp.transpose(t)

                for_out(n, lambda c: c.start())

            @pl.when(n + DEPTH - 1 < grad_tiles)
            def _():
                fetch(n + DEPTH - 1)

            return carry

        lax.fori_loop(0, grad_tiles, step, 0)
        if v == 0:
            for n in (grad_tiles - 2, grad_tiles - 1):
                for cond, copy in grad_out(n):
                    if bool(cond):
                        copy.wait()

    own_block(blocks - 1, ((grad_tiles // 2, done_ticks),))
    done_ticks += 1
    before = done_ticks
    lag = SLOTS - 2 - per_tile

    def grad_step(i, carry):
        tile, r = i // row_tiles, i % row_tiles

        @pl.when(r == 0)
        def _():
            mid = width // COL_TILE // 2
            taken = ((tile > mid) & (tile < mid + blocks - 1)).astype(jnp.int32)
            until = lag + per_tile * (tile + 1)
            ticks(
                jnp.maximum(before, until - per_tile + taken),
                jnp.maximum(before, until),
            )

            for v in range(1, blocks - 1):
                @pl.when(tile == mid + blocks - 2 - v)
                def _():
                    own_block(v, ((grad_tiles // 2, until),))

        at = aligned(r * ROW_TILE, ROW_TILE)
        t = dot(acts[at, pl.ds(0, mix_at)], wqu[aligned(tile * COL_TILE, COL_TILE), :], 1, 1)
        produce(chunks, tile, r, t)
        return carry

    lax.fori_loop(0, row_tiles * width // COL_TILE, grad_step, 0)
    done_ticks = lag + per_tile * (width // COL_TILE)
    last_block = every - 4
    late_copy = pltpu.make_async_copy(x_hbm, x_late, local.at[len(units)])
    late_copy.start()
    tables[...] = jnp.zeros_like(tables)
    late_copy.wait()

    ticks(done_ticks, last_block)
    own_block(0, ((grad_tiles // 4, last_block), (3 * grad_tiles // 4, last_block + 1)))
    ticks(last_block + 2, every + 4)
    for v in range(1, blocks):
        for p in range(2):
            for n in range(grad_tiles):
                if v == blocks - 1 and n < DEPTH * stages:
                    continue
                link_copy(v, p, n).wait_send()

    def row_slot(i):
        return vec_in.at[aligned((i % 2) * BACK_ROWS, BACK_ROWS), :]

    def row_copy(i):
        return pltpu.make_async_copy(
            row_slot(i), input_grad.at[aligned(i * BACK_ROWS, BACK_ROWS), :], row_sem.at[i % 2])

    def back_step(i, carry):
        at = aligned(i * BACK_ROWS, BACK_ROWS)
        mean, inv = stats[at, 0:1], stats[at, 1:2]
        first = jnp.sum(tables[0, at, :], axis=1, keepdims=True) * (inv / width)
        second = jnp.sum(tables[1, at, :], axis=1, keepdims=True) * (inv * inv / width)
        scaled = gn[at, :].astype(F32) * vec_ref[0:1, :]
        grad = scaled * inv - (x_late[at, :].astype(F32) - mean) * second - first

        @pl.when(i >= 2)
        def _():
            row_copy(i - 2).wait()

        row_slot(i)[...] = grad + cot[at, :].astype(F32)
        row_copy(i).start()
        return carry

    back_steps = rows // BACK_ROWS

    def sum_copy(i, bit):
        return remote_dp(sums_ref, sum_in.at[i], sum_send.at[i], sum_recv.at[i], flip(me, bit))

    trips = bits + [1]
    for i, bit in enumerate(trips):
        copy = sum_copy(i, bit)
        copy.start()
        lax.fori_loop(back_steps * i // len(trips), back_steps * (i + 1) // len(trips), back_step, 0)
        copy.wait()
        sums_ref[...] = sums_ref[...] + sum_in[i]
    mine_ref[...] = sums_ref[:, aligned(me * block_rows, block_rows)]
    row_copy(back_steps - 2).wait()
    row_copy(back_steps - 1).wait()


def fits(shards, depth, local_width, block_cols):
    return (
        shards & (shards - 1) == 0 and len(link_bits(shards)) == 2 and depth == 4
        and block_cols % COL_TILE == 0 and local_width % GRAD_TILE == 0
    )


def layer(x, cot, qkv_share, dense_share, up_share, down_share, vectors, segments):
    rows, width = x.shape
    count = lax.axis_size("dp")
    local_width = dense_share.shape[0]
    units_here = up_share.shape[1]
    block_rows = up_share.shape[0]
    seqs = rows // SEQ
    links = len(link_bits(count))
    blocks = 2 ** links
    slots = 2 * (blocks - 1) + blocks
    acts_cols = 4 * local_width + 2 * units_here
    grad_tiles = acts_cols // GRAD_TILE
    pieces = 0
    for order in range(2):
        pieces += sum(blocks // 2 ** (s + 1) for s in range(links))
    staged = (local_width + units_here) // block_rows * (width // GRAD_TILE) // grad_tiles * grad_tiles
    chunks = width // CHUNK
    any_ = pl.BlockSpec(memory_space=pl.ANY)
    vmem = pl.BlockSpec(memory_space=pltpu.VMEM)
    b16 = lambda *s: jax.ShapeDtypeStruct(s, BF16)
    f32 = lambda *s: jax.ShapeDtypeStruct(s, F32)
    dma = lambda *s: pltpu.SemaphoreType.DMA(s)
    outs = pl.pallas_call(
        layer_body,
        in_specs=[any_] * 6 + [vmem] * 6,
        out_specs=[any_] * 8 + [vmem] * 2,
        out_shape=[
            b16(rows, width), f32(rows, width), f32(3, block_rows, local_width),
            f32(local_width, block_rows), f32(block_rows, units_here), f32(units_here, block_rows),
            b16(blocks * grad_tiles, block_rows, GRAD_TILE),
            b16(pieces, grad_tiles, block_rows // 2, GRAD_TILE), f32(8, width),
            f32(8, block_rows),
        ],
        scratch_shapes=[
            pltpu.VMEM((width, 3 * local_width + units_here), BF16),
            pltpu.VMEM((local_width + units_here, width), BF16),
            pltpu.VMEM((rows, acts_cols), BF16), pltpu.VMEM((rows, width), BF16),
            pltpu.VMEM((rows, width), BF16), pltpu.VMEM((SEQ, SEQ), F32),
            pltpu.VMEM((8, width), F32), pltpu.VMEM((8 * count, width), F32),
            pltpu.VMEM((2, block_rows, rows), BF16), pltpu.VMEM((rows, width), BF16),
            pltpu.VMEM((chunks, rows, CHUNK), BF16), pltpu.VMEM((SLOTS, rows, CHUNK), BF16),
            pltpu.VMEM((SLOTS, rows, CHUNK), BF16),
            pltpu.VMEM((2, rows, LANES), F32), pltpu.VMEM((rows, LANES), F32),
            pltpu.VMEM((DEPTH, block_rows // 2, GRAD_TILE), BF16), pltpu.VMEM((links + 1, 8, width), F32),
            dma(2 + 2 * PARTS, slots), dma(2 + 2 * PARTS, slots), dma(count - 1), dma(count - 1),
            dma(7 + 2 * PARTS),
            dma(SLOTS), dma(SLOTS), dma(SLOTS), dma(SLOTS), dma(SLOTS), dma(SLOTS), dma(SLOTS),
            pltpu.SemaphoreType.REGULAR,
            dma(staged), dma(blocks * grad_tiles), dma(2 * (blocks - 1), grad_tiles),
            dma(pieces, grad_tiles), dma(DEPTH, 1 + 2 * links), dma(2), dma(2),
            dma(links + 1), dma(links + 1),
        ],
        compiler_params=pltpu.CompilerParams(
            collective_id=0, has_side_effects=True, vmem_limit_bytes=67_043_328),
        cost_estimate=pl.CostEstimate(
            flops=18 * rows * width * (local_width + units_here), bytes_accessed=80_000_000,
            transcendentals=rows * units_here),
        name="layer",
    )(
        x, cot, qkv_share, dense_share, up_share, down_share, *vectors, INVERSE,
        segments.reshape(seqs, 1, SEQ),
    )
    return outs[:6] + outs[8:]


def gelu_tanh(inputs):
    return jax.nn.gelu(inputs, approximate=True)


def line_sum(part, finish):
    size = lax.axis_size("tensor")
    if size != 4:
        return finish(lax.psum(part, "tensor").astype(F32))
    index = lax.axis_index("tensor")
    inward = lax.ppermute(part, "tensor", [(0, 1), (3, 2)])
    pair = (part.astype(F32) + inward.astype(F32)).astype(BF16)
    other = lax.ppermute(pair, "tensor", [(1, 2), (2, 1)])
    done = finish(pair.astype(F32) + other.astype(F32))
    back = lax.ppermute(done, "tensor", [(1, 0), (2, 3)])
    return jnp.where((index == 0) | (index == size - 1), back, done)


def local(
    block_input, segments, norm_gain, norm_bias, qkv_weight, query_value_bias, key_bias,
    dense_weight, dense_bias, up_weight, up_bias, down_weight, down_bias, cotangent,
):
    rows, width = block_input.shape
    local_width = qkv_weight.shape[2]
    heads = local_width // HEAD
    seqs = rows // SEQ
    shards = lax.axis_size("dp")
    fused = fits(shards, lax.axis_size("tensor"), local_width, down_weight.shape[1])
    if fused:
        mine = lax.axis_index("dp")
        four = jnp.stack([norm_gain, norm_bias, dense_bias, down_bias])
        block_output, input_grad, qkv_out, dense_out, up_out, down_out, total, own = layer(
            block_input, cotangent, qkv_weight.transpose(1, 0, 2), dense_weight, up_weight,
            down_weight, [four, up_bias.T, query_value_bias, key_bias.T], segments)

        def mine_of(value, lead):
            return lax.dynamic_index_in_dim(
                value.reshape(lead, shards, -1), mine, axis=1, keepdims=False)

        sums = total[4]
        qv_sums = jnp.stack([sums[:local_width], sums[2 * local_width : 3 * local_width]])
        key_sums = sums[local_width : 2 * local_width].reshape(heads, HEAD)[:, :ROT]
        gain_out, shift_out, bias_out = own[0], own[1], own[2]
        return (
            block_output, input_grad, gain_out, shift_out, qkv_out.transpose(1, 0, 2),
            mine_of(qv_sums, 2 * heads).reshape(query_value_bias.shape),
            mine_of(key_sums, heads), dense_out, bias_out, up_out,
            mine_of(total[3], up_bias.shape[0]), down_out, bias_out,
        )
    smalls = (norm_gain, norm_bias, dense_bias, down_bias, up_bias, query_value_bias, key_bias)
    packed = jnp.concatenate([s.reshape(1, -1) for s in smalls], axis=1)
    packed = lax.all_gather(packed, "dp", axis=0, tiled=True)
    pieces = []
    at = 0
    for s in smalls:
        pieces.append(packed[:, at : at + s.size].reshape((shards,) + s.shape).astype(F32))
        at += s.size
    gain, shift, dense_shift, down_shift = [p.reshape(1, -1) for p in pieces[:4]]
    up_shift = pieces[4].transpose(1, 0, 2).reshape(1, -1)
    qv_bias = pieces[5].transpose(1, 2, 0, 3).reshape(2, local_width)
    key_part = pieces[6].transpose(1, 0, 2).reshape(heads, ROT)
    key_full = jnp.concatenate([key_part, jnp.zeros((heads, HEAD - ROT), F32)], axis=1)
    bias = jnp.concatenate(
        [qv_bias[0:1], key_full.reshape(1, -1), qv_bias[1:2], jnp.zeros((5, local_width), F32)], axis=0
    )

    dense_all = lax.all_gather(dense_weight, "dp", axis=1, tiled=True)
    qkv_all = lax.all_gather(qkv_weight.reshape(qkv_weight.shape[0], -1), "dp", axis=0, tiled=True)
    up_all = lax.all_gather(up_weight, "dp", axis=0, tiled=True)
    down_all = lax.all_gather(down_weight, "dp", axis=1, tiled=True)

    wide = block_input.astype(F32)
    mean = jnp.mean(wide, axis=1, keepdims=True)
    centred = wide - mean
    inv_std = lax.rsqrt(jnp.mean(centred * centred, axis=1, keepdims=True) + EPSILON)
    normed = centred * inv_std
    low = (normed * gain + shift).astype(BF16)

    tables = rotary_tables(segments)
    grad_mixed = dot(cotangent, dense_all, 1, 1).astype(BF16)
    projected = dot(low, qkv_all)
    mixed, grad_projected, bias_sums = attention(projected, grad_mixed, bias, tables, segments)
    bias_sums = jnp.sum(bias_sums, axis=0)

    hidden = dot(low, up_all) + up_shift
    activated, gelu_back = jax.vjp(gelu_tanh, hidden)
    activated = activated.astype(BF16)
    grad_hidden = gelu_back(dot(cotangent, down_all, 1, 1))[0]
    grad_up_bias = jnp.sum(grad_hidden, axis=0)
    grad_hidden_low = grad_hidden.astype(BF16)
    grad_joined = jnp.concatenate([grad_projected[i] for i in range(3)], axis=1)

    branches = (dot(mixed, dense_all) + dot(activated, down_all)).astype(BF16)
    grad_part = (dot(grad_joined, qkv_all, 1, 1) + dot(grad_hidden_low, up_all, 1, 1)).astype(BF16)
    grad_dense = dot(mixed, cotangent, 0, 0).astype(BF16)
    grad_qkv = dot(low, grad_joined, 0, 0).astype(BF16)
    grad_down = dot(activated, cotangent, 0, 0).astype(BF16)
    grad_up = dot(low, grad_hidden_low, 0, 0).astype(BF16)

    outs, grads = [], []
    for s in range(seqs):
        at = slice(s * SEQ, (s + 1) * SEQ)
        outs.append(
            line_sum(
                branches[at],
                lambda t, at=at: (wide[at] + t + dense_shift + down_shift).astype(BF16),
            )
        )
    for s in range(seqs):
        at = slice(s * SEQ, (s + 1) * SEQ)
        grads.append(line_sum(grad_part[at], lambda t: t.astype(BF16)))
    block_output = jnp.concatenate(outs, axis=0)
    grad_normed = jnp.concatenate(grads, axis=0).astype(F32)

    grad_wide = cotangent.astype(F32)
    scaled = grad_normed * gain
    input_grad = (
        inv_std
        * (
            scaled
            - jnp.mean(scaled, axis=1, keepdims=True)
            - normed * jnp.mean(scaled * normed, axis=1, keepdims=True)
        )
        + grad_wide
    )

    def scatter(value, dim):
        return lax.psum_scatter(value, "dp", scatter_dimension=dim, tiled=True).astype(F32)

    qkv_out = scatter(grad_qkv, 0).reshape(qkv_weight.shape)
    dense_out = scatter(grad_dense, 1)
    up_out = scatter(grad_up, 0)
    down_out = scatter(grad_down, 1)

    key_sums = bias_sums[1].reshape(heads, HEAD)[:, :ROT]
    qv_sums = jnp.stack([bias_sums[0], bias_sums[2]]).reshape(2, heads, HEAD)
    small_sums = (
        jnp.sum(grad_normed * normed, axis=0).reshape(shards, -1),
        jnp.sum(grad_normed, axis=0).reshape(shards, -1),
        jnp.sum(grad_wide, axis=0).reshape(shards, -1),
        grad_up_bias.reshape(up_bias.shape[0], shards, -1).transpose(1, 0, 2).reshape(shards, -1),
        qv_sums.reshape(2, heads, shards, -1).transpose(2, 0, 1, 3).reshape(shards, -1),
        key_sums.reshape(heads, shards, -1).transpose(1, 0, 2).reshape(shards, -1),
    )
    total = lax.psum_scatter(
        jnp.concatenate(small_sums, axis=1), "dp", scatter_dimension=0, tiled=True
    ).reshape(-1)
    shapes = (norm_gain.shape, norm_bias.shape, dense_bias.shape, up_bias.shape,
              query_value_bias.shape, key_bias.shape)
    smalls_out = []
    at = 0
    for part, shape in zip(small_sums, shapes):
        smalls_out.append(total[at : at + part.shape[1]].reshape(shape))
        at += part.shape[1]
    gain_out, shift_out, bias_out, up_bias_out, qv_out, key_out = smalls_out
    return (
        block_output, input_grad, gain_out, shift_out, qkv_out, qv_out, key_out, dense_out,
        bias_out, up_out, up_bias_out, down_out, bias_out,
    )


def solution(mesh):
    in_specs = (
        P("dp", None),
        P("dp"),
        P("dp"),
        P("dp"),
        P("dp", None, "tensor"),
        P(None, "tensor", "dp"),
        P("tensor", "dp"),
        P("tensor", "dp"),
        P("dp"),
        P("dp", "tensor"),
        P("tensor", "dp"),
        P("tensor", "dp"),
        P("dp"),
        P("dp", None),
    )
    out_specs = (
        P("dp", None),
        P("dp", None),
        P("dp"),
        P("dp"),
        P("dp", None, "tensor"),
        P(None, "tensor", "dp"),
        P("tensor", "dp"),
        P("tensor", "dp"),
        P("dp"),
        P("dp", "tensor"),
        P("tensor", "dp"),
        P("tensor", "dp"),
        P("dp"),
    )
    return jax.shard_map(local, mesh=mesh, in_specs=in_specs, out_specs=out_specs, check_vma=False)
```
